8 devices in a mesh: dp: 1 (over z), tpx: 2 (over y), tpy: 4 (over x, core).
Axes of the slice: x: 2, y: 2, z: 1, core: 2. Of those that a mesh axis runs over, the one named last changes fastest.
Arguments:
- hidden: bfloat16 [256, 2048], P('dp', ('tpx', 'tpy'))
- ln_scale: float32 [2048], P(('tpx', 'tpy'))
- w_q: bfloat16 [2048, 2048], P('tpx', 'tpy')
- w_k: bfloat16 [2048, 256], P('tpx')
- w_v: bfloat16 [2048, 256], P('tpx')
- w_gate: bfloat16 [2048, 16384], P('tpx', 'tpy')
- w_up: bfloat16 [2048, 16384], P('tpx', 'tpy')
- w_o: bfloat16 [2048, 2048], P('tpy', 'tpx')
- w_down: bfloat16 [16384, 2048], P('tpy', 'tpx')
- k_cache: bfloat16 [256, 2048, 256], P(('dp', 'tpx', 'tpy'))
- v_cache: bfloat16 [256, 2048, 256], P(('dp', 'tpx', 'tpy'))
- positions: int32 [256], P(('dp', 'tpx', 'tpy'))
Outputs:
- output 1: bfloat16 [256, 2048], P('dp', ('tpx', 'tpy'))
- output 2: bfloat16 [256, 2048, 256], P(('dp', 'tpx', 'tpy'))
- output 3: bfloat16 [256, 2048, 256], P(('dp', 'tpx', 'tpy'))
All inputs are finite; a program needn't handle non-finite values.
Results may differ from the reference program's by a relative error of at most 0.00643104.
Values are sent between devices in bfloat16 or wider.
A program may use at most 1 GiB of HBM per device.

```python
import math
import jax
import jax.numpy as jnp
from jax import lax

D_MODEL = 2048
N_HEADS = 8
HEAD_DIM = 256
FF_DIM = 16384
SEQ_COUNT = 256
CACHE_LEN = 2048


def draw_positions(len_key, perm_key):
    pos_draw = jax.random.randint(len_key, (SEQ_COUNT,), 200, CACHE_LEN)
    seq_order = jax.random.permutation(perm_key, SEQ_COUNT)
    seq_ids = jnp.arange(SEQ_COUNT)
    positions = jnp.where(seq_ids == seq_order[0], CACHE_LEN - 1, pos_draw)
    positions = jnp.where(seq_ids == seq_order[1], 200, positions)
    return positions.astype(jnp.int32)


def setup_inputs(seed: int = 0, part: int = 0) -> dict:
    root_key = jax.random.key(seed)
    part_keys = jax.random.split(jax.random.fold_in(root_key, part), 8)
    shared_keys = jax.random.split(root_key, 8)
    d_scale = D_MODEL ** -0.5
    col_scale = 0.5 + 1.5 * jnp.arange(D_MODEL, dtype=jnp.float32) / D_MODEL
    hidden = 0.5 + col_scale * jax.random.normal(part_keys[0], (SEQ_COUNT, D_MODEL), jnp.float32)
    ln_scale = jax.random.uniform(shared_keys[0], (D_MODEL,), jnp.float32, 0.5, 1.5)
    w_k = jax.random.normal(shared_keys[1], (D_MODEL, HEAD_DIM), jnp.float32) * d_scale
    align_coef = min(0.9, math.log(CACHE_LEN / 2) / math.sqrt(HEAD_DIM))
    noise_coef = math.sqrt(1.0 - align_coef * align_coef)
    q_noise = jax.random.normal(shared_keys[2], (D_MODEL, N_HEADS, HEAD_DIM), jnp.float32) * d_scale
    w_q = (align_coef * w_k[:, None, :] + noise_coef * q_noise).reshape(D_MODEL, N_HEADS * HEAD_DIM)
    w_v = jax.random.normal(shared_keys[3], (D_MODEL, HEAD_DIM), jnp.float32) * d_scale
    w_gate = jax.random.normal(shared_keys[4], (D_MODEL, FF_DIM), jnp.float32) * d_scale
    w_up = jax.random.normal(shared_keys[5], (D_MODEL, FF_DIM), jnp.float32) * d_scale
    w_o = jax.random.normal(shared_keys[6], (N_HEADS * HEAD_DIM, D_MODEL), jnp.float32) * (N_HEADS * HEAD_DIM) ** -0.5
    w_down = jax.random.normal(shared_keys[7], (FF_DIM, D_MODEL), jnp.float32) * FF_DIM ** -0.5
    k_cache = jax.random.normal(part_keys[1], (SEQ_COUNT, CACHE_LEN, HEAD_DIM), jnp.float32)
    seq_mean = jax.random.normal(part_keys[2], (SEQ_COUNT, 1, HEAD_DIM), jnp.float32)
    v_cache = seq_mean + 0.5 * jax.random.normal(part_keys[3], (SEQ_COUNT, CACHE_LEN, HEAD_DIM), jnp.float32)
    positions = draw_positions(part_keys[4], part_keys[5])
    return {
        'hidden': hidden.astype(jnp.bfloat16),
        'ln_scale': ln_scale,
        'w_q': w_q.astype(jnp.bfloat16),
        'w_k': w_k.astype(jnp.bfloat16),
        'w_v': w_v.astype(jnp.bfloat16),
        'w_gate': w_gate.astype(jnp.bfloat16),
        'w_up': w_up.astype(jnp.bfloat16),
        'w_o': w_o.astype(jnp.bfloat16),
        'w_down': w_down.astype(jnp.bfloat16),
        'k_cache': k_cache.astype(jnp.bfloat16),
        'v_cache': v_cache.astype(jnp.bfloat16),
        'positions': positions,
    }


def rope_tables(positions):
    half_dim = HEAD_DIM // 2
    inv_freq = 10000.0 ** (-(jnp.arange(half_dim, dtype=jnp.float32) * 2.0 / HEAD_DIM))
    angles = positions.astype(jnp.float32)[:, None] * inv_freq[None, :]
    return jnp.cos(angles), jnp.sin(angles)


def apply_rope(vectors, cos_tab, sin_tab):
    half_dim = HEAD_DIM // 2
    lead_half = vectors[..., :half_dim]
    tail_half = vectors[..., half_dim:]
    return jnp.concatenate([lead_half * cos_tab - tail_half * sin_tab, lead_half * sin_tab + tail_half * cos_tab], axis=-1)


def reference(hidden, ln_scale, w_q, w_k, w_v, w_gate, w_up, w_o, w_down, k_cache, v_cache, positions):
    hidden_f = hidden.astype(jnp.float32)
    mean_val = jnp.mean(hidden_f, axis=1, keepdims=True)
    var_val = jnp.mean(jnp.square(hidden_f - mean_val), axis=1, keepdims=True)
    normed = ((hidden_f - mean_val) * lax.rsqrt(var_val + 1e-6) * ln_scale).astype(jnp.bfloat16)
    q_proj = jnp.dot(normed, w_q, preferred_element_type=jnp.float32).astype(jnp.bfloat16)
    k_proj = jnp.dot(normed, w_k, preferred_element_type=jnp.float32).astype(jnp.bfloat16)
    v_proj = jnp.dot(normed, w_v, preferred_element_type=jnp.float32).astype(jnp.bfloat16)
    gate_proj = jnp.dot(normed, w_gate, preferred_element_type=jnp.float32).astype(jnp.bfloat16)
    up_proj = jnp.dot(normed, w_up, preferred_element_type=jnp.float32).astype(jnp.bfloat16)
    mlp_act = (jax.nn.silu(gate_proj.astype(jnp.float32)) * up_proj.astype(jnp.float32)).astype(jnp.bfloat16)
    mlp_out = jnp.dot(mlp_act, w_down, preferred_element_type=jnp.float32)
    cos_tab, sin_tab = rope_tables(positions)
    q_heads = q_proj.astype(jnp.float32).reshape(SEQ_COUNT, N_HEADS, HEAD_DIM)
    q_rot = apply_rope(q_heads, cos_tab[:, None, :], sin_tab[:, None, :]).astype(jnp.bfloat16)
    k_rot = apply_rope(k_proj.astype(jnp.float32), cos_tab, sin_tab).astype(jnp.bfloat16)
    is_new = jnp.arange(CACHE_LEN)[None, :, None] == positions[:, None, None]
    k_out = jnp.where(is_new, k_rot[:, None, :], k_cache)
    v_out = jnp.where(is_new, v_proj[:, None, :], v_cache)

    def one_sequence(seq_item):
        q_seq, k_seq, v_seq, pos_seq = seq_item
        scores = jnp.dot(q_seq, k_seq.T, preferred_element_type=jnp.float32) * (HEAD_DIM ** -0.5)
        valid_rows = jnp.arange(CACHE_LEN)[None, :] <= pos_seq
        scores = jnp.where(valid_rows, scores, -jnp.inf)
        attn_prob = jax.nn.softmax(scores, axis=-1).astype(jnp.bfloat16)
        return jnp.dot(attn_prob, v_seq, preferred_element_type=jnp.float32).astype(jnp.bfloat16)

    attn_heads = lax.map(one_sequence, (q_rot, k_out, v_out, positions))
    attn_out = jnp.dot(attn_heads.reshape(SEQ_COUNT, N_HEADS * HEAD_DIM), w_o, preferred_element_type=jnp.float32)
    hidden_out = (hidden_f + attn_out + mlp_out).astype(jnp.bfloat16)
    return (hidden_out, k_out, v_out)
```

```python
import functools
import jax
import jax.numpy as jnp
from jax import lax
from jax.experimental import pallas as pl
from jax.experimental.pallas import tpu as pltpu
from jax.sharding import PartitionSpec as P

LN_EPS = 1e-6
ROPE_BASE = 10000.0
MESH = pl.DeviceIdType.MESH
F32 = jnp.float32
BF16 = jnp.bfloat16
RING = 8
AHEAD = 4


def rope_tables(positions, head_dim):
    half_dim = head_dim // 2
    inv_freq = ROPE_BASE ** (-(jnp.arange(half_dim, dtype=F32) * 2.0 / head_dim))
    angles = positions.astype(F32)[:, None] * inv_freq[None, :]
    return jnp.cos(angles), jnp.sin(angles)


def rotate(x, cos_tab, sin_tab):
    half = x.shape[-1] // 2
    lead, tail = x[:, :half], x[:, half:]
    return jnp.concatenate([lead * cos_tab - tail * sin_tab, lead * sin_tab + tail * cos_tab], axis=-1)


def others(px, py):
    return [(lax.rem(px + dx, 2), lax.rem(py + dy, 4)) for dx in range(2) for dy in range(4) if (dx, dy) != (0, 0)]


def enter(px, py):
    barrier = pltpu.get_barrier_semaphore()
    for qx, qy in others(px, py):
        pl.semaphore_signal(barrier, 1, device_id={'tpx': qx, 'tpy': qy}, device_id_type=MESH)
    pl.semaphore_wait(barrier, 7)


def remote(src, dst, send_sem, recv_sem, qx, qy):
    return pltpu.make_async_remote_copy(src, dst, send_sem, recv_sem, device_id={'tpx': qx, 'tpy': qy}, device_id_type=MESH)


def project_kernel(rows, h_hbm, scale_ref, cos_ref, sin_ref, wq_hbm, wk_hbm, wv_hbm, wg_hbm, wu_hbm,
                   q_out, kn_out, vn_out, own_out, first_out, *rest):
    n_late = len(rows) - 1
    late_outs = rest[:n_late]
    (hbuf, msg, u, wq, wkv, wg, wu, part, qpart, qrec, kvpart, kvrec, qsum, qall,
     load_sem, h_send, h_recv, m_send, m_recv, x_send, x_recv, a_send, a_recv, o_sem) = rest[n_late:]
    px, py = lax.axis_index('tpx'), lax.axis_index('tpy')
    me = px * 4 + py
    mate = py + 1 - 2 * lax.rem(py, 2)
    across = lax.rem(py + 2, 4)
    n_seq = 32

    loads = [
        pltpu.make_async_copy(h_hbm, hbuf.at[py], load_sem.at[0]),
        pltpu.make_async_copy(wq_hbm, wq, load_sem.at[1]),
        pltpu.make_async_copy(wk_hbm, wkv.at[:, pl.ds(0, 256)], load_sem.at[2]),
        pltpu.make_async_copy(wv_hbm, wkv.at[:, pl.ds(256, 256)], load_sem.at[3]),
        pltpu.make_async_copy(wg_hbm, wg, load_sem.at[4]),
        pltpu.make_async_copy(wu_hbm, wu, load_sem.at[5]),
    ]
    for copy in loads:
        copy.start()
    loads[0].wait()

    hf = hbuf[py].astype(F32)
    mean = jnp.sum(hf, axis=1, keepdims=True) * (1.0 / 256.0)
    dev = hf - mean
    m2 = jnp.sum(dev * dev, axis=1, keepdims=True)
    lane = lax.broadcasted_iota(jnp.int32, (256, 128), 1)
    stat = jnp.where(lane == 0, mean, m2)
    stat_t = stat.T
    msg[me] = jnp.concatenate([stat_t[0:2], scale_ref[...], jnp.zeros((5, 256), F32)], axis=0)
    enter(px, py)

    sends = [
        remote(hbuf.at[py], hbuf.at[py], h_send.at[0], h_recv.at[0], px, across),
        remote(hbuf.at[py], hbuf.at[py], h_send.at[1], h_recv.at[1], px, mate),
    ]
    for copy in sends:
        copy.start()
    msgs = []
    for i, (qx, qy) in enumerate(others(px, py)):
        copy = remote(msg.at[me], msg.at[me], m_send.at[i], m_recv.at[i], qx, qy)
        copy.start()
        msgs.append(copy)
    for copy in msgs:
        copy.wait_recv()

    means = jnp.concatenate([msg[e, 0:1] for e in range(8)], axis=0)
    m2s = jnp.concatenate([msg[e, 1:2] for e in range(8)], axis=0)
    mu = jnp.sum(means, axis=0, keepdims=True) * 0.125
    gap = means - mu
    var = (jnp.sum(m2s, axis=0, keepdims=True) + 256.0 * jnp.sum(gap * gap, axis=0, keepdims=True)) * (1.0 / 2048.0)
    rstd = lax.rsqrt(var + LN_EPS)
    both = jnp.concatenate([mu, rstd, jnp.zeros((126, 256), F32)], axis=0).T
    mu_col, rstd_col = both[:, 0:1], both[:, 1:2]

    def norm(t):
        cols = pl.ds(pl.multiple_of(t * 256, 256), 256)
        scale = msg[px * 4 + t, 2:3]
        u[:, cols] = ((hbuf[t].astype(F32) - mu_col) * rstd_col * scale).astype(BF16)

    norm(py)
    sends[0].wait_recv()
    relay = remote(hbuf.at[across], hbuf.at[across], h_send.at[2], h_recv.at[2], px, mate)
    relay.start()
    sends.append(relay)
    norm(across)
    sends[1].wait_recv()
    norm(mate)
    relay.wait_recv()
    norm(lax.rem(mate + 2, 4))

    loads[1].wait()
    qpart[...] = jnp.dot(u[...], wq[...], preferred_element_type=F32)
    far = pl.ds(pl.multiple_of((1 - px) * 128, 128), 128)
    near = pl.ds(pl.multiple_of(px * 128, 128), 128)
    q_copy = remote(qpart.at[far], qrec, x_send.at[0], x_recv.at[0], 1 - px, py)
    q_copy.start()
    loads[2].wait()
    loads[3].wait()
    far_seq = pl.ds(pl.multiple_of((1 - px) * 128 + py * n_seq, n_seq), n_seq)
    near_seq = pl.ds(pl.multiple_of(px * 128 + py * n_seq, n_seq), n_seq)
    u_kv = jnp.concatenate([u[far_seq, :], u[near_seq, :]], axis=0)
    kvpart[...] = jnp.dot(u_kv, wkv[...], preferred_element_type=F32)
    kv_copy = remote(kvpart.at[pl.ds(0, n_seq)], kvrec, x_send.at[1], x_recv.at[1], 1 - px, py)
    kv_copy.start()

    loads[4].wait()
    loads[5].wait()
    step = 512

    def columns(i, carry):
        cols = pl.ds(pl.multiple_of(i * step, step), step)
        part[:, cols] = jnp.dot(u[...], wg[:, cols], preferred_element_type=F32)
        up_cols = pl.ds(pl.multiple_of(4096 + i * step, step), step)
        part[:, up_cols] = jnp.dot(u[...], wu[:, cols], preferred_element_type=F32)
        return carry

    lax.fori_loop(0, 4096 // step, columns, 0)

    def far_rows(c):
        return pl.ds(pl.multiple_of((1 - px) * 128 + sum(rows[:c]), 8), rows[c])

    first = remote(part.at[far_rows(0)], first_out, x_send.at[2], x_recv.at[2], 1 - px, py)
    first.start()
    outs = [pltpu.make_async_copy(part.at[near], own_out, o_sem.at[0])]
    for c in range(1, len(rows)):
        outs.append(pltpu.make_async_copy(part.at[far_rows(c)], late_outs[c - 1], o_sem.at[c]))
    for copy in outs:
        copy.start()

    cos_tab, sin_tab = cos_ref[...], sin_ref[...]
    kv_copy.wait_recv()
    kv = (kvpart[pl.ds(n_seq, n_seq), :] + kvrec[...]).astype(BF16).astype(F32)
    kn_out[...] = rotate(kv[:, :256], cos_tab, sin_tab)
    vn_out[...] = kv[:, 256:]
    q_copy.wait_recv()
    for t in range(4):
        rows_t = pl.ds(pl.multiple_of(px * 128 + t * n_seq, n_seq), n_seq)
        qsum[t] = (qpart[rows_t, :] + qrec[pl.ds(t * n_seq, n_seq), :]).astype(BF16)
    hops = []
    for i in range(1, 4):
        t = lax.rem(py + i, 4)
        copy = remote(qsum.at[t], qall.at[py], a_send.at[i - 1], a_recv.at[i - 1], px, t)
        copy.start()
        hops.append(copy)

    def emit(t, block):
        block = block.astype(F32)
        for j in range(2):
            row = pl.multiple_of((2 * t + j) * n_seq, n_seq)
            turned = rotate(block[:, j * 256:(j + 1) * 256], cos_tab, sin_tab).astype(BF16).astype(F32)
            q_out[0, pl.ds(row, n_seq), :] = turned[:, :128]
            q_out[1, pl.ds(row, n_seq), :] = turned[:, 128:]

    emit(py, qsum[py])
    for i in range(1, 4):
        hops[i - 1].wait_recv()
        t = lax.rem(py + 4 - i, 4)
        emit(t, qall[t])
    kn_out[...] = kn_out[...].astype(BF16).astype(F32)

    for copy in outs:
        copy.wait()
    for copy in sends + msgs + hops + [q_copy, kv_copy]:
        copy.wait_send()
    first.wait()


def project(rows, hidden, ln_scale, cos_tab, sin_tab, w_q, w_k, w_v, w_gate, w_up):
    any_spec = pl.BlockSpec(memory_space=pl.ANY)
    vmem = pl.BlockSpec(memory_space=pltpu.VMEM)
    sds = jax.ShapeDtypeStruct
    dma = pltpu.SemaphoreType.DMA
    n_late = len(rows) - 1
    return pl.pallas_call(
        functools.partial(project_kernel, rows),
        out_shape=[sds((2, 256, 128), F32), sds((32, 256), F32), sds((32, 256), F32), sds((128, 8192), F32)] + [sds((r, 8192), F32) for r in rows],
        in_specs=[any_spec, vmem, vmem, vmem] + [any_spec] * 5,
        out_specs=[vmem, vmem, vmem, any_spec] + [any_spec] * len(rows),
        scratch_shapes=[
            pltpu.VMEM((4, 256, 256), BF16),
            pltpu.VMEM((8, 8, 256), F32),
            pltpu.VMEM((256, 1024), BF16),
            pltpu.VMEM((1024, 512), BF16),
            pltpu.VMEM((1024, 512), BF16),
            pltpu.VMEM((1024, 4096), BF16),
            pltpu.VMEM((1024, 4096), BF16),
            pltpu.VMEM((256, 8192), F32),
            pltpu.VMEM((256, 512), F32),
            pltpu.VMEM((128, 512), F32),
            pltpu.VMEM((64, 512), F32),
            pltpu.VMEM((32, 512), F32),
            pltpu.VMEM((4, 32, 512), BF16),
            pltpu.VMEM((4, 32, 512), BF16),
            dma((6,)), dma((3,)), dma((3,)), dma((7,)), dma((7,)), dma((3,)), dma((3,)), dma((3,)), dma((3,)), dma((n_late + 1,)),
        ],
        compiler_params=pltpu.CompilerParams(collective_id=0, has_side_effects=True, vmem_limit_bytes=48 * 2**20),
        cost_estimate=pl.CostEstimate(flops=5_000_000_000, bytes_accessed=28 * 2**20, transcendentals=0),
        name="project",
    )(hidden, ln_scale.reshape(1, 256), cos_tab, sin_tab, w_q, w_k, w_v, w_gate, w_up)


def attend_kernel(pos_ref, q_ref, kn_ref, vn_ref, k_hbm, v_hbm, k_out, v_out, o_ref, kbuf, vbuf, k_in, v_in, k_wr, v_wr):
    n_seq, cache_len, head_dim = k_hbm.shape

    def fetch(b):
        slot = lax.rem(b, RING)
        return (pltpu.make_async_copy(k_hbm.at[b], kbuf.at[slot], k_in.at[slot]),
                pltpu.make_async_copy(v_hbm.at[b], vbuf.at[slot], v_in.at[slot]))

    def drain(b):
        slot = lax.rem(b, RING)
        return (pltpu.make_async_copy(kbuf.at[slot], k_out.at[b], k_wr.at[slot]),
                pltpu.make_async_copy(vbuf.at[slot], v_out.at[b], v_wr.at[slot]))

    for b in range(AHEAD):
        for copy in fetch(b):
            copy.start()

    def patch(buf, slot, row, p):
        base = pl.multiple_of((p // 16) * 16, 16)
        tile = buf[slot, pl.ds(base, 16), :]
        hit = lax.broadcasted_iota(jnp.int32, (16, head_dim), 0) == p - base
        buf[slot, pl.ds(base, 16), :] = jnp.where(hit, row, tile.astype(F32)).astype(BF16)

    def one(b, carry):
        slot = lax.rem(b, RING)
        p = pos_ref[b]

        @pl.when(b + AHEAD < n_seq)
        def _():
            @pl.when(b + AHEAD >= RING)
            def _():
                for copy in drain(b + AHEAD - RING):
                    copy.wait()
            for copy in fetch(b + AHEAD):
                copy.start()

        k_copy, v_copy = fetch(b)
        k_save, v_save = drain(b)
        k_copy.wait()
        patch(kbuf, slot, kn_ref[pl.ds(b, 1), :], p)
        k_save.start()
        heads = pl.ds(b, 8, stride=n_seq)
        q = jnp.concatenate([q_ref[0, heads, :], q_ref[1, heads, :]], axis=1).astype(BF16)
        scores = lax.dot_general(q, kbuf[slot], (((1,), (1,)), ((), ())), preferred_element_type=F32) * (head_dim ** -0.5)
        valid = lax.broadcasted_iota(jnp.int32, scores.shape, 1) <= p
        scores = jnp.where(valid, scores, -jnp.inf)
        top = jnp.max(scores, axis=1, keepdims=True)
        e = jnp.exp(scores - top)
        prob = (e / jnp.sum(e, axis=1, keepdims=True)).astype(BF16)
        v_copy.wait()
        patch(vbuf, slot, vn_ref[pl.ds(b, 1), :], p)
        v_save.start()
        out = jnp.dot(prob, vbuf[slot], preferred_element_type=F32)
        o_ref[0, heads, :] = out[:, :128]
        o_ref[1, heads, :] = out[:, 128:]
        return carry

    lax.fori_loop(0, n_seq, one, 0)
    for b in range(n_seq - RING, n_seq):
        for copy in drain(b):
            copy.wait()


def attend(positions, q, kn, vn, k_cache, v_cache):
    any_spec = pl.BlockSpec(memory_space=pl.ANY)
    vmem = pl.BlockSpec(memory_space=pltpu.VMEM)
    n_seq, cache_len, head_dim = k_cache.shape
    dma = pltpu.SemaphoreType.DMA
    return pl.pallas_call(
        attend_kernel,
        out_shape=[jax.ShapeDtypeStruct(k_cache.shape, BF16), jax.ShapeDtypeStruct(v_cache.shape, BF16), jax.ShapeDtypeStruct((2, 256, 128), F32)],
        in_specs=[pl.BlockSpec(memory_space=pltpu.SMEM), vmem, vmem, vmem, any_spec, any_spec],
        out_specs=[any_spec, any_spec, vmem],
        scratch_shapes=[
            pltpu.VMEM((RING, cache_len, head_dim), BF16),
            pltpu.VMEM((RING, cache_len, head_dim), BF16),
            dma((RING,)), dma((RING,)), dma((RING,)), dma((RING,)),
        ],
        compiler_params=pltpu.CompilerParams(vmem_limit_bytes=48 * 2**20),
        cost_estimate=pl.CostEstimate(flops=100_000_000_000, bytes_accessed=128 * 2**20, transcendentals=0),
        name="attend",
    )(positions, q, kn, vn, k_cache, v_cache)


def combine_kernel(rows, h_hbm, attn_ref, wo_hbm, wd_hbm, own_hbm, last_hbm, *rest):
    n = len(rows)
    got_hbm = rest[:n - 1]
    (out_ref, h, wo, wd, own, got, act, a_snd, a_rcv, res, res_rcv,
     load_sem, own_sem, got_sem, l_send, l_recv, t_send, t_recv, g_send, g_recv, r_send, r_recv) = rest[n - 1:]
    px, py = lax.axis_index('tpx'), lax.axis_index('tpy')
    me = px * 4 + py
    starts = [sum(rows[:c]) for c in range(n)]
    loads = [
        pltpu.make_async_copy(wo_hbm, wo, load_sem.at[0]),
        pltpu.make_async_copy(wd_hbm, wd, load_sem.at[1]),
        pltpu.make_async_copy(h_hbm, h, load_sem.at[2]),
    ]
    pieces = []
    for c in range(n):
        seg = pl.ds(starts[c], rows[c])
        mine = pltpu.make_async_copy(own_hbm.at[seg], own.at[seg], own_sem.at[c])
        mine.start()
        theirs = None
        if c < n - 1:
            theirs = pltpu.make_async_copy(got_hbm[c], got.at[seg], got_sem.at[c])
            theirs.start()
        pieces.append((mine, theirs))
    for copy in loads:
        copy.start()
    for t in range(4):
        for j in range(2):
            at = pl.ds((2 * t + j) * 32, 32)
            a_snd[t, j] = jnp.concatenate([attn_ref[0, at, :], attn_ref[1, at, :]], axis=1).astype(BF16)
    enter(px, py)

    last = remote(last_hbm, got.at[pl.ds(starts[-1], rows[-1])], l_send.at[0], l_recv.at[0], 1 - px, py)
    last.start()
    rows_me = pl.ds(pl.multiple_of(me * 32, 32), 32)
    swaps = []
    for i, (qx, qy) in enumerate(others(px, py)):
        copy = remote(a_snd.at[qy], a_rcv.at[:, rows_me, :], t_send.at[i], t_recv.at[i], qx, qy)
        copy.start()
        swaps.append(copy)
    for j in range(2):
        a_rcv[j, rows_me, :] = a_snd[py, j]

    def activate(c):
        seg = pl.ds(starts[c], rows[c])

        def cols(i, carry):
            g_cols = pl.ds(pl.multiple_of(i * 512, 512), 512)
            u_cols = pl.ds(pl.multiple_of(4096 + i * 512, 512), 512)
            gate = (own[seg, g_cols] + got[seg, g_cols]).astype(BF16).astype(F32)
            up = (own[seg, u_cols] + got[seg, u_cols]).astype(BF16).astype(F32)
            act[pl.ds(2 * starts[c], rows[c]), g_cols] = (jax.nn.silu(gate) * up).astype(BF16)
            return carry

        lax.fori_loop(0, 8, cols, 0)
        copy = remote(act.at[pl.ds(2 * starts[c], rows[c])], act.at[pl.ds(2 * starts[c] + rows[c], rows[c])], g_send.at[c], g_recv.at[c], 1 - px, py)
        copy.start()
        return copy

    gathers = []
    for c in range(n - 1):
        for copy in pieces[c]:
            copy.wait()
        gathers.append(activate(c))

    loads[0].wait()
    for copy in swaps:
        copy.wait_recv()
    for c in range(n):
        for side in range(2):
            at = pl.ds(pl.multiple_of(lax.rem(px + side, 2) * 128 + starts[c], 16), rows[c])
            for t in range(4):
                cols = pl.ds(t * 256, 256)
                res[t, pl.ds(2 * starts[c] + side * rows[c], rows[c]), :] = (
                    jnp.dot(a_rcv[0, at, :], wo[pl.ds(0, 256), cols], preferred_element_type=F32)
                    + jnp.dot(a_rcv[1, at, :], wo[pl.ds(256, 256), cols], preferred_element_type=F32))
    pieces[n - 1][0].wait()
    last.wait_recv()
    gathers.append(activate(n - 1))

    loads[1].wait()
    loads[2].wait()
    reduces = []

    def finish(c):
        seg = pl.ds(2 * starts[c], 2 * rows[c])
        total = res[py, seg, :]
        for i in range(3):
            reduces[c][i].wait_recv()
            total = total + res_rcv[lax.rem(py + 4 - 1 - i, 4), seg, :]
        for side in range(2):
            at = pl.ds(pl.multiple_of(lax.rem(px + side, 2) * 128 + starts[c], 16), rows[c])
            out_ref[at, :] = (h[at, :].astype(F32) + total[side * rows[c]:(side + 1) * rows[c]]).astype(BF16)

    for c in range(n):
        seg = pl.ds(2 * starts[c], 2 * rows[c])
        gathers[c].wait_recv()
        hops = []
        for i in range(4):
            t = lax.rem(py + 1 + i, 4)
            cols = pl.ds(pl.multiple_of(t * 256, 256), 256)
            res[t, seg, :] += jnp.dot(act[seg, :], wd[:, cols], preferred_element_type=F32)
            if i < 3:
                copy = remote(res.at[t, seg], res_rcv.at[py, seg], r_send.at[3 * c + i], r_recv.at[3 * c + i], px, t)
                copy.start()
                hops.append(copy)
        reduces.append(hops)
        if c > 0:
            finish(c - 1)
    finish(n - 1)

    for copy in swaps + gathers + [last] + [x for hops in reduces for x in hops]:
        copy.wait_send()


def combine(rows, hidden, attn, w_o, w_down, own, last, got):
    any_spec = pl.BlockSpec(memory_space=pl.ANY)
    vmem = pl.BlockSpec(memory_space=pltpu.VMEM)
    dma = pltpu.SemaphoreType.DMA
    n = len(rows)
    return pl.pallas_call(
        functools.partial(combine_kernel, rows),
        out_shape=jax.ShapeDtypeStruct((256, 256), BF16),
        in_specs=[any_spec, vmem] + [any_spec] * (4 + len(got)),
        out_specs=vmem,
        scratch_shapes=[
            pltpu.VMEM((256, 256), BF16),
            pltpu.VMEM((512, 1024), BF16),
            pltpu.VMEM((4096, 1024), BF16),
            pltpu.VMEM((128, 8192), F32),
            pltpu.VMEM((128, 8192), F32),
            pltpu.VMEM((256, 4096), BF16),
            pltpu.VMEM((4, 2, 32, 256), BF16),
            pltpu.VMEM((2, 256, 256), BF16),
            pltpu.VMEM((4, 256, 256), F32),
            pltpu.VMEM((4, 256, 256), F32),
            dma((3,)), dma((n,)), dma((n,)), dma((1,)), dma((1,)), dma((7,)), dma((7,)), dma((n,)), dma((n,)), dma((3 * n,)), dma((3 * n,)),
        ],
        compiler_params=pltpu.CompilerParams(collective_id=1, has_side_effects=True, vmem_limit_bytes=48 * 2**20),
        cost_estimate=pl.CostEstimate(flops=3_000_000_000, bytes_accessed=18 * 2**20, transcendentals=0),
        name="combine",
    )(hidden, attn, w_o, w_down, own, last, *got)


def solution(mesh):
    hidden_spec = P('dp', ('tpx', 'tpy'))
    cache_spec = P(('dp', 'tpx', 'tpy'), None, None)
    in_specs = (hidden_spec, P(('tpx', 'tpy')), P('tpx', 'tpy'), P('tpx', None), P('tpx', None), P('tpx', 'tpy'), P('tpx', 'tpy'), P('tpy', 'tpx'), P('tpy', 'tpx'), cache_spec, cache_spec, P(('dp', 'tpx', 'tpy')))
    out_specs = (hidden_spec, cache_spec, cache_spec)
    rows = (32, 32, 32, 32)
    swap = [(0, 1), (1, 0)]

    def device_step(hidden, ln_scale, w_q, w_k, w_v, w_gate, w_up, w_o, w_down, k_cache, v_cache, positions):
        cos_tab, sin_tab = rope_tables(positions, k_cache.shape[2])
        q, kn, vn, own, first, *late = project(rows, hidden, ln_scale, cos_tab, sin_tab, w_q, w_k, w_v, w_gate, w_up)
        got = [first] + [lax.ppermute(x, 'tpx', swap) for x in late[:-1]]
        k_all, v_all, attn = attend(positions, q, kn, vn, k_cache, v_cache)
        hidden_out = combine(rows, hidden, attn, w_o, w_down, own, late[-1], got)
        return hidden_out, k_all, v_all

    return jax.shard_map(device_step, mesh=mesh, in_specs=in_specs, out_specs=out_specs, check_vma=False)
```

```python
import functools
import jax
import jax.numpy as jnp
from jax import lax
from jax.experimental import pallas as pl
from jax.experimental.pallas import tpu as pltpu
from jax.sharding import PartitionSpec as P

LN_EPS = 1e-6
ROPE_BASE = 10000.0
MESH = pl.DeviceIdType.MESH
F32 = jnp.float32
BF16 = jnp.bfloat16
RING = 8
AHEAD = 4


def rope_tables(positions, head_dim):
    half_dim = head_dim // 2
    inv_freq = ROPE_BASE ** (-(jnp.arange(half_dim, dtype=F32) * 2.0 / head_dim))
    angles = positions.astype(F32)[:, None] * inv_freq[None, :]
    return jnp.cos(angles), jnp.sin(angles)


def rotate(x, cos_tab, sin_tab):
    half = x.shape[-1] // 2
    lead, tail = x[:, :half], x[:, half:]
    return jnp.concatenate([lead * cos_tab - tail * sin_tab, lead * sin_tab + tail * cos_tab], axis=-1)


def others(px, py):
    return [(lax.rem(px + dx, 2), lax.rem(py + dy, 4)) for dx in range(2) for dy in range(4) if (dx, dy) != (0, 0)]


def greet(px, py):
    barrier = pltpu.get_barrier_semaphore()
    for qx, qy in others(px, py):
        pl.semaphore_signal(barrier, 1, device_id={'tpx': qx, 'tpy': qy}, device_id_type=MESH)


def met():
    pl.semaphore_wait(pltpu.get_barrier_semaphore(), 7)


def remote(src, dst, send_sem, recv_sem, qx, qy):
    return pltpu.make_async_remote_copy(src, dst, send_sem, recv_sem, device_id={'tpx': qx, 'tpy': qy}, device_id_type=MESH)


def project_kernel(split, h_hbm, scale_hbm, wq_hbm, wk_hbm, wv_hbm, wg_hbm, wu_hbm,
                   q_out, kn_out, vn_out, own_out, first_out, mid_out, last_out,
                   hbuf, scale, msg, u, wq, wkv, wg, wu, part, qpart, qrec, kvpart, kvrec, qsum, qall,
                   load_sem, h_send, h_recv, m_send, m_recv, x_send, x_recv, f_send, f_recv, a_send, a_recv, o_sem):
    px, py = lax.axis_index('tpx'), lax.axis_index('tpy')
    me = px * 4 + py
    mate = py + 1 - 2 * lax.rem(py, 2)
    across = lax.rem(py + 2, 4)
    n_seq = 32

    loads = [
        pltpu.make_async_copy(h_hbm, hbuf.at[py], load_sem.at[0]),
        pltpu.make_async_copy(scale_hbm, scale, load_sem.at[1]),
        pltpu.make_async_copy(wq_hbm, wq, load_sem.at[2]),
        pltpu.make_async_copy(wk_hbm, wkv.at[:, pl.ds(0, 256)], load_sem.at[3]),
        pltpu.make_async_copy(wv_hbm, wkv.at[:, pl.ds(256, 256)], load_sem.at[4]),
        pltpu.make_async_copy(wg_hbm, wg, load_sem.at[5]),
        pltpu.make_async_copy(wu_hbm, wu, load_sem.at[6]),
    ]
    for copy in loads[:2]:
        copy.start()
    greet(px, py)
    for copy in loads[2:]:
        copy.start()
    loads[0].wait()
    met()
    sends = [
        remote(hbuf.at[py], hbuf.at[py], h_send.at[0], h_recv.at[0], px, across),
        remote(hbuf.at[py], hbuf.at[py], h_send.at[1], h_recv.at[1], px, mate),
    ]
    for copy in sends:
        copy.start()

    hf = hbuf[py].astype(F32)
    mean = jnp.sum(hf, axis=1, keepdims=True) * (1.0 / 256.0)
    dev = hf - mean
    m2 = jnp.sum(dev * dev, axis=1, keepdims=True)
    lane = lax.broadcasted_iota(jnp.int32, (256, 128), 1)
    stat = jnp.where(lane == 0, mean, m2)
    stat_t = stat.T
    loads[1].wait()
    msg[me] = jnp.concatenate([stat_t[0:2], scale[...], jnp.zeros((5, 256), F32)], axis=0)
    msgs = []
    for i, (qx, qy) in enumerate(others(px, py)):
        copy = remote(msg.at[me], msg.at[me], m_send.at[i], m_recv.at[i], qx, qy)
        copy.start()
        msgs.append(copy)
    for copy in msgs:
        copy.wait_recv()

    means = jnp.concatenate([msg[e, 0:1] for e in range(8)], axis=0)
    m2s = jnp.concatenate([msg[e, 1:2] for e in range(8)], axis=0)
    mu = jnp.sum(means, axis=0, keepdims=True) * 0.125
    gap = means - mu
    var = (jnp.sum(m2s, axis=0, keepdims=True) + 256.0 * jnp.sum(gap * gap, axis=0, keepdims=True)) * (1.0 / 2048.0)
    rstd = lax.rsqrt(var + LN_EPS)
    both = jnp.concatenate([mu, rstd, jnp.zeros((126, 256), F32)], axis=0).T
    mu_col, rstd_col = both[:, 0:1], both[:, 1:2]

    def norm(t):
        cols = pl.ds(pl.multiple_of(t * 256, 256), 256)
        u[:, cols] = ((hbuf[t].astype(F32) - mu_col) * rstd_col * msg[px * 4 + t, 2:3]).astype(BF16)

    norm(py)
    sends[1].wait_recv()
    norm(mate)
    sends[0].wait_recv()
    relay = remote(hbuf.at[across], hbuf.at[across], h_send.at[2], h_recv.at[2], px, mate)
    relay.start()
    sends.append(relay)
    norm(across)
    relay.wait_recv()
    norm(lax.rem(mate + 2, 4))

    loads[2].wait()
    far = pl.ds(pl.multiple_of((1 - px) * 128, 128), 128)
    near = pl.ds(pl.multiple_of(px * 128, 128), 128)
    qpart[far, :] = jnp.dot(u[far, :], wq[...], preferred_element_type=F32)
    q_copy = remote(qpart.at[far], qrec, x_send.at[0], x_recv.at[0], 1 - px, py)
    q_copy.start()
    loads[3].wait()
    loads[4].wait()
    far_seq = pl.ds(pl.multiple_of((1 - px) * 128 + py * n_seq, n_seq), n_seq)
    near_seq = pl.ds(pl.multiple_of(px * 128 + py * n_seq, n_seq), n_seq)
    u_kv = jnp.concatenate([u[far_seq, :], u[near_seq, :]], axis=0)
    kvpart[...] = jnp.dot(u_kv, wkv[...], preferred_element_type=F32)
    kv_copy = remote(kvpart.at[pl.ds(0, n_seq)], kvrec, x_send.at[1], x_recv.at[1], 1 - px, py)
    kv_copy.start()

    loads[5].wait()
    loads[6].wait()
    step = 512
    n_step = 4096 // step
    n_first, n_mid, n_last = split
    first_rows = pl.ds(pl.multiple_of((1 - px) * 128, 8), n_first)
    mid_rows = pl.ds(pl.multiple_of((1 - px) * 128 + n_first, 8), n_mid)
    last_rows = pl.ds(pl.multiple_of((1 - px) * 128 + n_first + n_mid, 8), n_last)

    def first_copy(i, base):
        cols = pl.ds(pl.multiple_of(base * 4096 + i * step, step), step)
        at = base * n_step + i
        return remote(part.at[first_rows, cols], first_out.at[:, cols], f_send.at[at], f_recv.at[at], 1 - px, py)

    def columns(i, carry):
        cols = pl.ds(pl.multiple_of(i * step, step), step)
        part[:, cols] = jnp.dot(u[...], wg[:, cols], preferred_element_type=F32)
        first_copy(i, 0).start()
        up_cols = pl.ds(pl.multiple_of(4096 + i * step, step), step)
        part[:, up_cols] = jnp.dot(u[...], wu[:, cols], preferred_element_type=F32)
        first_copy(i, 1).start()
        return carry

    lax.fori_loop(0, n_step, columns, 0)
    outs = [
        pltpu.make_async_copy(part.at[near], own_out, o_sem.at[0]),
        pltpu.make_async_copy(part.at[mid_rows], mid_out, o_sem.at[1]),
        pltpu.make_async_copy(part.at[last_rows], last_out, o_sem.at[2]),
    ]
    for copy in outs:
        copy.start()
    qpart[near, :] = jnp.dot(u[near, :], wq[...], preferred_element_type=F32)

    q_copy.wait_recv()
    for t in range(4):
        rows_t = pl.ds(pl.multiple_of(px * 128 + t * n_seq, n_seq), n_seq)
        qsum[t] = (qpart[rows_t, :] + qrec[pl.ds(t * n_seq, n_seq), :]).astype(BF16)
    hops = []
    for i in range(1, 4):
        t = lax.rem(py + i, 4)
        copy = remote(qsum.at[t], qall.at[py], a_send.at[i - 1], a_recv.at[i - 1], px, t)
        copy.start()
        hops.append(copy)
    kv_copy.wait_recv()
    kv = (kvpart[pl.ds(n_seq, n_seq), :] + kvrec[...]).astype(BF16).astype(F32)
    kn_out[...] = kv[:, :256]
    vn_out[...] = kv[:, 256:]

    def emit(t, block):
        block = block.astype(F32)
        for j in range(2):
            row = pl.multiple_of((2 * t + j) * n_seq, n_seq)
            for half in range(2):
                q_out[half, pl.ds(row, n_seq), :] = block[:, (2 * j + half) * 128:(2 * j + half + 1) * 128]

    emit(py, qsum[py])
    for i in range(1, 4):
        hops[i - 1].wait_recv()
        t = lax.rem(py + 4 - i, 4)
        emit(t, qall[t])

    for copy in outs:
        copy.wait()
    for copy in sends + msgs + hops + [q_copy, kv_copy]:
        copy.wait_send()

    def settle(i, carry):
        first_copy(i, 0).wait()
        first_copy(i, 1).wait()
        return carry

    lax.fori_loop(0, n_step, settle, 0)


def project(split, hidden, ln_scale, w_q, w_k, w_v, w_gate, w_up):
    any_spec = pl.BlockSpec(memory_space=pl.ANY)
    hbm = pl.BlockSpec(memory_space=pltpu.HBM)
    vmem = pl.BlockSpec(memory_space=pltpu.VMEM)
    sds = jax.ShapeDtypeStruct
    dma = pltpu.SemaphoreType.DMA
    return pl.pallas_call(
        functools.partial(project_kernel, split),
        out_shape=[sds((2, 256, 128), F32), sds((32, 256), F32), sds((32, 256), F32), sds((128, 8192), F32)] + [sds((r, 8192), F32) for r in split],
        in_specs=[hbm] * 7,
        out_specs=[vmem, vmem, vmem] + [any_spec] * 4,
        scratch_shapes=[
            pltpu.VMEM((4, 256, 256), BF16),
            pltpu.VMEM((1, 256), F32),
            pltpu.VMEM((8, 8, 256), F32),
            pltpu.VMEM((256, 1024), BF16),
            pltpu.VMEM((1024, 512), BF16),
            pltpu.VMEM((1024, 512), BF16),
            pltpu.VMEM((1024, 4096), BF16),
            pltpu.VMEM((1024, 4096), BF16),
            pltpu.VMEM((256, 8192), F32),
            pltpu.VMEM((256, 512), F32),
            pltpu.VMEM((128, 512), F32),
            pltpu.VMEM((64, 512), F32),
            pltpu.VMEM((32, 512), F32),
            pltpu.VMEM((4, 32, 512), BF16),
            pltpu.VMEM((4, 32, 512), BF16),
            dma((7,)), dma((3,)), dma((3,)), dma((7,)), dma((7,)), dma((2,)), dma((2,)), dma((16,)), dma((16,)), dma((3,)), dma((3,)), dma((3,)),
        ],
        compiler_params=pltpu.CompilerParams(collective_id=0, has_side_effects=True, vmem_limit_bytes=48 * 2**20),
        cost_estimate=pl.CostEstimate(flops=5_000_000_000, bytes_accessed=28 * 2**20, transcendentals=0),
        name="project",
    )(*[pltpu.with_memory_space_constraint(x, pltpu.HBM) for x in (hidden, ln_scale.reshape(1, 256), w_q, w_k, w_v, w_gate, w_up)])


def attend_kernel(pos_ref, q_in, kn_in, vn_ref, cos_ref, sin_ref, k_hbm, v_hbm, k_out, v_out, o_ref, kbuf, vbuf, q_ref, kn_ref, k_in, v_in, k_wr, v_wr):
    n_seq, cache_len, head_dim = k_hbm.shape

    def fetch(b):
        slot = lax.rem(b, RING)
        return (pltpu.make_async_copy(k_hbm.at[b], kbuf.at[slot], k_in.at[slot]),
                pltpu.make_async_copy(v_hbm.at[b], vbuf.at[slot], v_in.at[slot]))

    def drain(b):
        slot = lax.rem(b, RING)
        return (pltpu.make_async_copy(kbuf.at[slot], k_out.at[b], k_wr.at[slot]),
                pltpu.make_async_copy(vbuf.at[slot], v_out.at[b], v_wr.at[slot]))

    for b in range(AHEAD):
        for copy in fetch(b):
            copy.start()

    cos_tab, sin_tab = cos_ref[...], sin_ref[...]
    kn_ref[...] = rotate(kn_in[...], cos_tab, sin_tab).astype(BF16).astype(F32)
    for h in range(8):
        rows = pl.ds(h * n_seq, n_seq)
        lead, tail = q_in[0, rows, :], q_in[1, rows, :]
        q_ref[0, rows, :] = (lead * cos_tab - tail * sin_tab).astype(BF16).astype(F32)
        q_ref[1, rows, :] = (lead * sin_tab + tail * cos_tab).astype(BF16).astype(F32)

    def patch(buf, slot, row, p):
        base = pl.multiple_of((p // 16) * 16, 16)
        tile = buf[slot, pl.ds(base, 16), :]
        hit = lax.broadcasted_iota(jnp.int32, (16, head_dim), 0) == p - base
        buf[slot, pl.ds(base, 16), :] = jnp.where(hit, row, tile.astype(F32)).astype(BF16)

    def one(b, carry):
        slot = lax.rem(b, RING)
        p = pos_ref[b]

        @pl.when(b + AHEAD < n_seq)
        def _():
            @pl.when(b + AHEAD >= RING)
            def _():
                for copy in drain(b + AHEAD - RING):
                    copy.wait()
            for copy in fetch(b + AHEAD):
                copy.start()

        k_copy, v_copy = fetch(b)
        k_save, v_save = drain(b)
        k_copy.wait()
        patch(kbuf, slot, kn_ref[pl.ds(b, 1), :], p)
        k_save.start()
        heads = pl.ds(b, 8, stride=n_seq)
        q = jnp.concatenate([q_ref[0, heads, :], q_ref[1, heads, :]], axis=1).astype(BF16)
        scores = lax.dot_general(q, kbuf[slot], (((1,), (1,)), ((), ())), preferred_element_type=F32) * (head_dim ** -0.5)
        valid = lax.broadcasted_iota(jnp.int32, scores.shape, 1) <= p
        scores = jnp.where(valid, scores, -jnp.inf)
        top = jnp.max(scores, axis=1, keepdims=True)
        e = jnp.exp(scores - top)
        prob = (e / jnp.sum(e, axis=1, keepdims=True)).astype(BF16)
        v_copy.wait()
        patch(vbuf, slot, vn_ref[pl.ds(b, 1), :], p)
        v_save.start()
        out = jnp.dot(prob, vbuf[slot], preferred_element_type=F32)
        o_ref[0, heads, :] = out[:, :128]
        o_ref[1, heads, :] = out[:, 128:]
        return carry

    lax.fori_loop(0, n_seq, one, 0)
    for b in range(n_seq - RING, n_seq):
        for copy in drain(b):
            copy.wait()


def attend(positions, q, kn, vn, cos_tab, sin_tab, k_cache, v_cache):
    any_spec = pl.BlockSpec(memory_space=pl.ANY)
    vmem = pl.BlockSpec(memory_space=pltpu.VMEM)
    n_seq, cache_len, head_dim = k_cache.shape
    dma = pltpu.SemaphoreType.DMA
    return pl.pallas_call(
        attend_kernel,
        out_shape=[jax.ShapeDtypeStruct(k_cache.shape, BF16), jax.ShapeDtypeStruct(v_cache.shape, BF16), jax.ShapeDtypeStruct((2, 256, 128), F32)],
        in_specs=[pl.BlockSpec(memory_space=pltpu.SMEM), vmem, vmem, vmem, vmem, vmem, any_spec, any_spec],
        out_specs=[any_spec, any_spec, vmem],
        scratch_shapes=[
            pltpu.VMEM((RING, cache_len, head_dim), BF16),
            pltpu.VMEM((RING, cache_len, head_dim), BF16),
            pltpu.VMEM((2, 256, 128), F32),
            pltpu.VMEM((n_seq, head_dim), F32),
            dma((RING,)), dma((RING,)), dma((RING,)), dma((RING,)),
        ],
        compiler_params=pltpu.CompilerParams(vmem_limit_bytes=48 * 2**20),
        cost_estimate=pl.CostEstimate(flops=100_000_000_000, bytes_accessed=128 * 2**20, transcendentals=0),
        name="attend",
    )(positions, q, kn, vn, cos_tab, sin_tab, k_cache, v_cache)


def combine_kernel(split, cuts, h_hbm, attn_ref, wo_hbm, wd_hbm, own_hbm, first_ref, mid_ref, last_ref,
                   out_ref, h, wo, wd, own, got, act, a_snd, a_rcv, res, res_rcv,
                   load_sem, l_send, l_recv, t_send, t_recv, g_send, g_recv, r_send, r_recv):
    px, py = lax.axis_index('tpx'), lax.axis_index('tpy')
    me = px * 4 + py
    n = len(cuts)
    starts = [sum(cuts[:c]) for c in range(n)]
    n_first, n_mid, n_last = split
    late = n_first + n_mid
    greet(px, py)
    loads = [
        pltpu.make_async_copy(own_hbm, own, load_sem.at[0]),
        pltpu.make_async_copy(wo_hbm, wo, load_sem.at[1]),
        pltpu.make_async_copy(wd_hbm, wd, load_sem.at[2]),
        pltpu.make_async_copy(h_hbm, h, load_sem.at[3]),
    ]
    for copy in loads:
        copy.start()
    for t in range(4):
        for j in range(2):
            at = pl.ds((2 * t + j) * 32, 32)
            a_snd[t, j] = jnp.concatenate([attn_ref[0, at, :], attn_ref[1, at, :]], axis=1).astype(BF16)
    met()

    lasts = {}
    for c in range(n):
        if starts[c] >= late:
            seg = pl.ds(starts[c] - late, cuts[c])
            lasts[c] = remote(last_ref.at[seg], got.at[seg], l_send.at[c], l_recv.at[c], 1 - px, py)
            lasts[c].start()
    rows_me = pl.ds(pl.multiple_of(me * 32, 32), 32)
    swaps = []
    for i, (qx, qy) in enumerate(others(px, py)):
        copy = remote(a_snd.at[qy], a_rcv.at[:, rows_me, :], t_send.at[i], t_recv.at[i], qx, qy)
        copy.start()
        swaps.append(copy)
    for j in range(2):
        a_rcv[j, rows_me, :] = a_snd[py, j]

    def activate(c):
        here = pl.ds(starts[c], cuts[c])
        if starts[c] < n_first:
            theirs, there = first_ref, here
        elif starts[c] < late:
            theirs, there = mid_ref, pl.ds(starts[c] - n_first, cuts[c])
        else:
            theirs, there = got, pl.ds(starts[c] - late, cuts[c])

        def piece(k):
            cols = pl.ds(pl.multiple_of(k * 1024, 1024), 1024)
            return remote(act.at[pl.ds(2 * starts[c], cuts[c]), cols], act.at[pl.ds(2 * starts[c] + cuts[c], cuts[c]), cols],
                          g_send.at[4 * c + k], g_recv.at[4 * c + k], 1 - px, py)

        def cols(k, carry):
            for i in range(2):
                g_cols = pl.ds(pl.multiple_of(k * 1024 + i * 512, 512), 512)
                u_cols = pl.ds(pl.multiple_of(4096 + k * 1024 + i * 512, 512), 512)
                gate = (own[here, g_cols] + theirs[there, g_cols]).astype(BF16).astype(F32)
                up = (own[here, u_cols] + theirs[there, u_cols]).astype(BF16).astype(F32)
                act[pl.ds(2 * starts[c], cuts[c]), g_cols] = (jax.nn.silu(gate) * up).astype(BF16)
            piece(k).start()
            return carry

        lax.fori_loop(0, 4, cols, 0)
        return piece

    loads[0].wait()
    gathers = [activate(c) for c in range(n) if starts[c] < late]

    loads[1].wait()
    for copy in swaps:
        copy.wait_recv()
    for c in range(n):
        for side in range(2):
            at = pl.ds(pl.multiple_of(lax.rem(px + side, 2) * 128 + starts[c], 16), cuts[c])
            for t in range(4):
                cols = pl.ds(t * 256, 256)
                res[t, pl.ds(2 * starts[c] + side * cuts[c], cuts[c]), :] = (
                    jnp.dot(a_rcv[0, at, :], wo[pl.ds(0, 256), cols], preferred_element_type=F32)
                    + jnp.dot(a_rcv[1, at, :], wo[pl.ds(256, 256), cols], preferred_element_type=F32))
    for c in lasts:
        lasts[c].wait_recv()
        gathers.append(activate(c))

    loads[2].wait()
    loads[3].wait()
    reduces = []

    def finish(c):
        seg = pl.ds(2 * starts[c], 2 * cuts[c])
        total = res[py, seg, :]
        for i in range(3):
            reduces[c][i].wait_recv()
            total = total + res_rcv[lax.rem(py + 4 - 1 - i, 4), seg, :]
        for side in range(2):
            at = pl.ds(pl.multiple_of(lax.rem(px + side, 2) * 128 + starts[c], 16), cuts[c])
            out_ref[at, :] = (h[at, :].astype(F32) + total[side * cuts[c]:(side + 1) * cuts[c]]).astype(BF16)

    for c in range(n):
        seg = pl.ds(2 * starts[c], 2 * cuts[c])
        hops = []
        parts = 4 if c == n - 1 else 1
        depth = 4096 // parts
        for p in range(parts):
            for k in range(p * 4 // parts, (p + 1) * 4 // parts):
                gathers[c](k).wait_recv()
            deep = pl.ds(p * depth, depth)
            for i in range(4):
                t = lax.rem(py + 1 + i, 4)
                cols = pl.ds(pl.multiple_of(t * 256, 256), 256)
                res[t, seg, :] += jnp.dot(act[seg, deep], wd[deep, cols], preferred_element_type=F32)
                if p == parts - 1 and i < 3:
                    copy = remote(res.at[t, seg], res_rcv.at[py, seg], r_send.at[3 * c + i], r_recv.at[3 * c + i], px, t)
                    copy.start()
                    hops.append(copy)
        reduces.append(hops)
        if c > 0:
            finish(c - 1)
    finish(n - 1)

    for copy in swaps + list(lasts.values()) + [x for hops in reduces for x in hops]:
        copy.wait_send()
    for c in range(n):
        for k in range(4):
            gathers[c](k).wait_send()


def combine(split, cuts, hidden, attn, w_o, w_down, own, first, mid, last):
    any_spec = pl.BlockSpec(memory_space=pl.ANY)
    hbm = pl.BlockSpec(memory_space=pltpu.HBM)
    vmem = pl.BlockSpec(memory_space=pltpu.VMEM)
    dma = pltpu.SemaphoreType.DMA
    n = len(cuts)
    return pl.pallas_call(
        functools.partial(combine_kernel, split, cuts),
        out_shape=jax.ShapeDtypeStruct((256, 256), BF16),
        in_specs=[hbm, vmem, hbm, hbm, any_spec, vmem, vmem, vmem],
        out_specs=vmem,
        scratch_shapes=[
            pltpu.VMEM((256, 256), BF16),
            pltpu.VMEM((512, 1024), BF16),
            pltpu.VMEM((4096, 1024), BF16),
            pltpu.VMEM((128, 8192), F32),
            pltpu.VMEM((split[2], 8192), F32),
            pltpu.VMEM((256, 4096), BF16),
            pltpu.VMEM((4, 2, 32, 256), BF16),
            pltpu.VMEM((2, 256, 256), BF16),
            pltpu.VMEM((4, 256, 256), F32),
            pltpu.VMEM((4, 256, 256), F32),
            dma((4,)), dma((n,)), dma((n,)), dma((7,)), dma((7,)), dma((4 * n,)), dma((4 * n,)), dma((3 * n,)), dma((3 * n,)),
        ],
        compiler_params=pltpu.CompilerParams(collective_id=1, has_side_effects=True, vmem_limit_bytes=48 * 2**20),
        cost_estimate=pl.CostEstimate(flops=3_000_000_000, bytes_accessed=18 * 2**20, transcendentals=0),
        name="combine",
    )(hidden, attn, w_o, w_down, own, first, mid, last)


def solution(mesh):
    hidden_spec = P('dp', ('tpx', 'tpy'))
    cache_spec = P(('dp', 'tpx', 'tpy'), None, None)
    in_specs = (hidden_spec, P(('tpx', 'tpy')), P('tpx', 'tpy'), P('tpx', None), P('tpx', None), P('tpx', 'tpy'), P('tpx', 'tpy'), P('tpy', 'tpx'), P('tpy', 'tpx'), cache_spec, cache_spec, P(('dp', 'tpx', 'tpy')))
    out_specs = (hidden_spec, cache_spec, cache_spec)
    split, cuts = (32, 64, 32), (32, 32, 32, 16, 16)
    swap = [(0, 1), (1, 0)]

    def device_step(hidden, ln_scale, w_q, w_k, w_v, w_gate, w_up, w_o, w_down, k_cache, v_cache, positions):
        q, kn, vn, own, first, mid, last = project(split, hidden, ln_scale, w_q, w_k, w_v, w_gate, w_up)
        mid = lax.ppermute(mid, 'tpx', swap)
        late_pos, kn = lax.optimization_barrier((positions, kn))
        cos_tab, sin_tab = rope_tables(late_pos, k_cache.shape[2])
        k_all, v_all, attn = attend(positions, q, kn, vn, cos_tab, sin_tab, k_cache, v_cache)
        hidden_out = combine(split, cuts, hidden, attn, w_o, w_down, own, first, mid, last)
        return hidden_out, k_all, v_all

    return jax.shard_map(device_step, mesh=mesh, in_specs=in_specs, out_specs=out_specs, check_vma=False)
```

```python
import functools
import jax
import jax.numpy as jnp
from jax import lax
from jax.experimental import pallas as pl
from jax.experimental.pallas import tpu as pltpu
from jax.sharding import PartitionSpec as P

LN_EPS = 1e-6
ROPE_BASE = 10000.0
MESH = pl.DeviceIdType.MESH
F32 = jnp.float32
BF16 = jnp.bfloat16
RING = 8
AHEAD = 4


def rope_tables(positions, head_dim):
    half_dim = head_dim // 2
    inv_freq = ROPE_BASE ** (-(jnp.arange(half_dim, dtype=F32) * 2.0 / head_dim))
    angles = positions.astype(F32)[:, None] * inv_freq[None, :]
    return jnp.cos(angles), jnp.sin(angles)


def rotate(x, cos_tab, sin_tab):
    half = x.shape[-1] // 2
    lead, tail = x[:, :half], x[:, half:]
    return jnp.concatenate([lead * cos_tab - tail * sin_tab, lead * sin_tab + tail * cos_tab], axis=-1)


def others(px, py):
    return [(lax.rem(px + dx, 2), lax.rem(py + dy, 4)) for dx in range(2) for dy in range(4) if (dx, dy) != (0, 0)]


def greet(px, py):
    barrier = pltpu.get_barrier_semaphore()
    for qx, qy in others(px, py):
        pl.semaphore_signal(barrier, 1, device_id={'tpx': qx, 'tpy': qy}, device_id_type=MESH)


def met():
    pl.semaphore_wait(pltpu.get_barrier_semaphore(), 7)


def remote(src, dst, send_sem, recv_sem, qx, qy):
    return pltpu.make_async_remote_copy(src, dst, send_sem, recv_sem, device_id={'tpx': qx, 'tpy': qy}, device_id_type=MESH)


def project_kernel(split, h_hbm, scale_hbm, wq_hbm, wk_hbm, wv_hbm, wg_hbm, wu_hbm,
                   q_out, kn_out, vn_out, own_out, first_out, mid_out, last_out,
                   hbuf, scale, msg, stats_col, u, wq, wkv, wg, wu, part, qpart, qrec, kvpart, kvrec, qsum, qall,
                   load_sem, h_send, h_recv, m_send, m_recv, x_send, x_recv, f_send, f_recv, a_send, a_recv, o_sem):
    px, py = lax.axis_index('tpx'), lax.axis_index('tpy')
    me = px * 4 + py
    mate = py + 1 - 2 * lax.rem(py, 2)
    across = lax.rem(py + 2, 4)
    n_seq = 32

    loads = [
        pltpu.make_async_copy(h_hbm, hbuf.at[py], load_sem.at[0]),
        pltpu.make_async_copy(scale_hbm, scale, load_sem.at[1]),
        pltpu.make_async_copy(wq_hbm, wq, load_sem.at[2]),
        pltpu.make_async_copy(wk_hbm, wkv.at[:, pl.ds(0, 256)], load_sem.at[3]),
        pltpu.make_async_copy(wv_hbm, wkv.at[:, pl.ds(256, 256)], load_sem.at[4]),
        pltpu.make_async_copy(wg_hbm, wg, load_sem.at[5]),
        pltpu.make_async_copy(wu_hbm, wu, load_sem.at[6]),
    ]
    for copy in loads[:2]:
        copy.start()
    greet(px, py)
    for copy in loads[2:]:
        copy.start()
    loads[0].wait()
    met()
    far = pl.ds(pl.multiple_of((1 - px) * 128, 128), 128)
    near = pl.ds(pl.multiple_of(px * 128, 128), 128)

    def h_copy(block, rows, at, qy):
        return remote(hbuf.at[block, rows], hbuf.at[block, rows], h_send.at[at], h_recv.at[at], px, qy)

    to_across = [h_copy(py, far, 0, across), h_copy(py, near, 1, across)]
    to_mate = [h_copy(py, far, 2, mate), h_copy(py, near, 3, mate)]
    relays = [h_copy(across, far, 4, mate), h_copy(across, near, 5, mate)]
    to_across[0].start()
    to_mate[0].start()

    hf = hbuf[py].astype(F32)
    mean = jnp.sum(hf, axis=1, keepdims=True) * (1.0 / 256.0)
    dev = hf - mean
    m2 = jnp.sum(dev * dev, axis=1, keepdims=True)
    lane = lax.broadcasted_iota(jnp.int32, (256, 128), 1)
    stat = jnp.where(lane == 0, mean, m2)
    stat_t = stat.T
    loads[1].wait()
    msg[me] = jnp.concatenate([stat_t[0:2], scale[...], jnp.zeros((5, 256), F32)], axis=0)
    msgs = []
    for i, (qx, qy) in enumerate(others(px, py)):
        copy = remote(msg.at[me], msg.at[me], m_send.at[i], m_recv.at[i], qx, qy)
        copy.start()
        msgs.append(copy)
    to_across[1].start()
    to_mate[1].start()
    for copy in msgs:
        copy.wait_recv()

    means = jnp.concatenate([msg[e, 0:1] for e in range(8)], axis=0)
    m2s = jnp.concatenate([msg[e, 1:2] for e in range(8)], axis=0)
    mu = jnp.sum(means, axis=0, keepdims=True) * 0.125
    gap = means - mu
    var = (jnp.sum(m2s, axis=0, keepdims=True) + 256.0 * jnp.sum(gap * gap, axis=0, keepdims=True)) * (1.0 / 2048.0)
    rstd = lax.rsqrt(var + LN_EPS)
    both = jnp.concatenate([mu, rstd, jnp.zeros((126, 256), F32)], axis=0).T
    stats_col[...] = both

    def norm(t, rows):
        cols = pl.ds(pl.multiple_of(t * 256, 256), 256)
        table = stats_col[rows, :]
        u[rows, cols] = ((hbuf[t, rows, :].astype(F32) - table[:, 0:1]) * table[:, 1:2] * msg[px * 4 + t, 2:3]).astype(BF16)

    def gather(i, rows):
        norm(py, rows)
        to_mate[i].wait_recv()
        norm(mate, rows)
        to_across[i].wait_recv()
        relays[i].start()
        norm(across, rows)
        relays[i].wait_recv()
        norm(lax.rem(mate + 2, 4), rows)

    gather(0, far)
    loads[2].wait()
    qpart[far, :] = jnp.dot(u[far, :], wq[...], preferred_element_type=F32)
    q_copy = remote(qpart.at[far], qrec, x_send.at[0], x_recv.at[0], 1 - px, py)
    q_copy.start()
    loads[3].wait()
    loads[4].wait()
    far_seq = pl.ds(pl.multiple_of((1 - px) * 128 + py * n_seq, n_seq), n_seq)
    near_seq = pl.ds(pl.multiple_of(px * 128 + py * n_seq, n_seq), n_seq)
    kvpart[pl.ds(0, n_seq), :] = jnp.dot(u[far_seq, :], wkv[...], preferred_element_type=F32)
    kv_copy = remote(kvpart.at[pl.ds(0, n_seq)], kvrec, x_send.at[1], x_recv.at[1], 1 - px, py)
    kv_copy.start()
    gather(1, near)

    loads[5].wait()
    loads[6].wait()
    step = 512
    n_step = 4096 // step
    n_first, n_mid, n_last = split
    first_rows = pl.ds(pl.multiple_of((1 - px) * 128, 8), n_first)
    mid_rows = pl.ds(pl.multiple_of((1 - px) * 128 + n_first, 8), n_mid)
    last_rows = pl.ds(pl.multiple_of((1 - px) * 128 + n_first + n_mid, 8), n_last)

    def first_copy(i, base):
        cols = pl.ds(pl.multiple_of(base * 4096 + i * step, step), step)
        at = base * n_step + i
        return remote(part.at[first_rows, cols], first_out.at[:, cols], f_send.at[at], f_recv.at[at], 1 - px, py)

    def columns(i, carry):
        cols = pl.ds(pl.multiple_of(i * step, step), step)
        part[:, cols] = jnp.dot(u[...], wg[:, cols], preferred_element_type=F32)
        first_copy(i, 0).start()
        up_cols = pl.ds(pl.multiple_of(4096 + i * step, step), step)
        part[:, up_cols] = jnp.dot(u[...], wu[:, cols], preferred_element_type=F32)
        first_copy(i, 1).start()
        return carry

    lax.fori_loop(0, n_step, columns, 0)
    outs = [
        pltpu.make_async_copy(part.at[near], own_out, o_sem.at[0]),
        pltpu.make_async_copy(part.at[mid_rows], mid_out, o_sem.at[1]),
        pltpu.make_async_copy(part.at[last_rows], last_out, o_sem.at[2]),
    ]
    for copy in outs:
        copy.start()
    qpart[near, :] = jnp.dot(u[near, :], wq[...], preferred_element_type=F32)
    kvpart[pl.ds(n_seq, n_seq), :] = jnp.dot(u[near_seq, :], wkv[...], preferred_element_type=F32)

    q_copy.wait_recv()
    for t in range(4):
        rows_t = pl.ds(pl.multiple_of(px * 128 + t * n_seq, n_seq), n_seq)
        qsum[t] = (qpart[rows_t, :] + qrec[pl.ds(t * n_seq, n_seq), :]).astype(BF16)
    hops = []
    for i in range(1, 4):
        t = lax.rem(py + i, 4)
        copy = remote(qsum.at[t], qall.at[py], a_send.at[i - 1], a_recv.at[i - 1], px, t)
        copy.start()
        hops.append(copy)
    kv_copy.wait_recv()
    kv = (kvpart[pl.ds(n_seq, n_seq), :] + kvrec[...]).astype(BF16).astype(F32)
    kn_out[...] = kv[:, :256]
    vn_out[...] = kv[:, 256:]

    def emit(t, block):
        block = block.astype(F32)
        for j in range(2):
            row = pl.multiple_of((2 * t + j) * n_seq, n_seq)
            for half in range(2):
                q_out[half, pl.ds(row, n_seq), :] = block[:, (2 * j + half) * 128:(2 * j + half + 1) * 128]

    emit(py, qsum[py])
    for i in range(1, 4):
        hops[i - 1].wait_recv()
        t = lax.rem(py + 4 - i, 4)
        emit(t, qall[t])

    for copy in outs:
        copy.wait()
    for copy in to_across + to_mate + relays + msgs + hops + [q_copy, kv_copy]:
        copy.wait_send()

    def settle(i, carry):
        first_copy(i, 0).wait()
        first_copy(i, 1).wait()
        return carry

    lax.fori_loop(0, n_step, settle, 0)


def project(split, hidden, ln_scale, w_q, w_k, w_v, w_gate, w_up):
    any_spec = pl.BlockSpec(memory_space=pl.ANY)
    hbm = pl.BlockSpec(memory_space=pltpu.HBM)
    vmem = pl.BlockSpec(memory_space=pltpu.VMEM)
    sds = jax.ShapeDtypeStruct
    dma = pltpu.SemaphoreType.DMA
    return pl.pallas_call(
        functools.partial(project_kernel, split),
        out_shape=[sds((2, 256, 128), F32), sds((32, 256), F32), sds((32, 256), F32), sds((128, 8192), F32)] + [sds((r, 8192), F32) for r in split],
        in_specs=[hbm] * 7,
        out_specs=[vmem, vmem, vmem] + [any_spec] * 4,
        scratch_shapes=[
            pltpu.VMEM((4, 256, 256), BF16),
            pltpu.VMEM((1, 256), F32),
            pltpu.VMEM((8, 8, 256), F32),
            pltpu.VMEM((256, 128), F32),
            pltpu.VMEM((256, 1024), BF16),
            pltpu.VMEM((1024, 512), BF16),
            pltpu.VMEM((1024, 512), BF16),
            pltpu.VMEM((1024, 4096), BF16),
            pltpu.VMEM((1024, 4096), BF16),
            pltpu.VMEM((256, 8192), F32),
            pltpu.VMEM((256, 512), F32),
            pltpu.VMEM((128, 512), F32),
            pltpu.VMEM((64, 512), F32),
            pltpu.VMEM((32, 512), F32),
            pltpu.VMEM((4, 32, 512), BF16),
            pltpu.VMEM((4, 32, 512), BF16),
            dma((7,)), dma((6,)), dma((6,)), dma((7,)), dma((7,)), dma((2,)), dma((2,)), dma((16,)), dma((16,)), dma((3,)), dma((3,)), dma((3,)),
        ],
        compiler_params=pltpu.CompilerParams(collective_id=0, has_side_effects=True, vmem_limit_bytes=48 * 2**20),
        cost_estimate=pl.CostEstimate(flops=5_000_000_000, bytes_accessed=28 * 2**20, transcendentals=0),
        name="project",
    )(*[pltpu.with_memory_space_constraint(x, pltpu.HBM) for x in (hidden, ln_scale.reshape(1, 256), w_q, w_k, w_v, w_gate, w_up)])


def attend_kernel(pos_ref, q_in, kn_in, vn_ref, cos_ref, sin_ref, k_hbm, v_hbm, k_out, v_out, o_ref, kbuf, vbuf, q_ref, kn_ref, k_in, v_in, k_wr, v_wr):
    n_seq, cache_len, head_dim = k_hbm.shape

    def fetch(b):
        slot = lax.rem(b, RING)
        return (pltpu.make_async_copy(k_hbm.at[b], kbuf.at[slot], k_in.at[slot]),
                pltpu.make_async_copy(v_hbm.at[b], vbuf.at[slot], v_in.at[slot]))

    def drain(b):
        slot = lax.rem(b, RING)
        return (pltpu.make_async_copy(kbuf.at[slot], k_out.at[b], k_wr.at[slot]),
                pltpu.make_async_copy(vbuf.at[slot], v_out.at[b], v_wr.at[slot]))

    for b in range(AHEAD):
        for copy in fetch(b):
            copy.start()

    cos_tab, sin_tab = cos_ref[...], sin_ref[...]
    kn_ref[...] = rotate(kn_in[...], cos_tab, sin_tab).astype(BF16).astype(F32)
    for h in range(8):
        rows = pl.ds(h * n_seq, n_seq)
        lead, tail = q_in[0, rows, :], q_in[1, rows, :]
        q_ref[0, rows, :] = (lead * cos_tab - tail * sin_tab).astype(BF16).astype(F32)
        q_ref[1, rows, :] = (lead * sin_tab + tail * cos_tab).astype(BF16).astype(F32)

    def patch(buf, slot, row, p):
        base = pl.multiple_of((p // 16) * 16, 16)
        tile = buf[slot, pl.ds(base, 16), :]
        hit = lax.broadcasted_iota(jnp.int32, (16, head_dim), 0) == p - base
        buf[slot, pl.ds(base, 16), :] = jnp.where(hit, row, tile.astype(F32)).astype(BF16)

    def one(b, carry):
        slot = lax.rem(b, RING)
        p = pos_ref[b]

        @pl.when(b + AHEAD < n_seq)
        def _():
            @pl.when(b + AHEAD >= RING)
            def _():
                for copy in drain(b + AHEAD - RING):
                    copy.wait()
            for copy in fetch(b + AHEAD):
                copy.start()

        k_copy, v_copy = fetch(b)
        k_save, v_save = drain(b)
        k_copy.wait()
        patch(kbuf, slot, kn_ref[pl.ds(b, 1), :], p)
        k_save.start()
        heads = pl.ds(b, 8, stride=n_seq)
        q = jnp.concatenate([q_ref[0, heads, :], q_ref[1, heads, :]], axis=1).astype(BF16)
        scores = lax.dot_general(q, kbuf[slot], (((1,), (1,)), ((), ())), preferred_element_type=F32) * (head_dim ** -0.5)
        valid = lax.broadcasted_iota(jnp.int32, scores.shape, 1) <= p
        scores = jnp.where(valid, scores, -jnp.inf)
        top = jnp.max(scores, axis=1, keepdims=True)
        e = jnp.exp(scores - top)
        prob = (e / jnp.sum(e, axis=1, keepdims=True)).astype(BF16)
        v_copy.wait()
        patch(vbuf, slot, vn_ref[pl.ds(b, 1), :], p)
        v_save.start()
        out = jnp.dot(prob, vbuf[slot], preferred_element_type=F32)
        o_ref[0, heads, :] = out[:, :128]
        o_ref[1, heads, :] = out[:, 128:]
        return carry

    lax.fori_loop(0, n_seq, one, 0)
    for b in range(n_seq - RING, n_seq):
        for copy in drain(b):
            copy.wait()


def attend(positions, q, kn, vn, cos_tab, sin_tab, k_cache, v_cache):
    any_spec = pl.BlockSpec(memory_space=pl.ANY)
    vmem = pl.BlockSpec(memory_space=pltpu.VMEM)
    n_seq, cache_len, head_dim = k_cache.shape
    dma = pltpu.SemaphoreType.DMA
    return pl.pallas_call(
        attend_kernel,
        out_shape=[jax.ShapeDtypeStruct(k_cache.shape, BF16), jax.ShapeDtypeStruct(v_cache.shape, BF16), jax.ShapeDtypeStruct((2, 256, 128), F32)],
        in_specs=[pl.BlockSpec(memory_space=pltpu.SMEM), vmem, vmem, vmem, vmem, vmem, any_spec, any_spec],
        out_specs=[any_spec, any_spec, vmem],
        scratch_shapes=[
            pltpu.VMEM((RING, cache_len, head_dim), BF16),
            pltpu.VMEM((RING, cache_len, head_dim), BF16),
            pltpu.VMEM((2, 256, 128), F32),
            pltpu.VMEM((n_seq, head_dim), F32),
            dma((RING,)), dma((RING,)), dma((RING,)), dma((RING,)),
        ],
        compiler_params=pltpu.CompilerParams(vmem_limit_bytes=48 * 2**20),
        cost_estimate=pl.CostEstimate(flops=100_000_000_000, bytes_accessed=128 * 2**20, transcendentals=0),
        name="attend",
    )(positions, q, kn, vn, cos_tab, sin_tab, k_cache, v_cache)


def combine_kernel(split, cuts, pieces, h_hbm, attn_ref, wo_hbm, wd_hbm, own_hbm, first_ref, mid_ref, last_ref,
                   out_ref, h, wo, wd, own, got, act, a_snd, a_rcv, res, res_rcv,
                   load_sem, l_send, l_recv, t_send, t_recv, g_send, g_recv, r_send, r_recv):
    px, py = lax.axis_index('tpx'), lax.axis_index('tpy')
    me = px * 4 + py
    n = len(cuts)
    starts = [sum(cuts[:c]) for c in range(n)]
    n_first, n_mid, n_last = split
    late = n_first + n_mid
    greet(px, py)
    loads = [
        pltpu.make_async_copy(own_hbm, own, load_sem.at[0]),
        pltpu.make_async_copy(wo_hbm, wo, load_sem.at[1]),
        pltpu.make_async_copy(wd_hbm, wd, load_sem.at[2]),
        pltpu.make_async_copy(h_hbm, h, load_sem.at[3]),
    ]
    for copy in loads:
        copy.start()
    for t in range(4):
        for j in range(2):
            at = pl.ds((2 * t + j) * 32, 32)
            a_snd[t, j] = jnp.concatenate([attn_ref[0, at, :], attn_ref[1, at, :]], axis=1).astype(BF16)
    met()

    lasts = {}
    for c in range(n):
        if starts[c] >= late:
            seg = pl.ds(starts[c] - late, cuts[c])
            lasts[c] = remote(last_ref.at[seg], got.at[seg], l_send.at[c], l_recv.at[c], 1 - px, py)
            lasts[c].start()
    rows_me = pl.ds(pl.multiple_of(me * 32, 32), 32)
    swaps = []
    for i, (qx, qy) in enumerate(others(px, py)):
        copy = remote(a_snd.at[qy], a_rcv.at[:, rows_me, :], t_send.at[i], t_recv.at[i], qx, qy)
        copy.start()
        swaps.append(copy)
    for j in range(2):
        a_rcv[j, rows_me, :] = a_snd[py, j]

    def activate(c):
        here = pl.ds(starts[c], cuts[c])
        if starts[c] < n_first:
            theirs, there = first_ref, here
        elif starts[c] < late:
            theirs, there = mid_ref, pl.ds(starts[c] - n_first, cuts[c])
        else:
            theirs, there = got, pl.ds(starts[c] - late, cuts[c])

        n_piece = pieces[c]
        width = 4096 // n_piece

        def piece(k):
            cols = pl.ds(pl.multiple_of(k * width, width), width)
            return remote(act.at[pl.ds(2 * starts[c], cuts[c]), cols], act.at[pl.ds(2 * starts[c] + cuts[c], cuts[c]), cols],
                          g_send.at[sum(pieces[:c]) + k], g_recv.at[sum(pieces[:c]) + k], 1 - px, py)

        def cols(k, carry):
            for i in range(width // 512):
                g_cols = pl.ds(pl.multiple_of(k * width + i * 512, 512), 512)
                u_cols = pl.ds(pl.multiple_of(4096 + k * width + i * 512, 512), 512)
                gate = (own[here, g_cols] + theirs[there, g_cols]).astype(BF16).astype(F32)
                up = (own[here, u_cols] + theirs[there, u_cols]).astype(BF16).astype(F32)
                act[pl.ds(2 * starts[c], cuts[c]), g_cols] = (jax.nn.silu(gate) * up).astype(BF16)
            piece(k).start()
            return carry

        lax.fori_loop(0, n_piece, cols, 0)
        return piece

    loads[0].wait()
    gathers = [activate(c) for c in range(n) if starts[c] < late]

    loads[1].wait()
    for copy in swaps:
        copy.wait_recv()
    for c in range(n):
        for side in range(2):
            at = pl.ds(pl.multiple_of(lax.rem(px + side, 2) * 128 + starts[c], 16), cuts[c])
            for t in range(4):
                cols = pl.ds(t * 256, 256)
                res[t, pl.ds(2 * starts[c] + side * cuts[c], cuts[c]), :] = (
                    jnp.dot(a_rcv[0, at, :], wo[pl.ds(0, 256), cols], preferred_element_type=F32)
                    + jnp.dot(a_rcv[1, at, :], wo[pl.ds(256, 256), cols], preferred_element_type=F32))
    for c in lasts:
        lasts[c].wait_recv()
        gathers.append(activate(c))

    loads[2].wait()
    loads[3].wait()
    reduces = []
    mate = py + 1 - 2 * lax.rem(py, 2)
    order = [lax.rem(py + 2, 4), lax.rem(mate + 2, 4), mate, py]

    def finish(c):
        seg = pl.ds(2 * starts[c], 2 * cuts[c])
        total = res[py, seg, :]
        for i in range(3):
            reduces[c][i].wait_recv()
            total = total + res_rcv[order[i], seg, :]
        for side in range(2):
            at = pl.ds(pl.multiple_of(lax.rem(px + side, 2) * 128 + starts[c], 16), cuts[c])
            out_ref[at, :] = (h[at, :].astype(F32) + total[side * cuts[c]:(side + 1) * cuts[c]]).astype(BF16)

    for c in range(n):
        seg = pl.ds(2 * starts[c], 2 * cuts[c])
        hops = []
        parts = pieces[c]
        depth = 4096 // parts
        for p in range(parts):
            gathers[c](p).wait_recv()
            deep = pl.ds(p * depth, depth)
            for i in range(4):
                t = order[i]
                cols = pl.ds(pl.multiple_of(t * 256, 256), 256)
                res[t, seg, :] += jnp.dot(act[seg, deep], wd[deep, cols], preferred_element_type=F32)
                if p == parts - 1 and i < 3:
                    copy = remote(res.at[t, seg], res_rcv.at[py, seg], r_send.at[3 * c + i], r_recv.at[3 * c + i], px, t)
                    copy.start()
                    hops.append(copy)
        reduces.append(hops)
        if c > 0:
            finish(c - 1)
    finish(n - 1)

    for copy in swaps + list(lasts.values()) + [x for hops in reduces for x in hops]:
        copy.wait_send()
    for c in range(n):
        for k in range(pieces[c]):
            gathers[c](k).wait_send()


def combine(split, cuts, pieces, hidden, attn, w_o, w_down, own, first, mid, last):
    any_spec = pl.BlockSpec(memory_space=pl.ANY)
    hbm = pl.BlockSpec(memory_space=pltpu.HBM)
    vmem = pl.BlockSpec(memory_space=pltpu.VMEM)
    dma = pltpu.SemaphoreType.DMA
    n = len(cuts)
    return pl.pallas_call(
        functools.partial(combine_kernel, split, cuts, pieces),
        out_shape=jax.ShapeDtypeStruct((256, 256), BF16),
        in_specs=[hbm, vmem, hbm, hbm, any_spec, vmem, vmem, vmem],
        out_specs=vmem,
        scratch_shapes=[
            pltpu.VMEM((256, 256), BF16),
            pltpu.VMEM((512, 1024), BF16),
            pltpu.VMEM((4096, 1024), BF16),
            pltpu.VMEM((128, 8192), F32),
            pltpu.VMEM((split[2], 8192), F32),
            pltpu.VMEM((256, 4096), BF16),
            pltpu.VMEM((4, 2, 32, 256), BF16),
            pltpu.VMEM((2, 256, 256), BF16),
            pltpu.VMEM((4, 256, 256), F32),
            pltpu.VMEM((4, 256, 256), F32),
            dma((4,)), dma((n,)), dma((n,)), dma((7,)), dma((7,)), dma((sum(pieces),)), dma((sum(pieces),)), dma((3 * n,)), dma((3 * n,)),
        ],
        compiler_params=pltpu.CompilerParams(collective_id=1, has_side_effects=True, vmem_limit_bytes=48 * 2**20),
        cost_estimate=pl.CostEstimate(flops=3_000_000_000, bytes_accessed=18 * 2**20, transcendentals=0),
        name="combine",
    )(hidden, attn, w_o, w_down, own, first, mid, last)


def solution(mesh):
    hidden_spec = P('dp', ('tpx', 'tpy'))
    cache_spec = P(('dp', 'tpx', 'tpy'), None, None)
    in_specs = (hidden_spec, P(('tpx', 'tpy')), P('tpx', 'tpy'), P('tpx', None), P('tpx', None), P('tpx', 'tpy'), P('tpx', 'tpy'), P('tpy', 'tpx'), P('tpy', 'tpx'), cache_spec, cache_spec, P(('dp', 'tpx', 'tpy')))
    out_specs = (hidden_spec, cache_spec, cache_spec)
    split, cuts, pieces = (32, 64, 32), (32, 32, 32, 32), (1, 1, 1, 4)
    swap = [(0, 1), (1, 0)]

    def device_step(hidden, ln_scale, w_q, w_k, w_v, w_gate, w_up, w_o, w_down, k_cache, v_cache, positions):
        q, kn, vn, own, first, mid, last = project(split, hidden, ln_scale, w_q, w_k, w_v, w_gate, w_up)
        mid = lax.ppermute(mid, 'tpx', swap)
        late_pos, kn = lax.optimization_barrier((positions, kn))
        cos_tab, sin_tab = rope_tables(late_pos, k_cache.shape[2])
        k_all, v_all, attn = attend(positions, q, kn, vn, cos_tab, sin_tab, k_cache, v_cache)
        hidden_out = combine(split, cuts, pieces, hidden, attn, w_o, w_down, own, first, mid, last)
        return hidden_out, k_all, v_all

    return jax.shard_map(device_step, mesh=mesh, in_specs=in_specs, out_specs=out_specs, check_vma=False)
```

```python
import functools
import jax
import jax.numpy as jnp
from jax import lax
from jax.experimental import pallas as pl
from jax.experimental.pallas import tpu as pltpu
from jax.sharding import PartitionSpec as P

LN_EPS = 1e-6
ROPE_BASE = 10000.0
MESH = pl.DeviceIdType.MESH
F32 = jnp.float32
BF16 = jnp.bfloat16
RING = 8
AHEAD = 4


def rope_tables(positions, head_dim):
    half_dim = head_dim // 2
    inv_freq = ROPE_BASE ** (-(jnp.arange(half_dim, dtype=F32) * 2.0 / head_dim))
    angles = positions.astype(F32)[:, None] * inv_freq[None, :]
    return jnp.cos(angles), jnp.sin(angles)


def rotate(x, cos_tab, sin_tab):
    half = x.shape[-1] // 2
    lead, tail = x[:, :half], x[:, half:]
    return jnp.concatenate([lead * cos_tab - tail * sin_tab, lead * sin_tab + tail * cos_tab], axis=-1)


def others(px, py):
    return [(lax.rem(px + dx, 2), lax.rem(py + dy, 4)) for dx in range(2) for dy in range(4) if (dx, dy) != (0, 0)]


def greet(px, py):
    barrier = pltpu.get_barrier_semaphore()
    for qx, qy in others(px, py):
        pl.semaphore_signal(barrier, 1, device_id={'tpx': qx, 'tpy': qy}, device_id_type=MESH)


def met():
    pl.semaphore_wait(pltpu.get_barrier_semaphore(), 7)


def remote(src, dst, send_sem, recv_sem, qx, qy):
    return pltpu.make_async_remote_copy(src, dst, send_sem, recv_sem, device_id={'tpx': qx, 'tpy': qy}, device_id_type=MESH)


def project_kernel(split, h_hbm, scale_hbm, wq_hbm, wk_hbm, wv_hbm, wg_hbm, wu_hbm,
                   q_out, kn_out, vn_out, own_out, first_out, mid_out, last_out,
                   hbuf, scale, msg, stats_col, u, wq, wkv, wg, wu, part, qpart, qrec, kvpart, kvrec, qsum, qall,
                   load_sem, h_send, h_recv, m_send, m_recv, x_send, x_recv, f_send, f_recv, a_send, a_recv, o_sem):
    px, py = lax.axis_index('tpx'), lax.axis_index('tpy')
    me = px * 4 + py
    mate = py + 1 - 2 * lax.rem(py, 2)
    across = lax.rem(py + 2, 4)
    n_seq = 32

    loads = [
        pltpu.make_async_copy(h_hbm, hbuf.at[py], load_sem.at[0]),
        pltpu.make_async_copy(scale_hbm, scale, load_sem.at[1]),
        pltpu.make_async_copy(wk_hbm, wkv.at[:, pl.ds(0, 256)], load_sem.at[2]),
        pltpu.make_async_copy(wv_hbm, wkv.at[:, pl.ds(256, 256)], load_sem.at[3]),
        pltpu.make_async_copy(wq_hbm, wq, load_sem.at[4]),
        pltpu.make_async_copy(wg_hbm, wg, load_sem.at[5]),
        pltpu.make_async_copy(wu_hbm, wu, load_sem.at[6]),
    ]
    for copy in loads[:2]:
        copy.start()
    greet(px, py)
    for copy in loads[2:]:
        copy.start()
    loads[0].wait()
    met()
    far = pl.ds(pl.multiple_of((1 - px) * 128, 128), 128)
    near = pl.ds(pl.multiple_of(px * 128, 128), 128)

    def h_copy(block, rows, at, qy):
        return remote(hbuf.at[block, rows], hbuf.at[block, rows], h_send.at[at], h_recv.at[at], px, qy)

    to_across = [h_copy(py, far, 0, across), h_copy(py, near, 1, across)]
    to_mate = [h_copy(py, far, 2, mate), h_copy(py, near, 3, mate)]
    relays = [h_copy(across, far, 4, mate), h_copy(across, near, 5, mate)]
    to_across[0].start()
    to_mate[0].start()

    hf = hbuf[py].astype(F32)
    mean = jnp.sum(hf, axis=1, keepdims=True) * (1.0 / 256.0)
    dev = hf - mean
    m2 = jnp.sum(dev * dev, axis=1, keepdims=True)
    lane = lax.broadcasted_iota(jnp.int32, (256, 128), 1)
    stat = jnp.where(lane == 0, mean, m2)
    stat_t = stat.T
    loads[1].wait()
    msg[me] = jnp.concatenate([stat_t[0:2], scale[...], jnp.zeros((5, 256), F32)], axis=0)
    msgs = []
    for i, (qx, qy) in enumerate(others(px, py)):
        copy = remote(msg.at[me], msg.at[me], m_send.at[i], m_recv.at[i], qx, qy)
        copy.start()
        msgs.append(copy)
    to_across[1].start()
    to_mate[1].start()
    to_across[0].wait_recv()
    relays[0].start()
    for copy in msgs:
        copy.wait_recv()

    means = jnp.concatenate([msg[e, 0:1] for e in range(8)], axis=0)
    m2s = jnp.concatenate([msg[e, 1:2] for e in range(8)], axis=0)
    mu = jnp.sum(means, axis=0, keepdims=True) * 0.125
    gap = means - mu
    var = (jnp.sum(m2s, axis=0, keepdims=True) + 256.0 * jnp.sum(gap * gap, axis=0, keepdims=True)) * (1.0 / 2048.0)
    rstd = lax.rsqrt(var + LN_EPS)
    both = jnp.concatenate([mu, rstd, jnp.zeros((126, 256), F32)], axis=0).T
    stats_col[...] = both

    def norm(t, rows):
        cols = pl.ds(pl.multiple_of(t * 256, 256), 256)
        table = stats_col[rows, :]
        u[rows, cols] = ((hbuf[t, rows, :].astype(F32) - table[:, 0:1]) * table[:, 1:2] * msg[px * 4 + t, 2:3]).astype(BF16)

    def gather(i, rows):
        norm(py, rows)
        to_mate[i].wait_recv()
        norm(mate, rows)
        norm(across, rows)
        relays[i].wait_recv()
        norm(lax.rem(mate + 2, 4), rows)

    gather(0, far)
    far_seq = pl.ds(pl.multiple_of((1 - px) * 128 + py * n_seq, n_seq), n_seq)
    near_seq = pl.ds(pl.multiple_of(px * 128 + py * n_seq, n_seq), n_seq)
    loads[2].wait()
    loads[3].wait()
    kvpart[pl.ds(0, n_seq), :] = jnp.dot(u[far_seq, :], wkv[...], preferred_element_type=F32)
    kv_copy = remote(kvpart.at[pl.ds(0, n_seq)], kvrec, x_send.at[1], x_recv.at[1], 1 - px, py)
    kv_copy.start()
    loads[4].wait()
    qpart[far, :] = jnp.dot(u[far, :], wq[...], preferred_element_type=F32)
    q_copy = remote(qpart.at[far], qrec, x_send.at[0], x_recv.at[0], 1 - px, py)
    q_copy.start()
    to_across[1].wait_recv()
    relays[1].start()
    gather(1, near)

    loads[5].wait()
    loads[6].wait()
    step = 512
    n_step = 4096 // step
    n_first, n_mid, n_last = split
    first_rows = pl.ds(pl.multiple_of((1 - px) * 128, 8), n_first)
    mid_rows = pl.ds(pl.multiple_of((1 - px) * 128 + n_first, 8), n_mid)
    last_rows = pl.ds(pl.multiple_of((1 - px) * 128 + n_first + n_mid, 8), n_last)

    def first_copy(i, base):
        cols = pl.ds(pl.multiple_of(base * 4096 + i * step, step), step)
        at = base * n_step + i
        return remote(part.at[first_rows, cols], first_out.at[:, cols], f_send.at[at], f_recv.at[at], 1 - px, py)

    def columns(i, carry):
        cols = pl.ds(pl.multiple_of(i * step, step), step)
        part[:, cols] = jnp.dot(u[...], wg[:, cols], preferred_element_type=F32)
        first_copy(i, 0).start()
        up_cols = pl.ds(pl.multiple_of(4096 + i * step, step), step)
        part[:, up_cols] = jnp.dot(u[...], wu[:, cols], preferred_element_type=F32)
        first_copy(i, 1).start()
        return carry

    lax.fori_loop(0, n_step, columns, 0)
    outs = [
        pltpu.make_async_copy(part.at[near], own_out, o_sem.at[0]),
        pltpu.make_async_copy(part.at[mid_rows], mid_out, o_sem.at[1]),
        pltpu.make_async_copy(part.at[last_rows], last_out, o_sem.at[2]),
    ]
    for copy in outs:
        copy.start()
    qpart[near, :] = jnp.dot(u[near, :], wq[...], preferred_element_type=F32)
    kvpart[pl.ds(n_seq, n_seq), :] = jnp.dot(u[near_seq, :], wkv[...], preferred_element_type=F32)

    q_copy.wait_recv()
    for t in range(4):
        rows_t = pl.ds(pl.multiple_of(px * 128 + t * n_seq, n_seq), n_seq)
        qsum[t] = (qpart[rows_t, :] + qrec[pl.ds(t * n_seq, n_seq), :]).astype(BF16)
    hops = []
    for i in range(1, 4):
        t = lax.rem(py + i, 4)
        copy = remote(qsum.at[t], qall.at[py], a_send.at[i - 1], a_recv.at[i - 1], px, t)
        copy.start()
        hops.append(copy)
    kv_copy.wait_recv()
    kv = (kvpart[pl.ds(n_seq, n_seq), :] + kvrec[...]).astype(BF16).astype(F32)
    kn_out[...] = kv[:, :256]
    vn_out[...] = kv[:, 256:]

    def emit(t, block):
        block = block.astype(F32)
        for j in range(2):
            row = pl.multiple_of((2 * t + j) * n_seq, n_seq)
            for half in range(2):
                q_out[half, pl.ds(row, n_seq), :] = block[:, (2 * j + half) * 128:(2 * j + half + 1) * 128]

    emit(py, qsum[py])
    for i in range(1, 4):
        hops[i - 1].wait_recv()
        t = lax.rem(py + 4 - i, 4)
        emit(t, qall[t])

    for copy in outs:
        copy.wait()
    for copy in to_across + to_mate + relays + msgs + hops + [q_copy, kv_copy]:
        copy.wait_send()

    def settle(i, carry):
        first_copy(i, 0).wait()
        first_copy(i, 1).wait()
        return carry

    lax.fori_loop(0, n_step, settle, 0)


def project(split, hidden, ln_scale, w_q, w_k, w_v, w_gate, w_up):
    any_spec = pl.BlockSpec(memory_space=pl.ANY)
    hbm = pl.BlockSpec(memory_space=pltpu.HBM)
    vmem = pl.BlockSpec(memory_space=pltpu.VMEM)
    sds = jax.ShapeDtypeStruct
    dma = pltpu.SemaphoreType.DMA
    return pl.pallas_call(
        functools.partial(project_kernel, split),
        out_shape=[sds((2, 256, 128), F32), sds((32, 256), F32), sds((32, 256), F32), sds((128, 8192), F32)] + [sds((r, 8192), F32) for r in split],
        in_specs=[hbm] * 7,
        out_specs=[vmem, vmem, vmem] + [any_spec] * 4,
        scratch_shapes=[
            pltpu.VMEM((4, 256, 256), BF16),
            pltpu.VMEM((1, 256), F32),
            pltpu.VMEM((8, 8, 256), F32),
            pltpu.VMEM((256, 128), F32),
            pltpu.VMEM((256, 1024), BF16),
            pltpu.VMEM((1024, 512), BF16),
            pltpu.VMEM((1024, 512), BF16),
            pltpu.VMEM((1024, 4096), BF16),
            pltpu.VMEM((1024, 4096), BF16),
            pltpu.VMEM((256, 8192), F32),
            pltpu.VMEM((256, 512), F32),
            pltpu.VMEM((128, 512), F32),
            pltpu.VMEM((64, 512), F32),
            pltpu.VMEM((32, 512), F32),
            pltpu.VMEM((4, 32, 512), BF16),
            pltpu.VMEM((4, 32, 512), BF16),
            dma((7,)), dma((6,)), dma((6,)), dma((7,)), dma((7,)), dma((2,)), dma((2,)), dma((16,)), dma((16,)), dma((3,)), dma((3,)), dma((3,)),
        ],
        compiler_params=pltpu.CompilerParams(collective_id=0, has_side_effects=True, vmem_limit_bytes=48 * 2**20),
        cost_estimate=pl.CostEstimate(flops=5_000_000_000, bytes_accessed=28 * 2**20, transcendentals=0),
        name="project",
    )(*[pltpu.with_memory_space_constraint(x, pltpu.HBM) for x in (hidden, ln_scale.reshape(1, 256), w_q, w_k, w_v, w_gate, w_up)])


def attend_kernel(pos_ref, q_in, kn_in, vn_ref, cos_ref, sin_ref, k_hbm, v_hbm, k_out, v_out, o_ref, kbuf, vbuf, q_ref, kn_ref, k_in, v_in, k_wr, v_wr):
    n_seq, cache_len, head_dim = k_hbm.shape

    def fetch(b):
        slot = lax.rem(b, RING)
        return (pltpu.make_async_copy(k_hbm.at[b], kbuf.at[slot], k_in.at[slot]),
                pltpu.make_async_copy(v_hbm.at[b], vbuf.at[slot], v_in.at[slot]))

    def drain(b):
        slot = lax.rem(b, RING)
        return (pltpu.make_async_copy(kbuf.at[slot], k_out.at[b], k_wr.at[slot]),
                pltpu.make_async_copy(vbuf.at[slot], v_out.at[b], v_wr.at[slot]))

    for b in range(AHEAD):
        for copy in fetch(b):
            copy.start()

    cos_tab, sin_tab = cos_ref[...], sin_ref[...]
    kn_ref[...] = rotate(kn_in[...], cos_tab, sin_tab).astype(BF16).astype(F32)
    for h in range(8):
        rows = pl.ds(h * n_seq, n_seq)
        lead, tail = q_in[0, rows, :], q_in[1, rows, :]
        q_ref[0, rows, :] = (lead * cos_tab - tail * sin_tab).astype(BF16).astype(F32)
        q_ref[1, rows, :] = (lead * sin_tab + tail * cos_tab).astype(BF16).astype(F32)

    def patch(buf, slot, row, p):
        base = pl.multiple_of((p // 16) * 16, 16)
        tile = buf[slot, pl.ds(base, 16), :]
        hit = lax.broadcasted_iota(jnp.int32, (16, head_dim), 0) == p - base
        buf[slot, pl.ds(base, 16), :] = jnp.where(hit, row, tile.astype(F32)).astype(BF16)

    def one(b, carry):
        slot = lax.rem(b, RING)
        p = pos_ref[b]

        @pl.when(b + AHEAD < n_seq)
        def _():
            @pl.when(b + AHEAD >= RING)
            def _():
                for copy in drain(b + AHEAD - RING):
                    copy.wait()
            for copy in fetch(b + AHEAD):
                copy.start()

        k_copy, v_copy = fetch(b)
        k_save, v_save = drain(b)
        k_copy.wait()
        patch(kbuf, slot, kn_ref[pl.ds(b, 1), :], p)
        k_save.start()
        heads = pl.ds(b, 8, stride=n_seq)
        q = jnp.concatenate([q_ref[0, heads, :], q_ref[1, heads, :]], axis=1).astype(BF16)
        scores = lax.dot_general(q, kbuf[slot], (((1,), (1,)), ((), ())), preferred_element_type=F32) * (head_dim ** -0.5)
        valid = lax.broadcasted_iota(jnp.int32, scores.shape, 1) <= p
        scores = jnp.where(valid, scores, -jnp.inf)
        top = jnp.max(scores, axis=1, keepdims=True)
        e = jnp.exp(scores - top)
        prob = (e / jnp.sum(e, axis=1, keepdims=True)).astype(BF16)
        v_copy.wait()
        patch(vbuf, slot, vn_ref[pl.ds(b, 1), :], p)
        v_save.start()
        out = jnp.dot(prob, vbuf[slot], preferred_element_type=F32)
        o_ref[0, heads, :] = out[:, :128]
        o_ref[1, heads, :] = out[:, 128:]
        return carry

    lax.fori_loop(0, n_seq, one, 0)
    for b in range(n_seq - RING, n_seq):
        for copy in drain(b):
            copy.wait()


def attend(positions, q, kn, vn, cos_tab, sin_tab, k_cache, v_cache):
    any_spec = pl.BlockSpec(memory_space=pl.ANY)
    vmem = pl.BlockSpec(memory_space=pltpu.VMEM)
    n_seq, cache_len, head_dim = k_cache.shape
    dma = pltpu.SemaphoreType.DMA
    return pl.pallas_call(
        attend_kernel,
        out_shape=[jax.ShapeDtypeStruct(k_cache.shape, BF16), jax.ShapeDtypeStruct(v_cache.shape, BF16), jax.ShapeDtypeStruct((2, 256, 128), F32)],
        in_specs=[pl.BlockSpec(memory_space=pltpu.SMEM), vmem, vmem, vmem, vmem, vmem, any_spec, any_spec],
        out_specs=[any_spec, any_spec, vmem],
        scratch_shapes=[
            pltpu.VMEM((RING, cache_len, head_dim), BF16),
            pltpu.VMEM((RING, cache_len, head_dim), BF16),
            pltpu.VMEM((2, 256, 128), F32),
            pltpu.VMEM((n_seq, head_dim), F32),
            dma((RING,)), dma((RING,)), dma((RING,)), dma((RING,)),
        ],
        compiler_params=pltpu.CompilerParams(vmem_limit_bytes=48 * 2**20),
        cost_estimate=pl.CostEstimate(flops=100_000_000_000, bytes_accessed=128 * 2**20, transcendentals=0),
        name="attend",
    )(positions, q, kn, vn, cos_tab, sin_tab, k_cache, v_cache)


def combine_kernel(split, cuts, pieces, h_hbm, attn_ref, wo_hbm, wd_hbm, own_hbm, first_ref, mid_ref, last_ref,
                   out_ref, h, wo, wd, own, got, act, a_snd, a_rcv, res, res_rcv,
                   load_sem, l_send, l_recv, t_send, t_recv, g_send, g_recv, r_send, r_recv):
    px, py = lax.axis_index('tpx'), lax.axis_index('tpy')
    me = px * 4 + py
    n = len(cuts)
    starts = [sum(cuts[:c]) for c in range(n)]
    n_first, n_mid, n_last = split
    late = n_first + n_mid
    greet(px, py)
    loads = [
        pltpu.make_async_copy(own_hbm, own, load_sem.at[0]),
        pltpu.make_async_copy(wo_hbm, wo, load_sem.at[1]),
        pltpu.make_async_copy(wd_hbm, wd, load_sem.at[2]),
        pltpu.make_async_copy(h_hbm, h, load_sem.at[3]),
    ]
    for copy in loads:
        copy.start()
    for t in range(4):
        for j in range(2):
            at = pl.ds((2 * t + j) * 32, 32)
            a_snd[t, j] = jnp.concatenate([attn_ref[0, at, :], attn_ref[1, at, :]], axis=1).astype(BF16)
    met()

    lasts = {}
    for c in range(n):
        if starts[c] >= late:
            seg = pl.ds(starts[c] - late, cuts[c])
            lasts[c] = remote(last_ref.at[seg], got.at[seg], l_send.at[c], l_recv.at[c], 1 - px, py)
            lasts[c].start()
    rows_me = pl.ds(pl.multiple_of(me * 32, 32), 32)
    swaps = []
    for i, (qx, qy) in enumerate(others(px, py)):
        copy = remote(a_snd.at[qy], a_rcv.at[:, rows_me, :], t_send.at[i], t_recv.at[i], qx, qy)
        copy.start()
        swaps.append(copy)
    for j in range(2):
        a_rcv[j, rows_me, :] = a_snd[py, j]

    def activate(c):
        here = pl.ds(starts[c], cuts[c])
        if starts[c] < n_first:
            theirs, there = first_ref, here
        elif starts[c] < late:
            theirs, there = mid_ref, pl.ds(starts[c] - n_first, cuts[c])
        else:
            theirs, there = got, pl.ds(starts[c] - late, cuts[c])

        n_piece = pieces[c]
        width = 4096 // n_piece

        def piece(k):
            cols = pl.ds(pl.multiple_of(k * width, width), width)
            return remote(act.at[pl.ds(2 * starts[c], cuts[c]), cols], act.at[pl.ds(2 * starts[c] + cuts[c], cuts[c]), cols],
                          g_send.at[sum(pieces[:c]) + k], g_recv.at[sum(pieces[:c]) + k], 1 - px, py)

        def cols(k, carry):
            for i in range(width // 512):
                g_cols = pl.ds(pl.multiple_of(k * width + i * 512, 512), 512)
                u_cols = pl.ds(pl.multiple_of(4096 + k * width + i * 512, 512), 512)
                gate = (own[here, g_cols] + theirs[there, g_cols]).astype(BF16).astype(F32)
                up = (own[here, u_cols] + theirs[there, u_cols]).astype(BF16).astype(F32)
                act[pl.ds(2 * starts[c], cuts[c]), g_cols] = (jax.nn.silu(gate) * up).astype(BF16)
            piece(k).start()
            return carry

        lax.fori_loop(0, n_piece, cols, 0)
        return piece

    loads[0].wait()
    gathers = [activate(c) for c in range(n) if starts[c] < late]

    loads[1].wait()
    for copy in swaps:
        copy.wait_recv()
    for c in range(n):
        for side in range(2):
            at = pl.ds(pl.multiple_of(lax.rem(px + side, 2) * 128 + starts[c], 16), cuts[c])
            for t in range(4):
                cols = pl.ds(t * 256, 256)
                res[t, pl.ds(2 * starts[c] + side * cuts[c], cuts[c]), :] = (
                    jnp.dot(a_rcv[0, at, :], wo[pl.ds(0, 256), cols], preferred_element_type=F32)
                    + jnp.dot(a_rcv[1, at, :], wo[pl.ds(256, 256), cols], preferred_element_type=F32))
    for c in lasts:
        lasts[c].wait_recv()
        gathers.append(activate(c))

    loads[2].wait()
    loads[3].wait()
    reduces = []
    mate = py + 1 - 2 * lax.rem(py, 2)
    order = [lax.rem(py + 2, 4), lax.rem(mate + 2, 4), mate, py]

    def finish(c):
        seg = pl.ds(2 * starts[c], 2 * cuts[c])
        total = res[py, seg, :]
        for i in range(3):
            reduces[c][i].wait_recv()
            total = total + res_rcv[order[i], seg, :]
        for side in range(2):
            at = pl.ds(pl.multiple_of(lax.rem(px + side, 2) * 128 + starts[c], 16), cuts[c])
            out_ref[at, :] = (h[at, :].astype(F32) + total[side * cuts[c]:(side + 1) * cuts[c]]).astype(BF16)

    for c in range(n):
        seg = pl.ds(2 * starts[c], 2 * cuts[c])
        hops = []
        parts = pieces[c]
        depth = 4096 // parts
        for p in range(parts):
            gathers[c](p).wait_recv()
            deep = pl.ds(p * depth, depth)
            if p < parts - 1:
                term = jnp.dot(act[seg, deep], wd[deep, :], preferred_element_type=F32)
                for t in range(4):
                    res[t, seg, :] += term[:, t * 256:(t + 1) * 256]
                continue
            for side in range(2):
                pair = lax.rem(py // 2 + 1 + side, 2)
                cols = pl.ds(pl.multiple_of(pair * 512, 512), 512)
                term = jnp.dot(act[seg, deep], wd[deep, cols], preferred_element_type=F32)
                res[2 * pair, seg, :] += term[:, :256]
                res[2 * pair + 1, seg, :] += term[:, 256:]
                for i in ((0, 1), (2,))[side]:
                    copy = remote(res.at[order[i], seg], res_rcv.at[py, seg], r_send.at[3 * c + i], r_recv.at[3 * c + i], px, order[i])
                    copy.start()
                    hops.append(copy)
        reduces.append(hops)
        if c > 0:
            finish(c - 1)
    finish(n - 1)

    for copy in swaps + list(lasts.values()) + [x for hops in reduces for x in hops]:
        copy.wait_send()
    for c in range(n):
        for k in range(pieces[c]):
            gathers[c](k).wait_send()


def combine(split, cuts, pieces, hidden, attn, w_o, w_down, own, first, mid, last):
    any_spec = pl.BlockSpec(memory_space=pl.ANY)
    hbm = pl.BlockSpec(memory_space=pltpu.HBM)
    vmem = pl.BlockSpec(memory_space=pltpu.VMEM)
    dma = pltpu.SemaphoreType.DMA
    n = len(cuts)
    return pl.pallas_call(
        functools.partial(combine_kernel, split, cuts, pieces),
        out_shape=jax.ShapeDtypeStruct((256, 256), BF16),
        in_specs=[hbm, vmem, hbm, hbm, any_spec, vmem, vmem, vmem],
        out_specs=vmem,
        scratch_shapes=[
            pltpu.VMEM((256, 256), BF16),
            pltpu.VMEM((512, 1024), BF16),
            pltpu.VMEM((4096, 1024), BF16),
            pltpu.VMEM((128, 8192), F32),
            pltpu.VMEM((split[2], 8192), F32),
            pltpu.VMEM((256, 4096), BF16),
            pltpu.VMEM((4, 2, 32, 256), BF16),
            pltpu.VMEM((2, 256, 256), BF16),
            pltpu.VMEM((4, 256, 256), F32),
            pltpu.VMEM((4, 256, 256), F32),
            dma((4,)), dma((n,)), dma((n,)), dma((7,)), dma((7,)), dma((sum(pieces),)), dma((sum(pieces),)), dma((3 * n,)), dma((3 * n,)),
        ],
        compiler_params=pltpu.CompilerParams(collective_id=1, has_side_effects=True, vmem_limit_bytes=48 * 2**20),
        cost_estimate=pl.CostEstimate(flops=3_000_000_000, bytes_accessed=18 * 2**20, transcendentals=0),
        name="combine",
    )(hidden, attn, w_o, w_down, own, first, mid, last)


def solution(mesh):
    hidden_spec = P('dp', ('tpx', 'tpy'))
    cache_spec = P(('dp', 'tpx', 'tpy'), None, None)
    in_specs = (hidden_spec, P(('tpx', 'tpy')), P('tpx', 'tpy'), P('tpx', None), P('tpx', None), P('tpx', 'tpy'), P('tpx', 'tpy'), P('tpy', 'tpx'), P('tpy', 'tpx'), cache_spec, cache_spec, P(('dp', 'tpx', 'tpy')))
    out_specs = (hidden_spec, cache_spec, cache_spec)
    split, cuts, pieces = (48, 64, 16), (48, 32, 32, 16), (1, 1, 4, 4)
    swap = [(0, 1), (1, 0)]

    def device_step(hidden, ln_scale, w_q, w_k, w_v, w_gate, w_up, w_o, w_down, k_cache, v_cache, positions):
        q, kn, vn, own, first, mid, last = project(split, hidden, ln_scale, w_q, w_k, w_v, w_gate, w_up)
        mid = lax.ppermute(mid, 'tpx', swap)
        late_pos, kn = lax.optimization_barrier((positions, kn))
        cos_tab, sin_tab = rope_tables(late_pos, k_cache.shape[2])
        k_all, v_all, attn = attend(positions, q, kn, vn, cos_tab, sin_tab, k_cache, v_cache)
        hidden_out = combine(split, cuts, pieces, hidden, attn, w_o, w_down, own, first, mid, last)
        return hidden_out, k_all, v_all

    return jax.shard_map(device_step, mesh=mesh, in_specs=in_specs, out_specs=out_specs, check_vma=False)
```

```python
import functools
import jax
import jax.numpy as jnp
from jax import lax
from jax.experimental import pallas as pl
from jax.experimental.pallas import tpu as pltpu
from jax.sharding import PartitionSpec as P

LN_EPS = 1e-6
ROPE_BASE = 10000.0
MESH = pl.DeviceIdType.MESH
F32 = jnp.float32
BF16 = jnp.bfloat16
RING = 8
AHEAD = 4
HELD = 4


def rope_tables(positions, head_dim):
    half_dim = head_dim // 2
    inv_freq = ROPE_BASE ** (-(jnp.arange(half_dim, dtype=F32) * 2.0 / head_dim))
    angles = positions.astype(F32)[:, None] * inv_freq[None, :]
    return jnp.cos(angles), jnp.sin(angles)


def rotate(x, cos_tab, sin_tab):
    half = x.shape[-1] // 2
    lead, tail = x[:, :half], x[:, half:]
    return jnp.concatenate([lead * cos_tab - tail * sin_tab, lead * sin_tab + tail * cos_tab], axis=-1)


def others(px, py):
    return [(lax.rem(px + dx, 2), lax.rem(py + dy, 4)) for dx in range(2) for dy in range(4) if (dx, dy) != (0, 0)]


def greet(peers):
    barrier = pltpu.get_barrier_semaphore()
    for qx, qy in peers:
        pl.semaphore_signal(barrier, 1, device_id={'tpx': qx, 'tpy': qy}, device_id_type=MESH)


def met(count):
    pl.semaphore_wait(pltpu.get_barrier_semaphore(), count)


def remote(src, dst, send_sem, recv_sem, qx, qy):
    return pltpu.make_async_remote_copy(src, dst, send_sem, recv_sem, device_id={'tpx': qx, 'tpy': qy}, device_id_type=MESH)


def project_kernel(split, h_hbm, scale_hbm, wq_hbm, wk_hbm, wv_hbm, wg_hbm, wu_hbm,
                   q_out, kn_out, vn_out, own_out, first_out, mid_out, last_out,
                   hbuf, scale, msg, stats_col, u, wq, wkv, wg, wu, part, qpart, qrec, kvpart, kvrec, qsum, qall,
                   load_sem, h_send, h_recv, m_send, m_recv, x_send, x_recv, f_send, f_recv, a_send, a_recv, o_sem, go_sem):
    px, py = lax.axis_index('tpx'), lax.axis_index('tpy')
    me = px * 4 + py
    mate = py + 1 - 2 * lax.rem(py, 2)
    across = lax.rem(py + 2, 4)
    n_seq = 32

    loads = [
        pltpu.make_async_copy(h_hbm, hbuf.at[py], load_sem.at[0]),
        pltpu.make_async_copy(scale_hbm, scale, load_sem.at[1]),
        pltpu.make_async_copy(wk_hbm, wkv.at[:, pl.ds(0, 256)], load_sem.at[2]),
        pltpu.make_async_copy(wv_hbm, wkv.at[:, pl.ds(256, 256)], load_sem.at[3]),
        pltpu.make_async_copy(wq_hbm, wq, load_sem.at[4]),
        pltpu.make_async_copy(wg_hbm, wg, load_sem.at[5]),
        pltpu.make_async_copy(wu_hbm, wu, load_sem.at[6]),
    ]
    for copy in loads[:2]:
        copy.start()
    greet(others(px, py))
    for copy in loads[2:]:
        copy.start()
    loads[0].wait()
    met(7)
    far = pl.ds(pl.multiple_of((1 - px) * 128, 128), 128)
    near = pl.ds(pl.multiple_of(px * 128, 128), 128)

    def h_copy(block, rows, at, qy):
        return remote(hbuf.at[block, rows], hbuf.at[block, rows], h_send.at[at], h_recv.at[at], px, qy)

    to_across = [h_copy(py, far, 0, across), h_copy(py, near, 1, across)]
    to_mate = [h_copy(py, far, 2, mate), h_copy(py, near, 3, mate)]
    relays = [h_copy(across, far, 4, mate), h_copy(across, near, 5, mate)]
    to_across[0].start()
    to_mate[0].start()

    hf = hbuf[py].astype(F32)
    mean = jnp.sum(hf, axis=1, keepdims=True) * (1.0 / 256.0)
    dev = hf - mean
    m2 = jnp.sum(dev * dev, axis=1, keepdims=True)
    lane = lax.broadcasted_iota(jnp.int32, (256, 128), 1)
    stat = jnp.where(lane == 0, mean, m2)
    stat_t = stat.T
    loads[1].wait()
    msg[me] = jnp.concatenate([stat_t[0:2], scale[...], jnp.zeros((5, 256), F32)], axis=0)
    msgs = []
    for i, (qx, qy) in enumerate(others(px, py)):
        copy = remote(msg.at[me], msg.at[me], m_send.at[i], m_recv.at[i], qx, qy)
        copy.start()
        msgs.append(copy)
    to_across[1].start()
    to_mate[1].start()
    to_across[0].wait_recv()
    relays[0].start()
    for copy in msgs:
        copy.wait_recv()

    means = jnp.concatenate([msg[e, 0:1] for e in range(8)], axis=0)
    m2s = jnp.concatenate([msg[e, 1:2] for e in range(8)], axis=0)
    mu = jnp.sum(means, axis=0, keepdims=True) * 0.125
    gap = means - mu
    var = (jnp.sum(m2s, axis=0, keepdims=True) + 256.0 * jnp.sum(gap * gap, axis=0, keepdims=True)) * (1.0 / 2048.0)
    rstd = lax.rsqrt(var + LN_EPS)
    both = jnp.concatenate([mu, rstd, jnp.zeros((126, 256), F32)], axis=0).T
    stats_col[...] = both

    def norm(t, rows):
        cols = pl.ds(pl.multiple_of(t * 256, 256), 256)
        table = stats_col[rows, :]
        u[rows, cols] = ((hbuf[t, rows, :].astype(F32) - table[:, 0:1]) * table[:, 1:2] * msg[px * 4 + t, 2:3]).astype(BF16)

    def gather(i, rows):
        norm(py, rows)
        to_mate[i].wait_recv()
        norm(mate, rows)
        norm(across, rows)
        relays[i].wait_recv()
        norm(lax.rem(mate + 2, 4), rows)

    gather(0, far)
    far_seq = pl.ds(pl.multiple_of((1 - px) * 128 + py * n_seq, n_seq), n_seq)
    near_seq = pl.ds(pl.multiple_of(px * 128 + py * n_seq, n_seq), n_seq)
    loads[2].wait()
    loads[3].wait()
    kvpart[pl.ds(0, n_seq), :] = jnp.dot(u[far_seq, :], wkv[...], preferred_element_type=F32)
    kv_copy = remote(kvpart.at[pl.ds(0, n_seq)], kvrec, x_send.at[1], x_recv.at[1], 1 - px, py)
    kv_copy.start()
    loads[4].wait()
    qpart[far, :] = jnp.dot(u[far, :], wq[...], preferred_element_type=F32)
    q_copy = remote(qpart.at[far], qrec, x_send.at[0], x_recv.at[0], 1 - px, py)
    q_copy.start()
    to_across[1].wait_recv()
    relays[1].start()
    gather(1, near)

    loads[5].wait()
    loads[6].wait()
    step = 512
    n_step = 4096 // step
    n_first, n_mid, n_last = split
    first_rows = pl.ds(pl.multiple_of((1 - px) * 128, 8), n_first)
    mid_rows = pl.ds(pl.multiple_of((1 - px) * 128 + n_first, 8), n_mid)
    last_rows = pl.ds(pl.multiple_of((1 - px) * 128 + n_first + n_mid, 8), n_last)

    def first_copy(i, base):
        cols = pl.ds(pl.multiple_of(base * 4096 + i * step, step), step)
        at = base * n_step + i
        return remote(part.at[first_rows, cols], first_out.at[:, cols], f_send.at[at], f_recv.at[at], 1 - px, py)

    holds = lax.rem(py, 2) == 1
    n_piece = 2 * n_step

    def columns(i, carry):
        cols = pl.ds(pl.multiple_of(i * step, step), step)
        part[:, cols] = jnp.dot(u[...], wg[:, cols], preferred_element_type=F32)
        up_cols = pl.ds(pl.multiple_of(4096 + i * step, step), step)

        @pl.when(jnp.logical_or(jnp.logical_not(holds), 2 * i < n_piece - HELD))
        def _():
            first_copy(i, 0).start()

        part[:, up_cols] = jnp.dot(u[...], wu[:, cols], preferred_element_type=F32)

        @pl.when(jnp.logical_or(jnp.logical_not(holds), 2 * i + 1 < n_piece - HELD))
        def _():
            first_copy(i, 1).start()

        return carry

    lax.fori_loop(0, n_step, columns, 0)
    outs = [
        pltpu.make_async_copy(part.at[near], own_out, o_sem.at[0]),
        pltpu.make_async_copy(part.at[mid_rows], mid_out, o_sem.at[1]),
        pltpu.make_async_copy(part.at[last_rows], last_out, o_sem.at[2]),
    ]
    for copy in outs:
        copy.start()
    qpart[near, :] = jnp.dot(u[near, :], wq[...], preferred_element_type=F32)
    kvpart[pl.ds(n_seq, n_seq), :] = jnp.dot(u[near_seq, :], wkv[...], preferred_element_type=F32)

    q_copy.wait_recv()
    for t in range(4):
        rows_t = pl.ds(pl.multiple_of(px * 128 + t * n_seq, n_seq), n_seq)
        qsum[t] = (qpart[rows_t, :] + qrec[pl.ds(t * n_seq, n_seq), :]).astype(BF16)
    hops = []
    for i in range(1, 4):
        t = lax.rem(py + i, 4)
        copy = remote(qsum.at[t], qall.at[py], a_send.at[i - 1], a_recv.at[i - 1], px, t)
        copy.start()
        hops.append(copy)
    kv_copy.wait_recv()
    kv = (kvpart[pl.ds(n_seq, n_seq), :] + kvrec[...]).astype(BF16).astype(F32)
    kn_out[...] = kv[:, :256]
    vn_out[...] = kv[:, 256:]

    def emit(t, block):
        block = block.astype(F32)
        for j in range(2):
            row = pl.multiple_of((2 * t + j) * n_seq, n_seq)
            for half in range(2):
                q_out[half, pl.ds(row, n_seq), :] = block[:, (2 * j + half) * 128:(2 * j + half + 1) * 128]

    emit(py, qsum[py])
    for i in range(1, 4):
        hops[i - 1].wait_recv()
        t = lax.rem(py + 4 - i, 4)
        emit(t, qall[t])

    for copy in outs:
        copy.wait()
    for copy in to_across + to_mate + relays + msgs + hops + [q_copy, kv_copy]:
        copy.wait_send()

    @pl.when(jnp.logical_not(holds))
    def _():
        first_copy(n_step - 1, 0).wait_send()
        pl.semaphore_signal(go_sem, 1, device_id={'tpx': px, 'tpy': mate}, device_id_type=MESH)

    @pl.when(holds)
    def _():
        pl.semaphore_wait(go_sem, 1)
        for k in range(n_piece - HELD, n_piece):
            first_copy(k // 2, k % 2).start()
        first_copy(n_step - 1, 0).wait_send()

    def settle(i, carry):
        first_copy(i, 0).wait_recv()
        first_copy(i, 1).wait()

        @pl.when(i < n_step - 1)
        def _():
            first_copy(i, 0).wait_send()

        return carry

    lax.fori_loop(0, n_step, settle, 0)


def project(split, hidden, ln_scale, w_q, w_k, w_v, w_gate, w_up):
    any_spec = pl.BlockSpec(memory_space=pl.ANY)
    hbm = pl.BlockSpec(memory_space=pltpu.HBM)
    vmem = pl.BlockSpec(memory_space=pltpu.VMEM)
    sds = jax.ShapeDtypeStruct
    dma = pltpu.SemaphoreType.DMA
    return pl.pallas_call(
        functools.partial(project_kernel, split),
        out_shape=[sds((2, 256, 128), F32), sds((32, 256), F32), sds((32, 256), F32), sds((128, 8192), F32)] + [sds((r, 8192), F32) for r in split],
        in_specs=[hbm] * 7,
        out_specs=[vmem, vmem, vmem] + [any_spec] * 4,
        scratch_shapes=[
            pltpu.VMEM((4, 256, 256), BF16),
            pltpu.VMEM((1, 256), F32),
            pltpu.VMEM((8, 8, 256), F32),
            pltpu.VMEM((256, 128), F32),
            pltpu.VMEM((256, 1024), BF16),
            pltpu.VMEM((1024, 512), BF16),
            pltpu.VMEM((1024, 512), BF16),
            pltpu.VMEM((1024, 4096), BF16),
            pltpu.VMEM((1024, 4096), BF16),
            pltpu.VMEM((256, 8192), F32),
            pltpu.VMEM((256, 512), F32),
            pltpu.VMEM((128, 512), F32),
            pltpu.VMEM((64, 512), F32),
            pltpu.VMEM((32, 512), F32),
            pltpu.VMEM((4, 32, 512), BF16),
            pltpu.VMEM((4, 32, 512), BF16),
            dma((7,)), dma((6,)), dma((6,)), dma((7,)), dma((7,)), dma((2,)), dma((2,)), dma((16,)), dma((16,)), dma((3,)), dma((3,)), dma((3,)), pltpu.SemaphoreType.REGULAR,
        ],
        compiler_params=pltpu.CompilerParams(collective_id=0, has_side_effects=True, vmem_limit_bytes=48 * 2**20),
        cost_estimate=pl.CostEstimate(flops=5_000_000_000, bytes_accessed=28 * 2**20, transcendentals=0),
        name="project",
    )(*[pltpu.with_memory_space_constraint(x, pltpu.HBM) for x in (hidden, ln_scale.reshape(1, 256), w_q, w_k, w_v, w_gate, w_up)])


def attend_kernel(pos_ref, q_in, kn_in, vn_ref, cos_ref, sin_ref, k_hbm, v_hbm, k_out, v_out, o_ref, kbuf, vbuf, q_ref, kn_ref, k_in, v_in, k_wr, v_wr):
    n_seq, cache_len, head_dim = k_hbm.shape

    def fetch(b):
        slot = lax.rem(b, RING)
        return (pltpu.make_async_copy(k_hbm.at[b], kbuf.at[slot], k_in.at[slot]),
                pltpu.make_async_copy(v_hbm.at[b], vbuf.at[slot], v_in.at[slot]))

    def drain(b):
        slot = lax.rem(b, RING)
        return (pltpu.make_async_copy(kbuf.at[slot], k_out.at[b], k_wr.at[slot]),
                pltpu.make_async_copy(vbuf.at[slot], v_out.at[b], v_wr.at[slot]))

    for b in range(AHEAD):
        for copy in fetch(b):
            copy.start()

    cos_tab, sin_tab = cos_ref[...], sin_ref[...]
    kn_ref[...] = rotate(kn_in[...], cos_tab, sin_tab).astype(BF16).astype(F32)
    for h in range(8):
        rows = pl.ds(h * n_seq, n_seq)
        lead, tail = q_in[0, rows, :], q_in[1, rows, :]
        q_ref[0, rows, :] = (lead * cos_tab - tail * sin_tab).astype(BF16).astype(F32)
        q_ref[1, rows, :] = (lead * sin_tab + tail * cos_tab).astype(BF16).astype(F32)

    def patch(buf, slot, row, p):
        base = pl.multiple_of((p // 16) * 16, 16)
        tile = buf[slot, pl.ds(base, 16), :]
        hit = lax.broadcasted_iota(jnp.int32, (16, head_dim), 0) == p - base
        buf[slot, pl.ds(base, 16), :] = jnp.where(hit, row, tile.astype(F32)).astype(BF16)

    def one(b, carry):
        slot = lax.rem(b, RING)
        p = pos_ref[b]

        @pl.when(b + AHEAD < n_seq)
        def _():
            @pl.when(b + AHEAD >= RING)
            def _():
                for copy in drain(b + AHEAD - RING):
                    copy.wait()
            for copy in fetch(b + AHEAD):
                copy.start()

        k_copy, v_copy = fetch(b)
        k_save, v_save = drain(b)
        k_copy.wait()
        patch(kbuf, slot, kn_ref[pl.ds(b, 1), :], p)
        k_save.start()
        heads = pl.ds(b, 8, stride=n_seq)
        q = jnp.concatenate([q_ref[0, heads, :], q_ref[1, heads, :]], axis=1).astype(BF16)
        scores = lax.dot_general(q, kbuf[slot], (((1,), (1,)), ((), ())), preferred_element_type=F32) * (head_dim ** -0.5)
        valid = lax.broadcasted_iota(jnp.int32, scores.shape, 1) <= p
        scores = jnp.where(valid, scores, -jnp.inf)
        top = jnp.max(scores, axis=1, keepdims=True)
        e = jnp.exp(scores - top)
        prob = (e / jnp.sum(e, axis=1, keepdims=True)).astype(BF16)
        v_copy.wait()
        patch(vbuf, slot, vn_ref[pl.ds(b, 1), :], p)
        v_save.start()
        out = jnp.dot(prob, vbuf[slot], preferred_element_type=F32)
        o_ref[0, heads, :] = out[:, :128]
        o_ref[1, heads, :] = out[:, 128:]
        return carry

    lax.fori_loop(0, n_seq, one, 0)
    for b in range(n_seq - RING, n_seq):
        for copy in drain(b):
            copy.wait()


def attend(positions, q, kn, vn, cos_tab, sin_tab, k_cache, v_cache):
    any_spec = pl.BlockSpec(memory_space=pl.ANY)
    vmem = pl.BlockSpec(memory_space=pltpu.VMEM)
    n_seq, cache_len, head_dim = k_cache.shape
    dma = pltpu.SemaphoreType.DMA
    return pl.pallas_call(
        attend_kernel,
        out_shape=[jax.ShapeDtypeStruct(k_cache.shape, BF16), jax.ShapeDtypeStruct(v_cache.shape, BF16), jax.ShapeDtypeStruct((2, 256, 128), F32)],
        in_specs=[pl.BlockSpec(memory_space=pltpu.SMEM), vmem, vmem, vmem, vmem, vmem, any_spec, any_spec],
        out_specs=[any_spec, any_spec, vmem],
        scratch_shapes=[
            pltpu.VMEM((RING, cache_len, head_dim), BF16),
            pltpu.VMEM((RING, cache_len, head_dim), BF16),
            pltpu.VMEM((2, 256, 128), F32),
            pltpu.VMEM((n_seq, head_dim), F32),
            dma((RING,)), dma((RING,)), dma((RING,)), dma((RING,)),
        ],
        compiler_params=pltpu.CompilerParams(vmem_limit_bytes=48 * 2**20),
        cost_estimate=pl.CostEstimate(flops=100_000_000_000, bytes_accessed=128 * 2**20, transcendentals=0),
        name="attend",
    )(positions, q, kn, vn, cos_tab, sin_tab, k_cache, v_cache)


def combine_kernel(split, cuts, pieces, h_hbm, attn_ref, wo_hbm, wd_hbm, own_hbm, first_ref, mid_ref, last_ref,
                   out_ref, h, wo, wd, own, got, act, a_snd, a_rcv, res, res_rcv,
                   load_sem, l_send, l_recv, t_send, t_recv, g_send, g_recv, r_send, r_recv):
    px, py = lax.axis_index('tpx'), lax.axis_index('tpy')
    me = px * 4 + py
    n = len(cuts)
    starts = [sum(cuts[:c]) for c in range(n)]
    n_first, n_mid, n_last = split
    late = n_first + n_mid
    mate = py + 1 - 2 * lax.rem(py, 2)
    order = [lax.rem(py + 2, 4), lax.rem(mate + 2, 4), mate, py]
    greet([(px, t) for t in order[:3]] + [(1 - px, py)])
    loads = [
        pltpu.make_async_copy(own_hbm, own, load_sem.at[0]),
        pltpu.make_async_copy(wo_hbm, wo, load_sem.at[1]),
        pltpu.make_async_copy(wd_hbm, wd, load_sem.at[2]),
        pltpu.make_async_copy(h_hbm, h, load_sem.at[3]),
    ]
    for copy in loads:
        copy.start()
    for t in range(4):
        for j in range(2):
            at = pl.ds((2 * t + j) * 32, 32)
            a_snd[t, j] = jnp.concatenate([attn_ref[0, at, :], attn_ref[1, at, :]], axis=1).astype(BF16)
    met(4)

    lasts = {}
    for c in range(n):
        if starts[c] >= late:
            seg = pl.ds(starts[c] - late, cuts[c])
            lasts[c] = remote(last_ref.at[seg], got.at[seg], l_send.at[c], l_recv.at[c], 1 - px, py)
            lasts[c].start()
    rows_me = pl.ds(pl.multiple_of(me * 32, 32), 32)
    swaps = []
    for i in range(3):
        copy = remote(a_snd.at[order[i]], a_rcv.at[:, rows_me, :], t_send.at[i], t_recv.at[i], px, order[i])
        copy.start()
        swaps.append(copy)
    for j in range(2):
        a_rcv[j, rows_me, :] = a_snd[py, j]

    def activate(c):
        here = pl.ds(starts[c], cuts[c])
        if starts[c] < n_first:
            theirs, there = first_ref, here
        elif starts[c] < late:
            theirs, there = mid_ref, pl.ds(starts[c] - n_first, cuts[c])
        else:
            theirs, there = got, pl.ds(starts[c] - late, cuts[c])

        n_piece = pieces[c]
        width = 4096 // n_piece

        def piece(k):
            cols = pl.ds(pl.multiple_of(k * width, width), width)
            return remote(act.at[pl.ds(2 * starts[c], cuts[c]), cols], act.at[pl.ds(2 * starts[c] + cuts[c], cuts[c]), cols],
                          g_send.at[sum(pieces[:c]) + k], g_recv.at[sum(pieces[:c]) + k], 1 - px, py)

        def cols(k, carry):
            for i in range(width // 512):
                g_cols = pl.ds(pl.multiple_of(k * width + i * 512, 512), 512)
                u_cols = pl.ds(pl.multiple_of(4096 + k * width + i * 512, 512), 512)
                gate = (own[here, g_cols] + theirs[there, g_cols]).astype(BF16).astype(F32)
                up = (own[here, u_cols] + theirs[there, u_cols]).astype(BF16).astype(F32)
                act[pl.ds(2 * starts[c], cuts[c]), g_cols] = (jax.nn.silu(gate) * up).astype(BF16)
            piece(k).start()
            return carry

        lax.fori_loop(0, n_piece, cols, 0)
        return piece

    for copy in swaps:
        copy.wait_recv()
    near = pl.ds(pl.multiple_of(px * 128, 128), 128)
    a_copy = remote(a_rcv.at[:, near, :], a_rcv.at[:, near, :], t_send.at[3], t_recv.at[3], 1 - px, py)
    a_copy.start()
    loads[0].wait()
    gathers = [activate(c) for c in range(n) if starts[c] < late]

    loads[1].wait()
    a_copy.wait_recv()
    for c in range(n):
        for side in range(2):
            at = pl.ds(pl.multiple_of(lax.rem(px + side, 2) * 128 + starts[c], 16), cuts[c])
            for t in range(4):
                cols = pl.ds(t * 256, 256)
                res[t, pl.ds(2 * starts[c] + side * cuts[c], cuts[c]), :] = (
                    jnp.dot(a_rcv[0, at, :], wo[pl.ds(0, 256), cols], preferred_element_type=F32)
                    + jnp.dot(a_rcv[1, at, :], wo[pl.ds(256, 256), cols], preferred_element_type=F32))
    for c in lasts:
        lasts[c].wait_recv()
        gathers.append(activate(c))

    loads[2].wait()
    loads[3].wait()
    reduces = []

    def finish(c):
        seg = pl.ds(2 * starts[c], 2 * cuts[c])
        total = res[py, seg, :]
        for i in range(3):
            reduces[c][i].wait_recv()
            total = total + res_rcv[order[i], seg, :]
        for side in range(2):
            at = pl.ds(pl.multiple_of(lax.rem(px + side, 2) * 128 + starts[c], 16), cuts[c])
            out_ref[at, :] = (h[at, :].astype(F32) + total[side * cuts[c]:(side + 1) * cuts[c]]).astype(BF16)

    for c in range(n):
        seg = pl.ds(2 * starts[c], 2 * cuts[c])
        hops = []
        parts = pieces[c]
        depth = 4096 // parts
        for p in range(parts):
            gathers[c](p).wait_recv()
            deep = pl.ds(p * depth, depth)
            if p < parts - 1:
                term = jnp.dot(act[seg, deep], wd[deep, :], preferred_element_type=F32)
                for t in range(4):
                    res[t, seg, :] += term[:, t * 256:(t + 1) * 256]
                continue
            for side in range(2):
                pair = lax.rem(py // 2 + 1 + side, 2)
                cols = pl.ds(pl.multiple_of(pair * 512, 512), 512)
                term = jnp.dot(act[seg, deep], wd[deep, cols], preferred_element_type=F32)
                res[2 * pair, seg, :] += term[:, :256]
                res[2 * pair + 1, seg, :] += term[:, 256:]
                for i in ((0, 1), (2,))[side]:
                    copy = remote(res.at[order[i], seg], res_rcv.at[py, seg], r_send.at[3 * c + i], r_recv.at[3 * c + i], px, order[i])
                    copy.start()
                    hops.append(copy)
        reduces.append(hops)
        if c > 0:
            finish(c - 1)
    finish(n - 1)

    for copy in swaps + [a_copy] + list(lasts.values()) + [x for hops in reduces for x in hops]:
        copy.wait_send()
    for c in range(n):
        for k in range(pieces[c]):
            gathers[c](k).wait_send()


def combine(split, cuts, pieces, hidden, attn, w_o, w_down, own, first, mid, last):
    any_spec = pl.BlockSpec(memory_space=pl.ANY)
    hbm = pl.BlockSpec(memory_space=pltpu.HBM)
    vmem = pl.BlockSpec(memory_space=pltpu.VMEM)
    dma = pltpu.SemaphoreType.DMA
    n = len(cuts)
    return pl.pallas_call(
        functools.partial(combine_kernel, split, cuts, pieces),
        out_shape=jax.ShapeDtypeStruct((256, 256), BF16),
        in_specs=[hbm, vmem, hbm, hbm, any_spec, vmem, vmem, vmem],
        out_specs=vmem,
        scratch_shapes=[
            pltpu.VMEM((256, 256), BF16),
            pltpu.VMEM((512, 1024), BF16),
            pltpu.VMEM((4096, 1024), BF16),
            pltpu.VMEM((128, 8192), F32),
            pltpu.VMEM((split[2], 8192), F32),
            pltpu.VMEM((256, 4096), BF16),
            pltpu.VMEM((4, 2, 32, 256), BF16),
            pltpu.VMEM((2, 256, 256), BF16),
            pltpu.VMEM((4, 256, 256), F32),
            pltpu.VMEM((4, 256, 256), F32),
            dma((4,)), dma((n,)), dma((n,)), dma((4,)), dma((4,)), dma((sum(pieces),)), dma((sum(pieces),)), dma((3 * n,)), dma((3 * n,)),
        ],
        compiler_params=pltpu.CompilerParams(collective_id=1, has_side_effects=True, vmem_limit_bytes=48 * 2**20),
        cost_estimate=pl.CostEstimate(flops=3_000_000_000, bytes_accessed=18 * 2**20, transcendentals=0),
        name="combine",
    )(hidden, attn, w_o, w_down, own, first, mid, last)


def solution(mesh):
    hidden_spec = P('dp', ('tpx', 'tpy'))
    cache_spec = P(('dp', 'tpx', 'tpy'), None, None)
    in_specs = (hidden_spec, P(('tpx', 'tpy')), P('tpx', 'tpy'), P('tpx', None), P('tpx', None), P('tpx', 'tpy'), P('tpx', 'tpy'), P('tpy', 'tpx'), P('tpy', 'tpx'), cache_spec, cache_spec, P(('dp', 'tpx', 'tpy')))
    out_specs = (hidden_spec, cache_spec, cache_spec)
    split, cuts, pieces = (48, 64, 16), (48, 32, 32, 16), (1, 1, 4, 4)
    swap = [(0, 1), (1, 0)]

    def device_step(hidden, ln_scale, w_q, w_k, w_v, w_gate, w_up, w_o, w_down, k_cache, v_cache, positions):
        q, kn, vn, own, first, mid, last = project(split, hidden, ln_scale, w_q, w_k, w_v, w_gate, w_up)
        mid = lax.ppermute(mid, 'tpx', swap)
        late_pos, kn = lax.optimization_barrier((positions, kn))
        cos_tab, sin_tab = rope_tables(late_pos, k_cache.shape[2])
        k_all, v_all, attn = attend(positions, q, kn, vn, cos_tab, sin_tab, k_cache, v_cache)
        hidden_out = combine(split, cuts, pieces, hidden, attn, w_o, w_down, own, first, mid, last)
        return hidden_out, k_all, v_all

    return jax.shard_map(device_step, mesh=mesh, in_specs=in_specs, out_specs=out_specs, check_vma=False)
```

```python
import functools
import jax
import jax.numpy as jnp
from jax import lax
from jax.experimental import pallas as pl
from jax.experimental.pallas import tpu as pltpu
from jax.sharding import PartitionSpec as P

LN_EPS = 1e-6
ROPE_BASE = 10000.0
MESH = pl.DeviceIdType.MESH
F32 = jnp.float32
BF16 = jnp.bfloat16
RING = 8
AHEAD = 4
HELD = 5


def rope_tables(positions, head_dim):
    half_dim = head_dim // 2
    inv_freq = ROPE_BASE ** (-(jnp.arange(half_dim, dtype=F32) * 2.0 / head_dim))
    angles = positions.astype(F32)[:, None] * inv_freq[None, :]
    return jnp.cos(angles), jnp.sin(angles)


def rotate(x, cos_tab, sin_tab):
    half = x.shape[-1] // 2
    lead, tail = x[:, :half], x[:, half:]
    return jnp.concatenate([lead * cos_tab - tail * sin_tab, lead * sin_tab + tail * cos_tab], axis=-1)


def others(px, py):
    return [(lax.rem(px + dx, 2), lax.rem(py + dy, 4)) for dx in range(2) for dy in range(4) if (dx, dy) != (0, 0)]


def greet(peers):
    barrier = pltpu.get_barrier_semaphore()
    for qx, qy in peers:
        pl.semaphore_signal(barrier, 1, device_id={'tpx': qx, 'tpy': qy}, device_id_type=MESH)


def met(count):
    pl.semaphore_wait(pltpu.get_barrier_semaphore(), count)


def remote(src, dst, send_sem, recv_sem, qx, qy):
    return pltpu.make_async_remote_copy(src, dst, send_sem, recv_sem, device_id={'tpx': qx, 'tpy': qy}, device_id_type=MESH)


def project_kernel(split, h_hbm, scale_hbm, wq_hbm, wk_hbm, wv_hbm, wg_hbm, wu_hbm,
                   q_out, kn_out, vn_out, own_out, first_out, mid_out, last_out,
                   hbuf, scale, msg, stats_col, u, wq, wkv, wg, wu, part, qpart, qrec, kvpart, kvrec, qsum, qall,
                   load_sem, h_send, h_recv, m_send, m_recv, x_send, x_recv, f_send, f_recv, a_send, a_recv, o_sem, go_sem):
    px, py = lax.axis_index('tpx'), lax.axis_index('tpy')
    me = px * 4 + py
    mate = py + 1 - 2 * lax.rem(py, 2)
    across = lax.rem(py + 2, 4)
    n_seq = 32

    loads = [
        pltpu.make_async_copy(h_hbm, hbuf.at[py], load_sem.at[0]),
        pltpu.make_async_copy(scale_hbm, scale, load_sem.at[1]),
        pltpu.make_async_copy(wk_hbm, wkv.at[:, pl.ds(0, 256)], load_sem.at[2]),
        pltpu.make_async_copy(wv_hbm, wkv.at[:, pl.ds(256, 256)], load_sem.at[3]),
        pltpu.make_async_copy(wq_hbm, wq, load_sem.at[4]),
        pltpu.make_async_copy(wg_hbm, wg, load_sem.at[5]),
        pltpu.make_async_copy(wu_hbm, wu, load_sem.at[6]),
    ]
    for copy in loads[:2]:
        copy.start()
    greet(others(px, py))
    for copy in loads[2:]:
        copy.start()
    loads[0].wait()
    met(7)
    far = pl.ds(pl.multiple_of((1 - px) * 128, 128), 128)
    near = pl.ds(pl.multiple_of(px * 128, 128), 128)

    def h_copy(block, rows, at, qy):
        return remote(hbuf.at[block, rows], hbuf.at[block, rows], h_send.at[at], h_recv.at[at], px, qy)

    to_across = [h_copy(py, far, 0, across), h_copy(py, near, 1, across)]
    to_mate = [h_copy(py, far, 2, mate), h_copy(py, near, 3, mate)]
    relays = [h_copy(across, far, 4, mate), h_copy(across, near, 5, mate)]
    to_across[0].start()
    to_mate[0].start()

    hf = hbuf[py].astype(F32)
    mean = jnp.sum(hf, axis=1, keepdims=True) * (1.0 / 256.0)
    dev = hf - mean
    m2 = jnp.sum(dev * dev, axis=1, keepdims=True)
    lane = lax.broadcasted_iota(jnp.int32, (256, 128), 1)
    stat = jnp.where(lane == 0, mean, m2)
    stat_t = stat.T
    loads[1].wait()
    msg[me] = jnp.concatenate([stat_t[0:2], scale[...], jnp.zeros((5, 256), F32)], axis=0)
    msgs = []
    for i, (qx, qy) in enumerate(others(px, py)):
        copy = remote(msg.at[me], msg.at[me], m_send.at[i], m_recv.at[i], qx, qy)
        copy.start()
        msgs.append(copy)
    to_across[1].start()
    to_mate[1].start()
    to_across[0].wait_recv()
    relays[0].start()
    for copy in msgs:
        copy.wait_recv()

    means = jnp.concatenate([msg[e, 0:1] for e in range(8)], axis=0)
    m2s = jnp.concatenate([msg[e, 1:2] for e in range(8)], axis=0)
    mu = jnp.sum(means, axis=0, keepdims=True) * 0.125
    gap = means - mu
    var = (jnp.sum(m2s, axis=0, keepdims=True) + 256.0 * jnp.sum(gap * gap, axis=0, keepdims=True)) * (1.0 / 2048.0)
    rstd = lax.rsqrt(var + LN_EPS)
    both = jnp.concatenate([mu, rstd, jnp.zeros((126, 256), F32)], axis=0).T
    stats_col[...] = both

    def norm(t, rows):
        cols = pl.ds(pl.multiple_of(t * 256, 256), 256)
        table = stats_col[rows, :]
        u[rows, cols] = ((hbuf[t, rows, :].astype(F32) - table[:, 0:1]) * table[:, 1:2] * msg[px * 4 + t, 2:3]).astype(BF16)

    def gather(i, rows):
        norm(py, rows)
        to_mate[i].wait_recv()
        norm(mate, rows)
        norm(across, rows)
        relays[i].wait_recv()
        norm(lax.rem(mate + 2, 4), rows)

    gather(0, far)
    far_seq = pl.ds(pl.multiple_of((1 - px) * 128 + py * n_seq, n_seq), n_seq)
    near_seq = pl.ds(pl.multiple_of(px * 128 + py * n_seq, n_seq), n_seq)
    loads[2].wait()
    loads[3].wait()
    kvpart[pl.ds(0, n_seq), :] = jnp.dot(u[far_seq, :], wkv[...], preferred_element_type=F32)
    kv_copy = remote(kvpart.at[pl.ds(0, n_seq)], kvrec, x_send.at[1], x_recv.at[1], 1 - px, py)
    kv_copy.start()
    loads[4].wait()
    qpart[far, :] = jnp.dot(u[far, :], wq[...], preferred_element_type=F32)
    q_copy = remote(qpart.at[far], qrec, x_send.at[0], x_recv.at[0], 1 - px, py)
    q_copy.start()
    to_across[1].wait_recv()
    relays[1].start()
    gather(1, near)

    loads[5].wait()
    loads[6].wait()
    step = 512
    n_step = 4096 // step
    n_first, n_mid, n_last = split
    first_rows = pl.ds(pl.multiple_of((1 - px) * 128, 8), n_first)
    mid_rows = pl.ds(pl.multiple_of((1 - px) * 128 + n_first, 8), n_mid)
    last_rows = pl.ds(pl.multiple_of((1 - px) * 128 + n_first + n_mid, 8), n_last)

    def first_copy(i, base):
        cols = pl.ds(pl.multiple_of(base * 4096 + i * step, step), step)
        at = base * n_step + i
        return remote(part.at[first_rows, cols], first_out.at[:, cols], f_send.at[at], f_recv.at[at], 1 - px, py)

    holds = lax.rem(py, 2) == 1
    n_piece = 2 * n_step

    def columns(i, carry):
        cols = pl.ds(pl.multiple_of(i * step, step), step)
        part[:, cols] = jnp.dot(u[...], wg[:, cols], preferred_element_type=F32)
        up_cols = pl.ds(pl.multiple_of(4096 + i * step, step), step)

        @pl.when(jnp.logical_or(jnp.logical_not(holds), 2 * i < n_piece - HELD))
        def _():
            first_copy(i, 0).start()

        part[:, up_cols] = jnp.dot(u[...], wu[:, cols], preferred_element_type=F32)

        @pl.when(jnp.logical_or(jnp.logical_not(holds), 2 * i + 1 < n_piece - HELD))
        def _():
            first_copy(i, 1).start()

        return carry

    lax.fori_loop(0, n_step, columns, 0)
    outs = [
        pltpu.make_async_copy(part.at[near], own_out, o_sem.at[0]),
        pltpu.make_async_copy(part.at[mid_rows], mid_out, o_sem.at[1]),
        pltpu.make_async_copy(part.at[last_rows], last_out, o_sem.at[2]),
    ]
    for copy in outs:
        copy.start()
    qpart[near, :] = jnp.dot(u[near, :], wq[...], preferred_element_type=F32)
    kvpart[pl.ds(n_seq, n_seq), :] = jnp.dot(u[near_seq, :], wkv[...], preferred_element_type=F32)

    q_copy.wait_recv()
    for t in range(4):
        rows_t = pl.ds(pl.multiple_of(px * 128 + t * n_seq, n_seq), n_seq)
        qsum[t] = (qpart[rows_t, :] + qrec[pl.ds(t * n_seq, n_seq), :]).astype(BF16)
    hops = []
    for i in range(1, 4):
        t = lax.rem(py + i, 4)
        copy = remote(qsum.at[t], qall.at[py], a_send.at[i - 1], a_recv.at[i - 1], px, t)
        copy.start()
        hops.append(copy)
    kv_copy.wait_recv()
    kv = (kvpart[pl.ds(n_seq, n_seq), :] + kvrec[...]).astype(BF16).astype(F32)
    kn_out[...] = kv[:, :256]
    vn_out[...] = kv[:, 256:]

    def emit(t, block):
        block = block.astype(F32)
        for j in range(2):
            row = pl.multiple_of((2 * t + j) * n_seq, n_seq)
            for half in range(2):
                q_out[half, pl.ds(row, n_seq), :] = block[:, (2 * j + half) * 128:(2 * j + half + 1) * 128]

    emit(py, qsum[py])
    for i in range(1, 4):
        hops[i - 1].wait_recv()
        t = lax.rem(py + 4 - i, 4)
        emit(t, qall[t])

    for copy in outs:
        copy.wait()
    for copy in to_across + to_mate + relays + msgs + hops + [q_copy, kv_copy]:
        copy.wait_send()

    @pl.when(jnp.logical_not(holds))
    def _():
        first_copy(n_step - 1, 0).wait_send()
        pl.semaphore_signal(go_sem, 1, device_id={'tpx': px, 'tpy': mate}, device_id_type=MESH)

    @pl.when(holds)
    def _():
        pl.semaphore_wait(go_sem, 1)
        for k in range(n_piece - HELD, n_piece):
            first_copy(k // 2, k % 2).start()
        first_copy(n_step - 1, 0).wait_send()

    def settle(i, carry):
        first_copy(i, 0).wait_recv()
        first_copy(i, 1).wait()

        @pl.when(i < n_step - 1)
        def _():
            first_copy(i, 0).wait_send()

        return carry

    lax.fori_loop(0, n_step, settle, 0)


def project(split, hidden, ln_scale, w_q, w_k, w_v, w_gate, w_up):
    any_spec = pl.BlockSpec(memory_space=pl.ANY)
    hbm = pl.BlockSpec(memory_space=pltpu.HBM)
    vmem = pl.BlockSpec(memory_space=pltpu.VMEM)
    sds = jax.ShapeDtypeStruct
    dma = pltpu.SemaphoreType.DMA
    return pl.pallas_call(
        functools.partial(project_kernel, split),
        out_shape=[sds((2, 256, 128), F32), sds((32, 256), F32), sds((32, 256), F32), sds((128, 8192), F32)] + [sds((r, 8192), F32) for r in split],
        in_specs=[hbm] * 7,
        out_specs=[vmem, vmem, vmem] + [any_spec] * 4,
        scratch_shapes=[
            pltpu.VMEM((4, 256, 256), BF16),
            pltpu.VMEM((1, 256), F32),
            pltpu.VMEM((8, 8, 256), F32),
            pltpu.VMEM((256, 128), F32),
            pltpu.VMEM((256, 1024), BF16),
            pltpu.VMEM((1024, 512), BF16),
            pltpu.VMEM((1024, 512), BF16),
            pltpu.VMEM((1024, 4096), BF16),
            pltpu.VMEM((1024, 4096), BF16),
            pltpu.VMEM((256, 8192), F32),
            pltpu.VMEM((256, 512), F32),
            pltpu.VMEM((128, 512), F32),
            pltpu.VMEM((64, 512), F32),
            pltpu.VMEM((32, 512), F32),
            pltpu.VMEM((4, 32, 512), BF16),
            pltpu.VMEM((4, 32, 512), BF16),
            dma((7,)), dma((6,)), dma((6,)), dma((7,)), dma((7,)), dma((2,)), dma((2,)), dma((16,)), dma((16,)), dma((3,)), dma((3,)), dma((3,)), pltpu.SemaphoreType.REGULAR,
        ],
        compiler_params=pltpu.CompilerParams(collective_id=0, has_side_effects=True, vmem_limit_bytes=48 * 2**20),
        cost_estimate=pl.CostEstimate(flops=5_000_000_000, bytes_accessed=28 * 2**20, transcendentals=0),
        name="project",
    )(*[pltpu.with_memory_space_constraint(x, pltpu.HBM) for x in (hidden, ln_scale.reshape(1, 256), w_q, w_k, w_v, w_gate, w_up)])


def attend_kernel(pos_ref, q_in, kn_in, vn_ref, cos_ref, sin_ref, k_hbm, v_hbm, k_out, v_out, o_ref, kbuf, vbuf, q_ref, kn_ref, k_in, v_in, k_wr, v_wr):
    n_seq, cache_len, head_dim = k_hbm.shape

    def fetch(b):
        slot = lax.rem(b, RING)
        return (pltpu.make_async_copy(k_hbm.at[b], kbuf.at[slot], k_in.at[slot]),
                pltpu.make_async_copy(v_hbm.at[b], vbuf.at[slot], v_in.at[slot]))

    def drain(b):
        slot = lax.rem(b, RING)
        return (pltpu.make_async_copy(kbuf.at[slot], k_out.at[b], k_wr.at[slot]),
                pltpu.make_async_copy(vbuf.at[slot], v_out.at[b], v_wr.at[slot]))

    for b in range(AHEAD):
        for copy in fetch(b):
            copy.start()

    cos_tab, sin_tab = cos_ref[...], sin_ref[...]
    kn_ref[...] = rotate(kn_in[...], cos_tab, sin_tab).astype(BF16).astype(F32)
    for h in range(8):
        rows = pl.ds(h * n_seq, n_seq)
        lead, tail = q_in[0, rows, :], q_in[1, rows, :]
        q_ref[0, rows, :] = (lead * cos_tab - tail * sin_tab).astype(BF16).astype(F32)
        q_ref[1, rows, :] = (lead * sin_tab + tail * cos_tab).astype(BF16).astype(F32)

    def patch(buf, slot, row, p):
        base = pl.multiple_of((p // 16) * 16, 16)
        tile = buf[slot, pl.ds(base, 16), :]
        hit = lax.broadcasted_iota(jnp.int32, (16, head_dim), 0) == p - base
        buf[slot, pl.ds(base, 16), :] = jnp.where(hit, row, tile.astype(F32)).astype(BF16)

    def one(b, carry):
        slot = lax.rem(b, RING)
        p = pos_ref[b]

        @pl.when(b + AHEAD < n_seq)
        def _():
            @pl.when(b + AHEAD >= RING)
            def _():
                for copy in drain(b + AHEAD - RING):
                    copy.wait()
            for copy in fetch(b + AHEAD):
                copy.start()

        k_copy, v_copy = fetch(b)
        k_save, v_save = drain(b)
        k_copy.wait()
        patch(kbuf, slot, kn_ref[pl.ds(b, 1), :], p)
        k_save.start()
        heads = pl.ds(b, 8, stride=n_seq)
        q = jnp.concatenate([q_ref[0, heads, :], q_ref[1, heads, :]], axis=1).astype(BF16)
        scores = lax.dot_general(q, kbuf[slot], (((1,), (1,)), ((), ())), preferred_element_type=F32) * (head_dim ** -0.5)
        valid = lax.broadcasted_iota(jnp.int32, scores.shape, 1) <= p
        scores = jnp.where(valid, scores, -jnp.inf)
        top = jnp.max(scores, axis=1, keepdims=True)
        e = jnp.exp(scores - top)
        prob = (e / jnp.sum(e, axis=1, keepdims=True)).astype(BF16)
        v_copy.wait()
        patch(vbuf, slot, vn_ref[pl.ds(b, 1), :], p)
        v_save.start()
        out = jnp.dot(prob, vbuf[slot], preferred_element_type=F32)
        o_ref[0, heads, :] = out[:, :128]
        o_ref[1, heads, :] = out[:, 128:]
        return carry

    lax.fori_loop(0, n_seq, one, 0)
    for b in range(n_seq - RING, n_seq):
        for copy in drain(b):
            copy.wait()


def attend(positions, q, kn, vn, cos_tab, sin_tab, k_cache, v_cache):
    any_spec = pl.BlockSpec(memory_space=pl.ANY)
    vmem = pl.BlockSpec(memory_space=pltpu.VMEM)
    n_seq, cache_len, head_dim = k_cache.shape
    dma = pltpu.SemaphoreType.DMA
    return pl.pallas_call(
        attend_kernel,
        out_shape=[jax.ShapeDtypeStruct(k_cache.shape, BF16), jax.ShapeDtypeStruct(v_cache.shape, BF16), jax.ShapeDtypeStruct((2, 256, 128), F32)],
        in_specs=[pl.BlockSpec(memory_space=pltpu.SMEM), vmem, vmem, vmem, vmem, vmem, any_spec, any_spec],
        out_specs=[any_spec, any_spec, vmem],
        scratch_shapes=[
            pltpu.VMEM((RING, cache_len, head_dim), BF16),
            pltpu.VMEM((RING, cache_len, head_dim), BF16),
            pltpu.VMEM((2, 256, 128), F32),
            pltpu.VMEM((n_seq, head_dim), F32),
            dma((RING,)), dma((RING,)), dma((RING,)), dma((RING,)),
        ],
        compiler_params=pltpu.CompilerParams(vmem_limit_bytes=48 * 2**20),
        cost_estimate=pl.CostEstimate(flops=100_000_000_000, bytes_accessed=128 * 2**20, transcendentals=0),
        name="attend",
    )(positions, q, kn, vn, cos_tab, sin_tab, k_cache, v_cache)


def combine_kernel(split, cuts, pieces, h_hbm, attn_ref, wo_hbm, wd_hbm, own_hbm, first_ref, mid_ref, last_ref,
                   out_ref, h, wo, wd, own, got, act, a_snd, a_rcv, res, res_rcv,
                   load_sem, l_send, l_recv, t_send, t_recv, g_send, g_recv, r_send, r_recv):
    px, py = lax.axis_index('tpx'), lax.axis_index('tpy')
    me = px * 4 + py
    n = len(cuts)
    starts = [sum(cuts[:c]) for c in range(n)]
    n_first, n_mid, n_last = split
    late = n_first + n_mid
    mate = py + 1 - 2 * lax.rem(py, 2)
    order = [lax.rem(py + 2, 4), lax.rem(mate + 2, 4), mate, py]
    leads = lax.rem(py, 2) == 0
    greet([(px, order[0]), (1 - px, py)])
    loads = [
        pltpu.make_async_copy(own_hbm, own, load_sem.at[0]),
        pltpu.make_async_copy(wo_hbm, wo, load_sem.at[1]),
        pltpu.make_async_copy(wd_hbm, wd, load_sem.at[2]),
        pltpu.make_async_copy(h_hbm, h, load_sem.at[3]),
    ]
    for copy in loads:
        copy.start()
    for t in range(4):
        for j in range(2):
            at = pl.ds((2 * t + j) * 32, 32)
            a_snd[t, j] = jnp.concatenate([attn_ref[0, at, :], attn_ref[1, at, :]], axis=1).astype(BF16)

    @pl.when(leads)
    def _():
        met(2)
        greet([(px, mate)])

    @pl.when(jnp.logical_not(leads))
    def _():
        met(3)
        greet([(px, mate)])

    lasts = {}
    for c in range(n):
        if starts[c] >= late:
            seg = pl.ds(starts[c] - late, cuts[c])
            lasts[c] = remote(last_ref.at[seg], got.at[seg], l_send.at[c], l_recv.at[c], 1 - px, py)
            lasts[c].start()
    rows_me = pl.ds(pl.multiple_of(me * 32, 32), 32)
    swaps = []
    for i in range(3):
        swaps.append(remote(a_snd.at[order[i]], a_rcv.at[:, rows_me, :], t_send.at[i], t_recv.at[i], px, order[i]))
    swaps[0].start()
    for j in range(2):
        a_rcv[j, rows_me, :] = a_snd[py, j]

    def activate(c):
        here = pl.ds(starts[c], cuts[c])
        if starts[c] < n_first:
            theirs, there = first_ref, here
        elif starts[c] < late:
            theirs, there = mid_ref, pl.ds(starts[c] - n_first, cuts[c])
        else:
            theirs, there = got, pl.ds(starts[c] - late, cuts[c])

        n_piece = pieces[c]
        width = 4096 // n_piece

        def piece(k):
            cols = pl.ds(pl.multiple_of(k * width, width), width)
            return remote(act.at[pl.ds(2 * starts[c], cuts[c]), cols], act.at[pl.ds(2 * starts[c] + cuts[c], cuts[c]), cols],
                          g_send.at[sum(pieces[:c]) + k], g_recv.at[sum(pieces[:c]) + k], 1 - px, py)

        def cols(k, carry):
            for i in range(width // 512):
                g_cols = pl.ds(pl.multiple_of(k * width + i * 512, 512), 512)
                u_cols = pl.ds(pl.multiple_of(4096 + k * width + i * 512, 512), 512)
                gate = (own[here, g_cols] + theirs[there, g_cols]).astype(BF16).astype(F32)
                up = (own[here, u_cols] + theirs[there, u_cols]).astype(BF16).astype(F32)
                act[pl.ds(2 * starts[c], cuts[c]), g_cols] = (jax.nn.silu(gate) * up).astype(BF16)
            piece(k).start()
            return carry

        lax.fori_loop(0, n_piece, cols, 0)
        return piece

    loads[0].wait()
    gathers = [activate(0)]

    @pl.when(leads)
    def _():
        met(1)

    swaps[1].start()
    swaps[2].start()
    for copy in swaps:
        copy.wait_recv()
    near = pl.ds(pl.multiple_of(px * 128, 128), 128)
    a_copy = remote(a_rcv.at[:, near, :], a_rcv.at[:, near, :], t_send.at[3], t_recv.at[3], 1 - px, py)
    a_copy.start()
    gathers += [activate(c) for c in range(1, n) if starts[c] < late]

    loads[1].wait()
    a_copy.wait_recv()
    for c in range(n):
        for side in range(2):
            at = pl.ds(pl.multiple_of(lax.rem(px + side, 2) * 128 + starts[c], 16), cuts[c])
            for t in range(4):
                cols = pl.ds(t * 256, 256)
                res[t, pl.ds(2 * starts[c] + side * cuts[c], cuts[c]), :] = (
                    jnp.dot(a_rcv[0, at, :], wo[pl.ds(0, 256), cols], preferred_element_type=F32)
                    + jnp.dot(a_rcv[1, at, :], wo[pl.ds(256, 256), cols], preferred_element_type=F32))
    for c in lasts:
        lasts[c].wait_recv()
        gathers.append(activate(c))

    loads[2].wait()
    loads[3].wait()
    reduces = []

    def finish(c):
        seg = pl.ds(2 * starts[c], 2 * cuts[c])
        total = res[py, seg, :]
        for i in range(3):
            reduces[c][i].wait_recv()
            total = total + res_rcv[order[i], seg, :]
        for side in range(2):
            at = pl.ds(pl.multiple_of(lax.rem(px + side, 2) * 128 + starts[c], 16), cuts[c])
            out_ref[at, :] = (h[at, :].astype(F32) + total[side * cuts[c]:(side + 1) * cuts[c]]).astype(BF16)

    for c in range(n):
        seg = pl.ds(2 * starts[c], 2 * cuts[c])
        hops = []
        parts = pieces[c]
        depth = 4096 // parts
        for p in range(parts):
            gathers[c](p).wait_recv()
            deep = pl.ds(p * depth, depth)
            if p < parts - 1:
                term = jnp.dot(act[seg, deep], wd[deep, :], preferred_element_type=F32)
                for t in range(4):
                    res[t, seg, :] += term[:, t * 256:(t + 1) * 256]
                continue
            for side in range(2):
                pair = lax.rem(py // 2 + 1 + side, 2)
                cols = pl.ds(pl.multiple_of(pair * 512, 512), 512)
                term = jnp.dot(act[seg, deep], wd[deep, cols], preferred_element_type=F32)
                res[2 * pair, seg, :] += term[:, :256]
                res[2 * pair + 1, seg, :] += term[:, 256:]
                for i in ((0, 1), (2,))[side]:
                    copy = remote(res.at[order[i], seg], res_rcv.at[py, seg], r_send.at[3 * c + i], r_recv.at[3 * c + i], px, order[i])
                    copy.start()
                    hops.append(copy)
        reduces.append(hops)
        if c > 0:
            finish(c - 1)
    finish(n - 1)

    for copy in swaps + [a_copy] + list(lasts.values()) + [x for hops in reduces for x in hops]:
        copy.wait_send()
    for c in range(n):
        for k in range(pieces[c]):
            gathers[c](k).wait_send()


def combine(split, cuts, pieces, hidden, attn, w_o, w_down, own, first, mid, last):
    any_spec = pl.BlockSpec(memory_space=pl.ANY)
    hbm = pl.BlockSpec(memory_space=pltpu.HBM)
    vmem = pl.BlockSpec(memory_space=pltpu.VMEM)
    dma = pltpu.SemaphoreType.DMA
    n = len(cuts)
    return pl.pallas_call(
        functools.partial(combine_kernel, split, cuts, pieces),
        out_shape=jax.ShapeDtypeStruct((256, 256), BF16),
        in_specs=[hbm, vmem, hbm, hbm, any_spec, vmem, vmem, vmem],
        out_specs=vmem,
        scratch_shapes=[
            pltpu.VMEM((256, 256), BF16),
            pltpu.VMEM((512, 1024), BF16),
            pltpu.VMEM((4096, 1024), BF16),
            pltpu.VMEM((128, 8192), F32),
            pltpu.VMEM((split[2], 8192), F32),
            pltpu.VMEM((256, 4096), BF16),
            pltpu.VMEM((4, 2, 32, 256), BF16),
            pltpu.VMEM((2, 256, 256), BF16),
            pltpu.VMEM((4, 256, 256), F32),
            pltpu.VMEM((4, 256, 256), F32),
            dma((4,)), dma((n,)), dma((n,)), dma((4,)), dma((4,)), dma((sum(pieces),)), dma((sum(pieces),)), dma((3 * n,)), dma((3 * n,)),
        ],
        compiler_params=pltpu.CompilerParams(collective_id=1, has_side_effects=True, vmem_limit_bytes=48 * 2**20),
        cost_estimate=pl.CostEstimate(flops=3_000_000_000, bytes_accessed=18 * 2**20, transcendentals=0),
        name="combine",
    )(hidden, attn, w_o, w_down, own, first, mid, last)


def solution(mesh):
    hidden_spec = P('dp', ('tpx', 'tpy'))
    cache_spec = P(('dp', 'tpx', 'tpy'), None, None)
    in_specs = (hidden_spec, P(('tpx', 'tpy')), P('tpx', 'tpy'), P('tpx', None), P('tpx', None), P('tpx', 'tpy'), P('tpx', 'tpy'), P('tpy', 'tpx'), P('tpy', 'tpx'), cache_spec, cache_spec, P(('dp', 'tpx', 'tpy')))
    out_specs = (hidden_spec, cache_spec, cache_spec)
    split, cuts, pieces = (48, 64, 16), (48, 32, 32, 16), (1, 1, 4, 4)
    swap = [(0, 1), (1, 0)]

    def device_step(hidden, ln_scale, w_q, w_k, w_v, w_gate, w_up, w_o, w_down, k_cache, v_cache, positions):
        q, kn, vn, own, first, mid, last = project(split, hidden, ln_scale, w_q, w_k, w_v, w_gate, w_up)
        mid = lax.ppermute(mid, 'tpx', swap)
        late_pos, kn = lax.optimization_barrier((positions, kn))
        cos_tab, sin_tab = rope_tables(late_pos, k_cache.shape[2])
        k_all, v_all, attn = attend(positions, q, kn, vn, cos_tab, sin_tab, k_cache, v_cache)
        hidden_out = combine(split, cuts, pieces, hidden, attn, w_o, w_down, own, first, mid, last)
        return hidden_out, k_all, v_all

    return jax.shard_map(device_step, mesh=mesh, in_specs=in_specs, out_specs=out_specs, check_vma=False)
```

```python
import functools
import jax
import jax.numpy as jnp
from jax import lax
from jax.experimental import pallas as pl
from jax.experimental.pallas import tpu as pltpu
from jax.sharding import PartitionSpec as P

LN_EPS = 1e-6
ROPE_BASE = 10000.0
MESH = pl.DeviceIdType.MESH
F32 = jnp.float32
BF16 = jnp.bfloat16
RING = 8
AHEAD = 4
HELD = 5


def rope_tables(positions, head_dim):
    half_dim = head_dim // 2
    inv_freq = ROPE_BASE ** (-(jnp.arange(half_dim, dtype=F32) * 2.0 / head_dim))
    angles = positions.astype(F32)[:, None] * inv_freq[None, :]
    return jnp.cos(angles), jnp.sin(angles)


def rotate(x, cos_tab, sin_tab):
    half = x.shape[-1] // 2
    lead, tail = x[:, :half], x[:, half:]
    return jnp.concatenate([lead * cos_tab - tail * sin_tab, lead * sin_tab + tail * cos_tab], axis=-1)


def others(px, py):
    return [(lax.rem(px + dx, 2), lax.rem(py + dy, 4)) for dx in range(2) for dy in range(4) if (dx, dy) != (0, 0)]


def greet(peers):
    barrier = pltpu.get_barrier_semaphore()
    for qx, qy in peers:
        pl.semaphore_signal(barrier, 1, device_id={'tpx': qx, 'tpy': qy}, device_id_type=MESH)


def met(count):
    pl.semaphore_wait(pltpu.get_barrier_semaphore(), count)


def remote(src, dst, send_sem, recv_sem, qx, qy):
    return pltpu.make_async_remote_copy(src, dst, send_sem, recv_sem, device_id={'tpx': qx, 'tpy': qy}, device_id_type=MESH)


def project_kernel(split, h_hbm, scale_hbm, wq_hbm, wk_hbm, wv_hbm, wg_hbm, wu_hbm,
                   q_out, kn_out, vn_out, own_out, first_out, mid_out, last_out,
                   hbuf, scale, msg, stats_col, u, wq, wkv, wg, wu, part, qpart, qrec, kvpart, kvrec, qsum, qall,
                   load_sem, h_send, h_recv, m_send, m_recv, x_send, x_recv, f_send, f_recv, a_send, a_recv, o_sem, go_sem):
    px, py = lax.axis_index('tpx'), lax.axis_index('tpy')
    me = px * 4 + py
    mate = py + 1 - 2 * lax.rem(py, 2)
    across = lax.rem(py + 2, 4)
    n_seq = 32

    loads = [
        pltpu.make_async_copy(h_hbm, hbuf.at[py], load_sem.at[0]),
        pltpu.make_async_copy(scale_hbm, scale, load_sem.at[1]),
        pltpu.make_async_copy(wk_hbm, wkv.at[:, pl.ds(0, 256)], load_sem.at[2]),
        pltpu.make_async_copy(wv_hbm, wkv.at[:, pl.ds(256, 256)], load_sem.at[3]),
        pltpu.make_async_copy(wq_hbm, wq, load_sem.at[4]),
        pltpu.make_async_copy(wg_hbm, wg, load_sem.at[5]),
        pltpu.make_async_copy(wu_hbm, wu, load_sem.at[6]),
    ]
    for copy in loads[:2]:
        copy.start()
    greet(others(px, py))
    for copy in loads[2:]:
        copy.start()
    loads[0].wait()
    met(7)
    far = pl.ds(pl.multiple_of((1 - px) * 128, 128), 128)
    near = pl.ds(pl.multiple_of(px * 128, 128), 128)

    def h_copy(block, rows, at, qy):
        return remote(hbuf.at[block, rows], hbuf.at[block, rows], h_send.at[at], h_recv.at[at], px, qy)

    to_across = [h_copy(py, far, 0, across), h_copy(py, near, 1, across)]
    to_mate = [h_copy(py, far, 2, mate), h_copy(py, near, 3, mate)]
    relays = [h_copy(across, far, 4, mate), h_copy(across, near, 5, mate)]
    to_across[0].start()
    to_mate[0].start()

    hf = hbuf[py].astype(F32)
    mean = jnp.sum(hf, axis=1, keepdims=True) * (1.0 / 256.0)
    dev = hf - mean
    m2 = jnp.sum(dev * dev, axis=1, keepdims=True)
    lane = lax.broadcasted_iota(jnp.int32, (256, 128), 1)
    stat = jnp.where(lane == 0, mean, m2)
    stat_t = stat.T
    loads[1].wait()
    msg[me] = jnp.concatenate([stat_t[0:2], scale[...], jnp.zeros((5, 256), F32)], axis=0)
    msgs = []
    for i, (qx, qy) in enumerate(others(px, py)):
        copy = remote(msg.at[me], msg.at[me], m_send.at[i], m_recv.at[i], qx, qy)
        copy.start()
        msgs.append(copy)
    to_across[1].start()
    to_mate[1].start()
    to_across[0].wait_recv()
    relays[0].start()
    for copy in msgs:
        copy.wait_recv()

    means = jnp.concatenate([msg[e, 0:1] for e in range(8)], axis=0)
    m2s = jnp.concatenate([msg[e, 1:2] for e in range(8)], axis=0)
    mu = jnp.sum(means, axis=0, keepdims=True) * 0.125
    gap = means - mu
    var = (jnp.sum(m2s, axis=0, keepdims=True) + 256.0 * jnp.sum(gap * gap, axis=0, keepdims=True)) * (1.0 / 2048.0)
    rstd = lax.rsqrt(var + LN_EPS)
    both = jnp.concatenate([mu, rstd, jnp.zeros((126, 256), F32)], axis=0).T
    stats_col[...] = both

    def norm(t, rows):
        cols = pl.ds(pl.multiple_of(t * 256, 256), 256)
        table = stats_col[rows, :]
        u[rows, cols] = ((hbuf[t, rows, :].astype(F32) - table[:, 0:1]) * table[:, 1:2] * msg[px * 4 + t, 2:3]).astype(BF16)

    def gather(i, rows):
        norm(py, rows)
        norm(across, rows)
        to_mate[i].wait_recv()
        norm(mate, rows)
        relays[i].wait_recv()
        norm(lax.rem(mate + 2, 4), rows)

    far_seq = pl.ds(pl.multiple_of((1 - px) * 128 + py * n_seq, n_seq), n_seq)
    near_seq = pl.ds(pl.multiple_of(px * 128 + py * n_seq, n_seq), n_seq)
    loads[2].wait()
    loads[3].wait()
    gather(0, far_seq)
    kvpart[pl.ds(0, n_seq), :] = jnp.dot(u[far_seq, :], wkv[...], preferred_element_type=F32)
    kv_copy = remote(kvpart.at[pl.ds(0, n_seq)], kvrec, x_send.at[1], x_recv.at[1], 1 - px, py)
    kv_copy.start()
    for t in range(4):
        norm(t, far)
    loads[4].wait()
    qpart[far, :] = jnp.dot(u[far, :], wq[...], preferred_element_type=F32)
    q_copy = remote(qpart.at[far], qrec, x_send.at[0], x_recv.at[0], 1 - px, py)
    q_copy.start()
    to_across[1].wait_recv()
    relays[1].start()
    gather(1, near)

    loads[5].wait()
    loads[6].wait()
    step = 512
    n_step = 4096 // step
    n_first, n_mid, n_last = split
    first_rows = pl.ds(pl.multiple_of((1 - px) * 128, 8), n_first)
    mid_rows = pl.ds(pl.multiple_of((1 - px) * 128 + n_first, 8), n_mid)
    last_rows = pl.ds(pl.multiple_of((1 - px) * 128 + n_first + n_mid, 8), n_last)

    def first_copy(i, base):
        cols = pl.ds(pl.multiple_of(base * 4096 + i * step, step), step)
        at = base * n_step + i
        return remote(part.at[first_rows, cols], first_out.at[:, cols], f_send.at[at], f_recv.at[at], 1 - px, py)

    holds = lax.rem(py, 2) == 1
    n_piece = 2 * n_step

    def columns(i, carry):
        cols = pl.ds(pl.multiple_of(i * step, step), step)
        part[:, cols] = jnp.dot(u[...], wg[:, cols], preferred_element_type=F32)
        up_cols = pl.ds(pl.multiple_of(4096 + i * step, step), step)

        @pl.when(jnp.logical_or(jnp.logical_not(holds), 2 * i < n_piece - HELD))
        def _():
            first_copy(i, 0).start()

        part[:, up_cols] = jnp.dot(u[...], wu[:, cols], preferred_element_type=F32)

        @pl.when(jnp.logical_or(jnp.logical_not(holds), 2 * i + 1 < n_piece - HELD))
        def _():
            first_copy(i, 1).start()

        return carry

    lax.fori_loop(0, n_step, columns, 0)
    outs = [
        pltpu.make_async_copy(part.at[near], own_out, o_sem.at[0]),
        pltpu.make_async_copy(part.at[mid_rows], mid_out, o_sem.at[1]),
        pltpu.make_async_copy(part.at[last_rows], last_out, o_sem.at[2]),
    ]
    for copy in outs:
        copy.start()
    qpart[near, :] = jnp.dot(u[near, :], wq[...], preferred_element_type=F32)
    kvpart[pl.ds(n_seq, n_seq), :] = jnp.dot(u[near_seq, :], wkv[...], preferred_element_type=F32)

    q_copy.wait_recv()
    for t in range(4):
        rows_t = pl.ds(pl.multiple_of(px * 128 + t * n_seq, n_seq), n_seq)
        qsum[t] = (qpart[rows_t, :] + qrec[pl.ds(t * n_seq, n_seq), :]).astype(BF16)
    hops = []
    for i in range(1, 4):
        t = lax.rem(py + i, 4)
        copy = remote(qsum.at[t], qall.at[py], a_send.at[i - 1], a_recv.at[i - 1], px, t)
        copy.start()
        hops.append(copy)
    kv_copy.wait_recv()
    kv = (kvpart[pl.ds(n_seq, n_seq), :] + kvrec[...]).astype(BF16).astype(F32)
    kn_out[...] = kv[:, :256]
    vn_out[...] = kv[:, 256:]

    def emit(t, block):
        block = block.astype(F32)
        for j in range(2):
            row = pl.multiple_of((2 * t + j) * n_seq, n_seq)
            for half in range(2):
                q_out[half, pl.ds(row, n_seq), :] = block[:, (2 * j + half) * 128:(2 * j + half + 1) * 128]

    emit(py, qsum[py])
    for i in range(1, 4):
        hops[i - 1].wait_recv()
        t = lax.rem(py + 4 - i, 4)
        emit(t, qall[t])

    for copy in outs:
        copy.wait()
    for copy in to_across + to_mate + relays + msgs + hops + [q_copy, kv_copy]:
        copy.wait_send()

    @pl.when(jnp.logical_not(holds))
    def _():
        first_copy(n_step - 1, 0).wait_send()
        pl.semaphore_signal(go_sem, 1, device_id={'tpx': px, 'tpy': mate}, device_id_type=MESH)

    @pl.when(holds)
    def _():
        pl.semaphore_wait(go_sem, 1)
        for k in range(n_piece - HELD, n_piece):
            first_copy(k // 2, k % 2).start()
        first_copy(n_step - 1, 0).wait_send()

    def settle(i, carry):
        first_copy(i, 0).wait_recv()
        first_copy(i, 1).wait()

        @pl.when(i < n_step - 1)
        def _():
            first_copy(i, 0).wait_send()

        return carry

    lax.fori_loop(0, n_step, settle, 0)


def project(split, hidden, ln_scale, w_q, w_k, w_v, w_gate, w_up):
    any_spec = pl.BlockSpec(memory_space=pl.ANY)
    hbm = pl.BlockSpec(memory_space=pltpu.HBM)
    vmem = pl.BlockSpec(memory_space=pltpu.VMEM)
    sds = jax.ShapeDtypeStruct
    dma = pltpu.SemaphoreType.DMA
    return pl.pallas_call(
        functools.partial(project_kernel, split),
        out_shape=[sds((2, 256, 128), F32), sds((32, 256), F32), sds((32, 256), F32), sds((128, 8192), F32)] + [sds((r, 8192), F32) for r in split],
        in_specs=[hbm] * 7,
        out_specs=[vmem, vmem, vmem] + [any_spec] * 4,
        scratch_shapes=[
            pltpu.VMEM((4, 256, 256), BF16),
            pltpu.VMEM((1, 256), F32),
            pltpu.VMEM((8, 8, 256), F32),
            pltpu.VMEM((256, 128), F32),
            pltpu.VMEM((256, 1024), BF16),
            pltpu.VMEM((1024, 512), BF16),
            pltpu.VMEM((1024, 512), BF16),
            pltpu.VMEM((1024, 4096), BF16),
            pltpu.VMEM((1024, 4096), BF16),
            pltpu.VMEM((256, 8192), F32),
            pltpu.VMEM((256, 512), F32),
            pltpu.VMEM((128, 512), F32),
            pltpu.VMEM((64, 512), F32),
            pltpu.VMEM((32, 512), F32),
            pltpu.VMEM((4, 32, 512), BF16),
            pltpu.VMEM((4, 32, 512), BF16),
            dma((7,)), dma((6,)), dma((6,)), dma((7,)), dma((7,)), dma((2,)), dma((2,)), dma((16,)), dma((16,)), dma((3,)), dma((3,)), dma((3,)), pltpu.SemaphoreType.REGULAR,
        ],
        compiler_params=pltpu.CompilerParams(collective_id=0, has_side_effects=True, vmem_limit_bytes=48 * 2**20),
        cost_estimate=pl.CostEstimate(flops=5_000_000_000, bytes_accessed=28 * 2**20, transcendentals=0),
        name="project",
    )(*[pltpu.with_memory_space_constraint(x, pltpu.HBM) for x in (hidden, ln_scale.reshape(1, 256), w_q, w_k, w_v, w_gate, w_up)])


def attend_kernel(pos_ref, q_in, kn_in, vn_ref, cos_ref, sin_ref, k_hbm, v_hbm, k_out, v_out, o_ref, kbuf, vbuf, q_ref, kn_ref, k_in, v_in, k_wr, v_wr):
    n_seq, cache_len, head_dim = k_hbm.shape

    def fetch(b):
        slot = lax.rem(b, RING)
        return (pltpu.make_async_copy(k_hbm.at[b], kbuf.at[slot], k_in.at[slot]),
                pltpu.make_async_copy(v_hbm.at[b], vbuf.at[slot], v_in.at[slot]))

    def drain(b):
        slot = lax.rem(b, RING)
        return (pltpu.make_async_copy(kbuf.at[slot], k_out.at[b], k_wr.at[slot]),
                pltpu.make_async_copy(vbuf.at[slot], v_out.at[b], v_wr.at[slot]))

    for b in range(AHEAD):
        for copy in fetch(b):
            copy.start()

    cos_tab, sin_tab = cos_ref[...], sin_ref[...]
    kn_ref[...] = rotate(kn_in[...], cos_tab, sin_tab).astype(BF16).astype(F32)
    for h in range(8):
        rows = pl.ds(h * n_seq, n_seq)
        lead, tail = q_in[0, rows, :], q_in[1, rows, :]
        q_ref[0, rows, :] = (lead * cos_tab - tail * sin_tab).astype(BF16).astype(F32)
        q_ref[1, rows, :] = (lead * sin_tab + tail * cos_tab).astype(BF16).astype(F32)

    def patch(buf, slot, row, p):
        base = pl.multiple_of((p // 16) * 16, 16)
        tile = buf[slot, pl.ds(base, 16), :]
        hit = lax.broadcasted_iota(jnp.int32, (16, head_dim), 0) == p - base
        buf[slot, pl.ds(base, 16), :] = jnp.where(hit, row, tile.astype(F32)).astype(BF16)

    def one(b, carry):
        slot = lax.rem(b, RING)
        p = pos_ref[b]

        @pl.when(b + AHEAD < n_seq)
        def _():
            @pl.when(b + AHEAD >= RING)
            def _():
                for copy in drain(b + AHEAD - RING):
                    copy.wait()
            for copy in fetch(b + AHEAD):
                copy.start()

        k_copy, v_copy = fetch(b)
        k_save, v_save = drain(b)
        k_copy.wait()
        patch(kbuf, slot, kn_ref[pl.ds(b, 1), :], p)
        k_save.start()
        heads = pl.ds(b, 8, stride=n_seq)
        q = jnp.concatenate([q_ref[0, heads, :], q_ref[1, heads, :]], axis=1).astype(BF16)
        scores = lax.dot_general(q, kbuf[slot], (((1,), (1,)), ((), ())), preferred_element_type=F32) * (head_dim ** -0.5)
        valid = lax.broadcasted_iota(jnp.int32, scores.shape, 1) <= p
        scores = jnp.where(valid, scores, -jnp.inf)
        top = jnp.max(scores, axis=1, keepdims=True)
        e = jnp.exp(scores - top)
        prob = (e / jnp.sum(e, axis=1, keepdims=True)).astype(BF16)
        v_copy.wait()
        patch(vbuf, slot, vn_ref[pl.ds(b, 1), :], p)
        v_save.start()
        out = jnp.dot(prob, vbuf[slot], preferred_element_type=F32)
        o_ref[0, heads, :] = out[:, :128]
        o_ref[1, heads, :] = out[:, 128:]
        return carry

    lax.fori_loop(0, n_seq, one, 0)
    for b in range(n_seq - RING, n_seq):
        for copy in drain(b):
            copy.wait()


def attend(positions, q, kn, vn, cos_tab, sin_tab, k_cache, v_cache):
    any_spec = pl.BlockSpec(memory_space=pl.ANY)
    vmem = pl.BlockSpec(memory_space=pltpu.VMEM)
    n_seq, cache_len, head_dim = k_cache.shape
    dma = pltpu.SemaphoreType.DMA
    return pl.pallas_call(
        attend_kernel,
        out_shape=[jax.ShapeDtypeStruct(k_cache.shape, BF16), jax.ShapeDtypeStruct(v_cache.shape, BF16), jax.ShapeDtypeStruct((2, 256, 128), F32)],
        in_specs=[pl.BlockSpec(memory_space=pltpu.SMEM), vmem, vmem, vmem, vmem, vmem, any_spec, any_spec],
        out_specs=[any_spec, any_spec, vmem],
        scratch_shapes=[
            pltpu.VMEM((RING, cache_len, head_dim), BF16),
            pltpu.VMEM((RING, cache_len, head_dim), BF16),
            pltpu.VMEM((2, 256, 128), F32),
            pltpu.VMEM((n_seq, head_dim), F32),
            dma((RING,)), dma((RING,)), dma((RING,)), dma((RING,)),
        ],
        compiler_params=pltpu.CompilerParams(vmem_limit_bytes=48 * 2**20),
        cost_estimate=pl.CostEstimate(flops=100_000_000_000, bytes_accessed=128 * 2**20, transcendentals=0),
        name="attend",
    )(positions, q, kn, vn, cos_tab, sin_tab, k_cache, v_cache)


def combine_kernel(split, cuts, pieces, h_hbm, attn_ref, wo_hbm, wd_hbm, own_hbm, first_ref, mid_ref, last_ref,
                   out_ref, h, wo, wd, own, got, act, a_snd, a_rcv, res, res_rcv,
                   load_sem, l_send, l_recv, t_send, t_recv, g_send, g_recv, r_send, r_recv):
    px, py = lax.axis_index('tpx'), lax.axis_index('tpy')
    me = px * 4 + py
    n = len(cuts)
    starts = [sum(cuts[:c]) for c in range(n)]
    n_first, n_mid, n_last = split
    late = n_first + n_mid
    mate = py + 1 - 2 * lax.rem(py, 2)
    order = [lax.rem(py + 2, 4), lax.rem(mate + 2, 4), mate, py]
    leads = lax.rem(py, 2) == 0
    greet([(px, order[0]), (1 - px, py)])
    loads = [
        pltpu.make_async_copy(own_hbm, own, load_sem.at[0]),
        pltpu.make_async_copy(wo_hbm, wo, load_sem.at[1]),
        pltpu.make_async_copy(wd_hbm, wd, load_sem.at[2]),
        pltpu.make_async_copy(h_hbm, h, load_sem.at[3]),
    ]
    for copy in loads:
        copy.start()
    for t in range(4):
        for j in range(2):
            at = pl.ds((2 * t + j) * 32, 32)
            a_snd[t, j] = jnp.concatenate([attn_ref[0, at, :], attn_ref[1, at, :]], axis=1).astype(BF16)

    @pl.when(leads)
    def _():
        met(2)
        greet([(px, mate)])

    @pl.when(jnp.logical_not(leads))
    def _():
        met(3)
        greet([(px, mate)])

    lasts = {}
    for c in range(n):
        if starts[c] >= late:
            seg = pl.ds(starts[c] - late, cuts[c])
            lasts[c] = remote(last_ref.at[seg], got.at[seg], l_send.at[c], l_recv.at[c], 1 - px, py)
            lasts[c].start()
    rows_me = pl.ds(pl.multiple_of(me * 32, 32), 32)
    swaps = []
    for i in range(3):
        swaps.append(remote(a_snd.at[order[i]], a_rcv.at[:, rows_me, :], t_send.at[i], t_recv.at[i], px, order[i]))
    swaps[0].start()
    for j in range(2):
        a_rcv[j, rows_me, :] = a_snd[py, j]

    def activate(c):
        here = pl.ds(starts[c], cuts[c])
        if starts[c] < n_first:
            theirs, there = first_ref, here
        elif starts[c] < late:
            theirs, there = mid_ref, pl.ds(starts[c] - n_first, cuts[c])
        else:
            theirs, there = got, pl.ds(starts[c] - late, cuts[c])

        n_piece = pieces[c]
        width = 4096 // n_piece

        def piece(k):
            cols = pl.ds(pl.multiple_of(k * width, width), width)
            return remote(act.at[pl.ds(2 * starts[c], cuts[c]), cols], act.at[pl.ds(2 * starts[c] + cuts[c], cuts[c]), cols],
                          g_send.at[sum(pieces[:c]) + k], g_recv.at[sum(pieces[:c]) + k], 1 - px, py)

        def cols(k, carry):
            for i in range(width // 512):
                g_cols = pl.ds(pl.multiple_of(k * width + i * 512, 512), 512)
                u_cols = pl.ds(pl.multiple_of(4096 + k * width + i * 512, 512), 512)
                gate = (own[here, g_cols] + theirs[there, g_cols]).astype(BF16).astype(F32)
                up = (own[here, u_cols] + theirs[there, u_cols]).astype(BF16).astype(F32)
                act[pl.ds(2 * starts[c], cuts[c]), g_cols] = (jax.nn.silu(gate) * up).astype(BF16)
            piece(k).start()
            return carry

        lax.fori_loop(0, n_piece, cols, 0)
        return piece

    loads[0].wait()
    gathers = [activate(0)]

    @pl.when(leads)
    def _():
        met(1)

    swaps[1].start()
    swaps[2].start()
    for copy in swaps:
        copy.wait_recv()
    near = pl.ds(pl.multiple_of(px * 128, 128), 128)
    a_copy = remote(a_rcv.at[:, near, :], a_rcv.at[:, near, :], t_send.at[3], t_recv.at[3], 1 - px, py)
    a_copy.start()
    gathers += [activate(c) for c in range(1, n) if starts[c] < late]

    loads[1].wait()
    a_copy.wait_recv()
    for c in range(n):
        for side in range(2):
            at = pl.ds(pl.multiple_of(lax.rem(px + side, 2) * 128 + starts[c], 16), cuts[c])
            for t in range(4):
                cols = pl.ds(t * 256, 256)
                res[t, pl.ds(2 * starts[c] + side * cuts[c], cuts[c]), :] = (
                    jnp.dot(a_rcv[0, at, :], wo[pl.ds(0, 256), cols], preferred_element_type=F32)
                    + jnp.dot(a_rcv[1, at, :], wo[pl.ds(256, 256), cols], preferred_element_type=F32))
    for c in lasts:
        lasts[c].wait_recv()
        gathers.append(activate(c))

    loads[2].wait()
    loads[3].wait()
    reduces = []

    def finish(c):
        seg = pl.ds(2 * starts[c], 2 * cuts[c])
        total = res[py, seg, :]
        for i in range(3):
            reduces[c][i].wait_recv()
            total = total + res_rcv[order[i], seg, :]
        for side in range(2):
            at = pl.ds(pl.multiple_of(lax.rem(px + side, 2) * 128 + starts[c], 16), cuts[c])
            out_ref[at, :] = (h[at, :].astype(F32) + total[side * cuts[c]:(side + 1) * cuts[c]]).astype(BF16)

    for c in range(n):
        seg = pl.ds(2 * starts[c], 2 * cuts[c])
        hops = []
        parts = pieces[c]
        depth = 4096 // parts
        for p in range(parts):
            gathers[c](p).wait_recv()
            deep = pl.ds(p * depth, depth)
            if p < parts - 1:
                term = jnp.dot(act[seg, deep], wd[deep, :], preferred_element_type=F32)
                for t in range(4):
                    res[t, seg, :] += term[:, t * 256:(t + 1) * 256]
                continue
            for side in range(2):
                pair = lax.rem(py // 2 + 1 + side, 2)
                cols = pl.ds(pl.multiple_of(pair * 512, 512), 512)
                term = jnp.dot(act[seg, deep], wd[deep, cols], preferred_element_type=F32)
                res[2 * pair, seg, :] += term[:, :256]
                res[2 * pair + 1, seg, :] += term[:, 256:]
                for i in ((0, 1), (2,))[side]:
                    copy = remote(res.at[order[i], seg], res_rcv.at[py, seg], r_send.at[3 * c + i], r_recv.at[3 * c + i], px, order[i])
                    copy.start()
                    hops.append(copy)
        reduces.append(hops)
        if c > 0:
            finish(c - 1)
    finish(n - 1)

    for copy in swaps + [a_copy] + list(lasts.values()) + [x for hops in reduces for x in hops]:
        copy.wait_send()
    for c in range(n):
        for k in range(pieces[c]):
            gathers[c](k).wait_send()


def combine(split, cuts, pieces, hidden, attn, w_o, w_down, own, first, mid, last):
    any_spec = pl.BlockSpec(memory_space=pl.ANY)
    hbm = pl.BlockSpec(memory_space=pltpu.HBM)
    vmem = pl.BlockSpec(memory_space=pltpu.VMEM)
    dma = pltpu.SemaphoreType.DMA
    n = len(cuts)
    return pl.pallas_call(
        functools.partial(combine_kernel, split, cuts, pieces),
        out_shape=jax.ShapeDtypeStruct((256, 256), BF16),
        in_specs=[hbm, vmem, hbm, hbm, any_spec, vmem, vmem, vmem],
        out_specs=vmem,
        scratch_shapes=[
            pltpu.VMEM((256, 256), BF16),
            pltpu.VMEM((512, 1024), BF16),
            pltpu.VMEM((4096, 1024), BF16),
            pltpu.VMEM((128, 8192), F32),
            pltpu.VMEM((split[2], 8192), F32),
            pltpu.VMEM((256, 4096), BF16),
            pltpu.VMEM((4, 2, 32, 256), BF16),
            pltpu.VMEM((2, 256, 256), BF16),
            pltpu.VMEM((4, 256, 256), F32),
            pltpu.VMEM((4, 256, 256), F32),
            dma((4,)), dma((n,)), dma((n,)), dma((4,)), dma((4,)), dma((sum(pieces),)), dma((sum(pieces),)), dma((3 * n,)), dma((3 * n,)),
        ],
        compiler_params=pltpu.CompilerParams(collective_id=1, has_side_effects=True, vmem_limit_bytes=48 * 2**20),
        cost_estimate=pl.CostEstimate(flops=3_000_000_000, bytes_accessed=18 * 2**20, transcendentals=0),
        name="combine",
    )(hidden, attn, w_o, w_down, own, first, mid, last)


def solution(mesh):
    hidden_spec = P('dp', ('tpx', 'tpy'))
    cache_spec = P(('dp', 'tpx', 'tpy'), None, None)
    in_specs = (hidden_spec, P(('tpx', 'tpy')), P('tpx', 'tpy'), P('tpx', None), P('tpx', None), P('tpx', 'tpy'), P('tpx', 'tpy'), P('tpy', 'tpx'), P('tpy', 'tpx'), cache_spec, cache_spec, P(('dp', 'tpx', 'tpy')))
    out_specs = (hidden_spec, cache_spec, cache_spec)
    split, cuts, pieces = (48, 64, 16), (48, 32, 32, 16), (1, 1, 2, 2)
    swap = [(0, 1), (1, 0)]

    def device_step(hidden, ln_scale, w_q, w_k, w_v, w_gate, w_up, w_o, w_down, k_cache, v_cache, positions):
        q, kn, vn, own, first, mid, last = project(split, hidden, ln_scale, w_q, w_k, w_v, w_gate, w_up)
        mid = lax.ppermute(mid, 'tpx', swap)
        late_pos, kn = lax.optimization_barrier((positions, kn))
        cos_tab, sin_tab = rope_tables(late_pos, k_cache.shape[2])
        k_all, v_all, attn = attend(positions, q, kn, vn, cos_tab, sin_tab, k_cache, v_cache)
        hidden_out = combine(split, cuts, pieces, hidden, attn, w_o, w_down, own, first, mid, last)
        return hidden_out, k_all, v_all

    return jax.shard_map(device_step, mesh=mesh, in_specs=in_specs, out_specs=out_specs, check_vma=False)
```

```python
import functools
import jax
import jax.numpy as jnp
from jax import lax
from jax.experimental import pallas as pl
from jax.experimental.pallas import tpu as pltpu
from jax.sharding import PartitionSpec as P

LN_EPS = 1e-6
ROPE_BASE = 10000.0
MESH = pl.DeviceIdType.MESH
F32 = jnp.float32
BF16 = jnp.bfloat16
RING = 8
AHEAD = 4
HELD = 5


def rope_tables(positions, head_dim):
    half_dim = head_dim // 2
    inv_freq = ROPE_BASE ** (-(jnp.arange(half_dim, dtype=F32) * 2.0 / head_dim))
    angles = positions.astype(F32)[:, None] * inv_freq[None, :]
    return jnp.cos(angles), jnp.sin(angles)


def rotate(x, cos_tab, sin_tab):
    half = x.shape[-1] // 2
    lead, tail = x[:, :half], x[:, half:]
    return jnp.concatenate([lead * cos_tab - tail * sin_tab, lead * sin_tab + tail * cos_tab], axis=-1)


def others(px, py):
    return [(lax.rem(px + dx, 2), lax.rem(py + dy, 4)) for dx in range(2) for dy in range(4) if (dx, dy) != (0, 0)]


def greet(peers):
    barrier = pltpu.get_barrier_semaphore()
    for qx, qy in peers:
        pl.semaphore_signal(barrier, 1, device_id={'tpx': qx, 'tpy': qy}, device_id_type=MESH)


def met(count):
    pl.semaphore_wait(pltpu.get_barrier_semaphore(), count)


def remote(src, dst, send_sem, recv_sem, qx, qy):
    return pltpu.make_async_remote_copy(src, dst, send_sem, recv_sem, device_id={'tpx': qx, 'tpy': qy}, device_id_type=MESH)


def project_kernel(split, h_hbm, scale_hbm, wq_hbm, wk_hbm, wv_hbm, wg_hbm, wu_hbm,
                   q_out, kn_out, vn_out, own_out, first_out, mid_out, last_out,
                   hbuf, scale, msg, stats_col, u, wq, wkv, wg, wu, part, qpart, qrec, kvpart, kvrec, qsum, qall,
                   load_sem, h_send, h_recv, m_send, m_recv, x_send, x_recv, f_send, f_recv, a_send, a_recv, o_sem, go_sem):
    px, py = lax.axis_index('tpx'), lax.axis_index('tpy')
    me = px * 4 + py
    mate = py + 1 - 2 * lax.rem(py, 2)
    across = lax.rem(py + 2, 4)
    n_seq = 32

    loads = [
        pltpu.make_async_copy(h_hbm, hbuf.at[py], load_sem.at[0]),
        pltpu.make_async_copy(scale_hbm, scale, load_sem.at[1]),
        pltpu.make_async_copy(wk_hbm, wkv.at[:, pl.ds(0, 256)], load_sem.at[2]),
        pltpu.make_async_copy(wv_hbm, wkv.at[:, pl.ds(256, 256)], load_sem.at[3]),
        pltpu.make_async_copy(wq_hbm, wq, load_sem.at[4]),
        pltpu.make_async_copy(wg_hbm, wg, load_sem.at[5]),
        pltpu.make_async_copy(wu_hbm, wu, load_sem.at[6]),
    ]
    for copy in loads[:2]:
        copy.start()
    greet(others(px, py))
    for copy in loads[2:]:
        copy.start()
    loads[0].wait()
    far = pl.ds(pl.multiple_of((1 - px) * 128, 128), 128)
    near = pl.ds(pl.multiple_of(px * 128, 128), 128)

    def h_copy(block, rows, at, qy):
        return remote(hbuf.at[block, rows], hbuf.at[block, rows], h_send.at[at], h_recv.at[at], px, qy)

    to_across = [h_copy(py, far, 0, across), h_copy(py, near, 1, across)]
    to_mate = [h_copy(py, far, 2, mate), h_copy(py, near, 3, mate)]
    relays = [h_copy(across, far, 4, mate), h_copy(across, near, 5, mate)]

    hf = hbuf[py].astype(F32)
    mean = jnp.sum(hf, axis=1, keepdims=True) * (1.0 / 256.0)
    dev = hf - mean
    m2 = jnp.sum(dev * dev, axis=1, keepdims=True)
    lane = lax.broadcasted_iota(jnp.int32, (256, 128), 1)
    stat = jnp.where(lane == 0, mean, m2)
    stat_t = stat.T
    loads[1].wait()
    msg[me] = jnp.concatenate([stat_t[0:2], scale[...], jnp.zeros((5, 256), F32)], axis=0)
    met(7)
    msgs = []
    for i, (qx, qy) in enumerate(others(px, py)):
        copy = remote(msg.at[me], msg.at[me], m_send.at[i], m_recv.at[i], qx, qy)
        copy.start()
        msgs.append(copy)
    to_across[0].start()
    to_mate[0].start()
    to_across[1].start()
    to_mate[1].start()
    to_across[0].wait_recv()
    relays[0].start()
    for copy in msgs:
        copy.wait_recv()

    means = jnp.concatenate([msg[e, 0:1] for e in range(8)], axis=0)
    m2s = jnp.concatenate([msg[e, 1:2] for e in range(8)], axis=0)
    mu = jnp.sum(means, axis=0, keepdims=True) * 0.125
    gap = means - mu
    var = (jnp.sum(m2s, axis=0, keepdims=True) + 256.0 * jnp.sum(gap * gap, axis=0, keepdims=True)) * (1.0 / 2048.0)
    rstd = lax.rsqrt(var + LN_EPS)
    both = jnp.concatenate([mu, rstd, jnp.zeros((126, 256), F32)], axis=0).T
    stats_col[...] = both

    def norm(t, rows):
        cols = pl.ds(pl.multiple_of(t * 256, 256), 256)
        table = stats_col[rows, :]
        u[rows, cols] = ((hbuf[t, rows, :].astype(F32) - table[:, 0:1]) * table[:, 1:2] * msg[px * 4 + t, 2:3]).astype(BF16)

    def gather(i, rows):
        norm(py, rows)
        norm(across, rows)
        to_mate[i].wait_recv()
        norm(mate, rows)
        relays[i].wait_recv()
        norm(lax.rem(mate + 2, 4), rows)

    far_seq = pl.ds(pl.multiple_of((1 - px) * 128 + py * n_seq, n_seq), n_seq)
    near_seq = pl.ds(pl.multiple_of(px * 128 + py * n_seq, n_seq), n_seq)
    loads[2].wait()
    loads[3].wait()
    gather(0, far_seq)
    kvpart[pl.ds(0, n_seq), :] = jnp.dot(u[far_seq, :], wkv[...], preferred_element_type=F32)
    kv_copy = remote(kvpart.at[pl.ds(0, n_seq)], kvrec, x_send.at[1], x_recv.at[1], 1 - px, py)
    kv_copy.start()
    for t in range(4):
        norm(t, far)
    loads[4].wait()
    qpart[far, :] = jnp.dot(u[far, :], wq[...], preferred_element_type=F32)
    q_copy = remote(qpart.at[far], qrec, x_send.at[0], x_recv.at[0], 1 - px, py)
    q_copy.start()
    to_across[1].wait_recv()
    relays[1].start()
    gather(1, near)

    loads[5].wait()
    loads[6].wait()
    step = 512
    n_step = 4096 // step
    n_first, n_mid, n_last = split
    first_rows = pl.ds(pl.multiple_of((1 - px) * 128, 8), n_first)
    mid_rows = pl.ds(pl.multiple_of((1 - px) * 128 + n_first, 8), n_mid)
    last_rows = pl.ds(pl.multiple_of((1 - px) * 128 + n_first + n_mid, 8), n_last)

    def first_copy(i, base):
        cols = pl.ds(pl.multiple_of(base * 4096 + i * step, step), step)
        at = base * n_step + i
        return remote(part.at[first_rows, cols], first_out.at[:, cols], f_send.at[at], f_recv.at[at], 1 - px, py)

    holds = lax.rem(py, 2) == 1
    n_piece = 2 * n_step

    def columns(i, carry):
        cols = pl.ds(pl.multiple_of(i * step, step), step)
        part[:, cols] = jnp.dot(u[...], wg[:, cols], preferred_element_type=F32)
        up_cols = pl.ds(pl.multiple_of(4096 + i * step, step), step)

        @pl.when(jnp.logical_or(jnp.logical_not(holds), 2 * i < n_piece - HELD))
        def _():
            first_copy(i, 0).start()

        part[:, up_cols] = jnp.dot(u[...], wu[:, cols], preferred_element_type=F32)

        @pl.when(jnp.logical_or(jnp.logical_not(holds), 2 * i + 1 < n_piece - HELD))
        def _():
            first_copy(i, 1).start()

        return carry

    lax.fori_loop(0, n_step, columns, 0)
    outs = [
        pltpu.make_async_copy(part.at[near], own_out, o_sem.at[0]),
        pltpu.make_async_copy(part.at[mid_rows], mid_out, o_sem.at[1]),
        pltpu.make_async_copy(part.at[last_rows], last_out, o_sem.at[2]),
    ]
    for copy in outs:
        copy.start()
    qpart[near, :] = jnp.dot(u[near, :], wq[...], preferred_element_type=F32)
    kvpart[pl.ds(n_seq, n_seq), :] = jnp.dot(u[near_seq, :], wkv[...], preferred_element_type=F32)

    q_copy.wait_recv()
    for t in range(4):
        rows_t = pl.ds(pl.multiple_of(px * 128 + t * n_seq, n_seq), n_seq)
        qsum[t] = (qpart[rows_t, :] + qrec[pl.ds(t * n_seq, n_seq), :]).astype(BF16)
    hops = []
    for i in range(1, 4):
        t = lax.rem(py + i, 4)
        copy = remote(qsum.at[t], qall.at[py], a_send.at[i - 1], a_recv.at[i - 1], px, t)
        copy.start()
        hops.append(copy)
    kv_copy.wait_recv()
    kv = (kvpart[pl.ds(n_seq, n_seq), :] + kvrec[...]).astype(BF16).astype(F32)
    kn_out[...] = kv[:, :256]
    vn_out[...] = kv[:, 256:]

    def emit(t, block):
        block = block.astype(F32)
        for j in range(2):
            row = pl.multiple_of((2 * t + j) * n_seq, n_seq)
            for half in range(2):
                q_out[half, pl.ds(row, n_seq), :] = block[:, (2 * j + half) * 128:(2 * j + half + 1) * 128]

    emit(py, qsum[py])
    for i in range(1, 4):
        hops[i - 1].wait_recv()
        t = lax.rem(py + 4 - i, 4)
        emit(t, qall[t])

    for copy in outs:
        copy.wait()
    for copy in to_across + to_mate + relays + msgs + hops + [q_copy, kv_copy]:
        copy.wait_send()

    @pl.when(jnp.logical_not(holds))
    def _():
        first_copy(n_step - 1, 0).wait_send()
        pl.semaphore_signal(go_sem, 1, device_id={'tpx': px, 'tpy': mate}, device_id_type=MESH)

    @pl.when(holds)
    def _():
        pl.semaphore_wait(go_sem, 1)
        for k in range(n_piece - HELD, n_piece):
            first_copy(k // 2, k % 2).start()
        first_copy(n_step - 1, 0).wait_send()

    def settle(i, carry):
        first_copy(i, 0).wait_recv()
        first_copy(i, 1).wait()

        @pl.when(i < n_step - 1)
        def _():
            first_copy(i, 0).wait_send()

        return carry

    lax.fori_loop(0, n_step, settle, 0)


def project(split, hidden, ln_scale, w_q, w_k, w_v, w_gate, w_up):
    any_spec = pl.BlockSpec(memory_space=pl.ANY)
    hbm = pl.BlockSpec(memory_space=pltpu.HBM)
    vmem = pl.BlockSpec(memory_space=pltpu.VMEM)
    sds = jax.ShapeDtypeStruct
    dma = pltpu.SemaphoreType.DMA
    return pl.pallas_call(
        functools.partial(project_kernel, split),
        out_shape=[sds((2, 256, 128), F32), sds((32, 256), F32), sds((32, 256), F32), sds((128, 8192), F32)] + [sds((r, 8192), F32) for r in split],
        in_specs=[hbm] * 7,
        out_specs=[vmem, vmem, vmem] + [any_spec] * 4,
        scratch_shapes=[
            pltpu.VMEM((4, 256, 256), BF16),
            pltpu.VMEM((1, 256), F32),
            pltpu.VMEM((8, 8, 256), F32),
            pltpu.VMEM((256, 128), F32),
            pltpu.VMEM((256, 1024), BF16),
            pltpu.VMEM((1024, 512), BF16),
            pltpu.VMEM((1024, 512), BF16),
            pltpu.VMEM((1024, 4096), BF16),
            pltpu.VMEM((1024, 4096), BF16),
            pltpu.VMEM((256, 8192), F32),
            pltpu.VMEM((256, 512), F32),
            pltpu.VMEM((128, 512), F32),
            pltpu.VMEM((64, 512), F32),
            pltpu.VMEM((32, 512), F32),
            pltpu.VMEM((4, 32, 512), BF16),
            pltpu.VMEM((4, 32, 512), BF16),
            dma((7,)), dma((6,)), dma((6,)), dma((7,)), dma((7,)), dma((2,)), dma((2,)), dma((16,)), dma((16,)), dma((3,)), dma((3,)), dma((3,)), pltpu.SemaphoreType.REGULAR,
        ],
        compiler_params=pltpu.CompilerParams(collective_id=0, has_side_effects=True, vmem_limit_bytes=48 * 2**20),
        cost_estimate=pl.CostEstimate(flops=5_000_000_000, bytes_accessed=28 * 2**20, transcendentals=0),
        name="project",
    )(*[pltpu.with_memory_space_constraint(x, pltpu.HBM) for x in (hidden, ln_scale.reshape(1, 256), w_q, w_k, w_v, w_gate, w_up)])


def attend_kernel(pos_ref, q_in, kn_in, vn_ref, cos_ref, sin_ref, k_hbm, v_hbm, k_out, v_out, o_ref, kbuf, vbuf, q_ref, kn_ref, k_in, v_in, k_wr, v_wr):
    n_seq, cache_len, head_dim = k_hbm.shape

    def fetch(b):
        slot = lax.rem(b, RING)
        return (pltpu.make_async_copy(k_hbm.at[b], kbuf.at[slot], k_in.at[slot]),
                pltpu.make_async_copy(v_hbm.at[b], vbuf.at[slot], v_in.at[slot]))

    def drain(b):
        slot = lax.rem(b, RING)
        return (pltpu.make_async_copy(kbuf.at[slot], k_out.at[b], k_wr.at[slot]),
                pltpu.make_async_copy(vbuf.at[slot], v_out.at[b], v_wr.at[slot]))

    for b in range(AHEAD):
        for copy in fetch(b):
            copy.start()

    cos_tab, sin_tab = cos_ref[...], sin_ref[...]
    kn_ref[...] = rotate(kn_in[...], cos_tab, sin_tab).astype(BF16).astype(F32)
    for h in range(8):
        rows = pl.ds(h * n_seq, n_seq)
        lead, tail = q_in[0, rows, :], q_in[1, rows, :]
        q_ref[0, rows, :] = (lead * cos_tab - tail * sin_tab).astype(BF16).astype(F32)
        q_ref[1, rows, :] = (lead * sin_tab + tail * cos_tab).astype(BF16).astype(F32)

    def patch(buf, slot, row, p):
        base = pl.multiple_of((p // 16) * 16, 16)
        tile = buf[slot, pl.ds(base, 16), :]
        hit = lax.broadcasted_iota(jnp.int32, (16, head_dim), 0) == p - base
        buf[slot, pl.ds(base, 16), :] = jnp.where(hit, row, tile.astype(F32)).astype(BF16)

    def one(b, carry):
        slot = lax.rem(b, RING)
        p = pos_ref[b]

        @pl.when(b + AHEAD < n_seq)
        def _():
            @pl.when(b + AHEAD >= RING)
            def _():
                for copy in drain(b + AHEAD - RING):
                    copy.wait()
            for copy in fetch(b + AHEAD):
                copy.start()

        k_copy, v_copy = fetch(b)
        k_save, v_save = drain(b)
        k_copy.wait()
        patch(kbuf, slot, kn_ref[pl.ds(b, 1), :], p)
        k_save.start()
        heads = pl.ds(b, 8, stride=n_seq)
        q = jnp.concatenate([q_ref[0, heads, :], q_ref[1, heads, :]], axis=1).astype(BF16)
        scores = lax.dot_general(q, kbuf[slot], (((1,), (1,)), ((), ())), preferred_element_type=F32) * (head_dim ** -0.5)
        valid = lax.broadcasted_iota(jnp.int32, scores.shape, 1) <= p
        scores = jnp.where(valid, scores, -jnp.inf)
        top = jnp.max(scores, axis=1, keepdims=True)
        e = jnp.exp(scores - top)
        prob = (e / jnp.sum(e, axis=1, keepdims=True)).astype(BF16)
        v_copy.wait()
        patch(vbuf, slot, vn_ref[pl.ds(b, 1), :], p)
        v_save.start()
        out = jnp.dot(prob, vbuf[slot], preferred_element_type=F32)
        o_ref[0, heads, :] = out[:, :128]
        o_ref[1, heads, :] = out[:, 128:]
        return carry

    lax.fori_loop(0, n_seq, one, 0)
    for b in range(n_seq - RING, n_seq):
        for copy in drain(b):
            copy.wait()


def attend(positions, q, kn, vn, cos_tab, sin_tab, k_cache, v_cache):
    any_spec = pl.BlockSpec(memory_space=pl.ANY)
    vmem = pl.BlockSpec(memory_space=pltpu.VMEM)
    n_seq, cache_len, head_dim = k_cache.shape
    dma = pltpu.SemaphoreType.DMA
    return pl.pallas_call(
        attend_kernel,
        out_shape=[jax.ShapeDtypeStruct(k_cache.shape, BF16), jax.ShapeDtypeStruct(v_cache.shape, BF16), jax.ShapeDtypeStruct((2, 256, 128), F32)],
        in_specs=[pl.BlockSpec(memory_space=pltpu.SMEM), vmem, vmem, vmem, vmem, vmem, any_spec, any_spec],
        out_specs=[any_spec, any_spec, vmem],
        scratch_shapes=[
            pltpu.VMEM((RING, cache_len, head_dim), BF16),
            pltpu.VMEM((RING, cache_len, head_dim), BF16),
            pltpu.VMEM((2, 256, 128), F32),
            pltpu.VMEM((n_seq, head_dim), F32),
            dma((RING,)), dma((RING,)), dma((RING,)), dma((RING,)),
        ],
        compiler_params=pltpu.CompilerParams(vmem_limit_bytes=48 * 2**20),
        cost_estimate=pl.CostEstimate(flops=100_000_000_000, bytes_accessed=128 * 2**20, transcendentals=0),
        name="attend",
    )(positions, q, kn, vn, cos_tab, sin_tab, k_cache, v_cache)


def combine_kernel(split, cuts, pieces, h_hbm, attn_ref, wo_hbm, wd_hbm, own_hbm, first_ref, mid_ref, last_ref,
                   out_ref, h, wo, wd, own, got, act, a_snd, a_rcv, res, res_rcv,
                   load_sem, l_send, l_recv, t_send, t_recv, g_send, g_recv, r_send, r_recv):
    px, py = lax.axis_index('tpx'), lax.axis_index('tpy')
    me = px * 4 + py
    n = len(cuts)
    starts = [sum(cuts[:c]) for c in range(n)]
    n_first, n_mid, n_last = split
    late = n_first + n_mid
    mate = py + 1 - 2 * lax.rem(py, 2)
    order = [lax.rem(py + 2, 4), lax.rem(mate + 2, 4), mate, py]
    leads = lax.rem(py, 2) == 0
    greet([(px, order[0]), (1 - px, py)])
    loads = [
        pltpu.make_async_copy(own_hbm, own, load_sem.at[0]),
        pltpu.make_async_copy(wo_hbm, wo, load_sem.at[1]),
        pltpu.make_async_copy(wd_hbm, wd, load_sem.at[2]),
        pltpu.make_async_copy(h_hbm, h, load_sem.at[3]),
    ]
    for copy in loads:
        copy.start()
    for t in range(4):
        for j in range(2):
            at = pl.ds((2 * t + j) * 32, 32)
            a_snd[t, j] = jnp.concatenate([attn_ref[0, at, :], attn_ref[1, at, :]], axis=1).astype(BF16)

    @pl.when(leads)
    def _():
        met(2)
        greet([(px, mate)])

    @pl.when(jnp.logical_not(leads))
    def _():
        met(3)
        greet([(px, mate)])

    lasts = {}
    for c in range(n):
        if starts[c] >= late:
            seg = pl.ds(starts[c] - late, cuts[c])
            lasts[c] = remote(last_ref.at[seg], got.at[seg], l_send.at[c], l_recv.at[c], 1 - px, py)
            lasts[c].start()
    rows_me = pl.ds(pl.multiple_of(me * 32, 32), 32)
    swaps = []
    for i in range(3):
        swaps.append(remote(a_snd.at[order[i]], a_rcv.at[:, rows_me, :], t_send.at[i], t_recv.at[i], px, order[i]))
    swaps[0].start()
    for j in range(2):
        a_rcv[j, rows_me, :] = a_snd[py, j]

    def activate(c):
        here = pl.ds(starts[c], cuts[c])
        if starts[c] < n_first:
            theirs, there = first_ref, here
        elif starts[c] < late:
            theirs, there = mid_ref, pl.ds(starts[c] - n_first, cuts[c])
        else:
            theirs, there = got, pl.ds(starts[c] - late, cuts[c])

        n_piece = pieces[c]
        width = 4096 // n_piece

        def piece(k):
            cols = pl.ds(pl.multiple_of(k * width, width), width)
            return remote(act.at[pl.ds(2 * starts[c], cuts[c]), cols], act.at[pl.ds(2 * starts[c] + cuts[c], cuts[c]), cols],
                          g_send.at[sum(pieces[:c]) + k], g_recv.at[sum(pieces[:c]) + k], 1 - px, py)

        def cols(k, carry):
            for i in range(width // 512):
                g_cols = pl.ds(pl.multiple_of(k * width + i * 512, 512), 512)
                u_cols = pl.ds(pl.multiple_of(4096 + k * width + i * 512, 512), 512)
                gate = (own[here, g_cols] + theirs[there, g_cols]).astype(BF16).astype(F32)
                up = (own[here, u_cols] + theirs[there, u_cols]).astype(BF16).astype(F32)
                act[pl.ds(2 * starts[c], cuts[c]), g_cols] = (jax.nn.silu(gate) * up).astype(BF16)
            piece(k).start()
            return carry

        lax.fori_loop(0, n_piece, cols, 0)
        return piece

    loads[0].wait()
    gathers = [activate(0)]

    @pl.when(leads)
    def _():
        met(1)

    swaps[1].start()
    swaps[2].start()
    for copy in swaps:
        copy.wait_recv()
    near = pl.ds(pl.multiple_of(px * 128, 128), 128)
    a_copy = remote(a_rcv.at[:, near, :], a_rcv.at[:, near, :], t_send.at[3], t_recv.at[3], 1 - px, py)
    a_copy.start()
    gathers += [activate(c) for c in range(1, n) if starts[c] < late]

    loads[1].wait()
    a_copy.wait_recv()
    for c in range(n):
        for side in range(2):
            at = pl.ds(pl.multiple_of(lax.rem(px + side, 2) * 128 + starts[c], 16), cuts[c])
            for t in range(4):
                cols = pl.ds(t * 256, 256)
                res[t, pl.ds(2 * starts[c] + side * cuts[c], cuts[c]), :] = (
                    jnp.dot(a_rcv[0, at, :], wo[pl.ds(0, 256), cols], preferred_element_type=F32)
                    + jnp.dot(a_rcv[1, at, :], wo[pl.ds(256, 256), cols], preferred_element_type=F32))
    for c in lasts:
        lasts[c].wait_recv()
        gathers.append(activate(c))

    loads[2].wait()
    loads[3].wait()
    reduces = []

    def finish(c):
        seg = pl.ds(2 * starts[c], 2 * cuts[c])
        total = res[py, seg, :]
        for i in range(3):
            reduces[c][i].wait_recv()
            total = total + res_rcv[order[i], seg, :]
        for side in range(2):
            at = pl.ds(pl.multiple_of(lax.rem(px + side, 2) * 128 + starts[c], 16), cuts[c])
            out_ref[at, :] = (h[at, :].astype(F32) + total[side * cuts[c]:(side + 1) * cuts[c]]).astype(BF16)

    for c in range(n):
        seg = pl.ds(2 * starts[c], 2 * cuts[c])
        hops = []
        parts = pieces[c]
        depth = 4096 // parts
        for p in range(parts):
            gathers[c](p).wait_recv()
            deep = pl.ds(p * depth, depth)
            if p < parts - 1:
                term = jnp.dot(act[seg, deep], wd[deep, :], preferred_element_type=F32)
                for t in range(4):
                    res[t, seg, :] += term[:, t * 256:(t + 1) * 256]
                continue
            for side in range(2):
                pair = lax.rem(py // 2 + 1 + side, 2)
                cols = pl.ds(pl.multiple_of(pair * 512, 512), 512)
                term = jnp.dot(act[seg, deep], wd[deep, cols], preferred_element_type=F32)
                res[2 * pair, seg, :] += term[:, :256]
                res[2 * pair + 1, seg, :] += term[:, 256:]
                for i in ((0, 1), (2,))[side]:
                    copy = remote(res.at[order[i], seg], res_rcv.at[py, seg], r_send.at[3 * c + i], r_recv.at[3 * c + i], px, order[i])
                    copy.start()
                    hops.append(copy)
        reduces.append(hops)
        if c > 0:
            finish(c - 1)
    finish(n - 1)

    for copy in swaps + [a_copy] + list(lasts.values()) + [x for hops in reduces for x in hops]:
        copy.wait_send()
    for c in range(n):
        for k in range(pieces[c]):
            gathers[c](k).wait_send()


def combine(split, cuts, pieces, hidden, attn, w_o, w_down, own, first, mid, last):
    any_spec = pl.BlockSpec(memory_space=pl.ANY)
    hbm = pl.BlockSpec(memory_space=pltpu.HBM)
    vmem = pl.BlockSpec(memory_space=pltpu.VMEM)
    dma = pltpu.SemaphoreType.DMA
    n = len(cuts)
    return pl.pallas_call(
        functools.partial(combine_kernel, split, cuts, pieces),
        out_shape=jax.ShapeDtypeStruct((256, 256), BF16),
        in_specs=[hbm, vmem, hbm, hbm, any_spec, vmem, vmem, vmem],
        out_specs=vmem,
        scratch_shapes=[
            pltpu.VMEM((256, 256), BF16),
            pltpu.VMEM((512, 1024), BF16),
            pltpu.VMEM((4096, 1024), BF16),
            pltpu.VMEM((128, 8192), F32),
            pltpu.VMEM((split[2], 8192), F32),
            pltpu.VMEM((256, 4096), BF16),
            pltpu.VMEM((4, 2, 32, 256), BF16),
            pltpu.VMEM((2, 256, 256), BF16),
            pltpu.VMEM((4, 256, 256), F32),
            pltpu.VMEM((4, 256, 256), F32),
            dma((4,)), dma((n,)), dma((n,)), dma((4,)), dma((4,)), dma((sum(pieces),)), dma((sum(pieces),)), dma((3 * n,)), dma((3 * n,)),
        ],
        compiler_params=pltpu.CompilerParams(collective_id=1, has_side_effects=True, vmem_limit_bytes=48 * 2**20),
        cost_estimate=pl.CostEstimate(flops=3_000_000_000, bytes_accessed=18 * 2**20, transcendentals=0),
        name="combine",
    )(hidden, attn, w_o, w_down, own, first, mid, last)


def solution(mesh):
    hidden_spec = P('dp', ('tpx', 'tpy'))
    cache_spec = P(('dp', 'tpx', 'tpy'), None, None)
    in_specs = (hidden_spec, P(('tpx', 'tpy')), P('tpx', 'tpy'), P('tpx', None), P('tpx', None), P('tpx', 'tpy'), P('tpx', 'tpy'), P('tpy', 'tpx'), P('tpy', 'tpx'), cache_spec, cache_spec, P(('dp', 'tpx', 'tpy')))
    out_specs = (hidden_spec, cache_spec, cache_spec)
    split, cuts, pieces = (48, 64, 16), (48, 32, 32, 16), (1, 1, 2, 2)
    swap = [(0, 1), (1, 0)]

    def device_step(hidden, ln_scale, w_q, w_k, w_v, w_gate, w_up, w_o, w_down, k_cache, v_cache, positions):
        q, kn, vn, own, first, mid, last = project(split, hidden, ln_scale, w_q, w_k, w_v, w_gate, w_up)
        mid = lax.ppermute(mid, 'tpx', swap)
        late_pos, kn = lax.optimization_barrier((positions, kn))
        cos_tab, sin_tab = rope_tables(late_pos, k_cache.shape[2])
        k_all, v_all, attn = attend(positions, q, kn, vn, cos_tab, sin_tab, k_cache, v_cache)
        hidden_out = combine(split, cuts, pieces, hidden, attn, w_o, w_down, own, first, mid, last)
        return hidden_out, k_all, v_all

    return jax.shard_map(device_step, mesh=mesh, in_specs=in_specs, out_specs=out_specs, check_vma=False)
```
